32 devices in a mesh: section: 2 (over core), dp: 8 (over z, x), mp: 2 (over y).
Axes of the slice: x: 2, y: 2, z: 4, core: 2. Of those that a mesh axis runs over, the one named last changes fastest.
Arguments:
- images: bfloat16 [2, 16, 197, 1024], P(None, 'dp'), may hold values from -6 to 6
- cotangent: bfloat16 [2, 16, 197, 1024], P(None, 'dp'), may hold values from -6 to 6
- live_count: int32 [2, 8], P(None, 'dp'), may hold values from 1 to 2, as said below
- ln1_gain: bfloat16 [2, 1024], P('section', 'dp'), may hold values from 0.099609375 to 1.8984375
- ln1_bias: bfloat16 [2, 1024], P('section', 'dp'), may hold values from -3 to 3
- qkv_weight: bfloat16 [2, 3, 1024, 1024], P('section', None, 'dp', 'mp'), may hold values from -0.1875 to 0.1875
- qv_bias: bfloat16 [2, 2, 16, 64], P('section', None, 'mp', 'dp'), may hold values from -3 to 3
- out_weight: bfloat16 [2, 1024, 1024], P('section', 'mp', 'dp'), may hold values from -1.5 to 1.5
- out_bias: bfloat16 [2, 1024], P('section', 'dp'), may hold values from -3 to 3
- ln2_gain: bfloat16 [2, 1024], P('section', 'dp'), may hold values from 0.099609375 to 1.8984375
- ln2_bias: bfloat16 [2, 1024], P('section', 'dp'), may hold values from -3 to 3
- up_weight: bfloat16 [2, 1024, 4096], P('section', 'dp', 'mp'), may hold values from -0.1875 to 0.1875
- up_bias: bfloat16 [2, 16, 256], P('section', 'mp', 'dp'), may hold values from -3 to 3
- down_weight: bfloat16 [2, 4096, 1024], P('section', 'mp', 'dp'), may hold values from -0.09375 to 0.09375
- down_bias: bfloat16 [2, 1024], P('section', 'dp'), may hold values from -3 to 3
Outputs:
- activations: bfloat16 [2, 2, 16, 197, 1024], P('section', None, 'dp')
- input_grads: bfloat16 [2, 2, 16, 197, 1024], P('section', None, 'dp')
- grad_ln1_gain: float32 [2, 1024], P('section', 'dp')
- grad_ln1_bias: float32 [2, 1024], P('section', 'dp')
- grad_qkv_weight: float32 [2, 3, 1024, 1024], P('section', None, 'dp', 'mp')
- grad_qv_bias: float32 [2, 2, 16, 64], P('section', None, 'mp', 'dp')
- grad_out_weight: float32 [2, 1024, 1024], P('section', 'mp', 'dp')
- grad_out_bias: float32 [2, 1024], P('section', 'dp')
- grad_ln2_gain: float32 [2, 1024], P('section', 'dp')
- grad_ln2_bias: float32 [2, 1024], P('section', 'dp')
- grad_up_weight: float32 [2, 1024, 4096], P('section', 'dp', 'mp')
- grad_up_bias: float32 [2, 16, 256], P('section', 'mp', 'dp')
- grad_down_weight: float32 [2, 4096, 1024], P('section', 'mp', 'dp')
- grad_down_bias: float32 [2, 1024], P('section', 'dp')
The draws below stay inside these ranges and needn't reach their ends.
Inputs may be any that keep to these rules, and one draw needn't show every extreme that they name: Micro-batch m has live_count[m, d] images on data device d, in its first slots; its other slots hold values that no output reads.
All inputs are finite; a program needn't handle non-finite values.
Results may differ from the reference program's by a relative error of at most 0.015.
Values may be sent and summed in bfloat16 or wider, within the bound.
A program may use at most 256 MiB of HBM per device.

```python
import math
import jax
import jax.numpy as jnp
from jax import lax

D = 1024
H = 16
HD = 64
FF = 4096
L = 197
SL = 2
MB = 2
SECTIONS = 2
SLOTS = 16
DATA_DEVS = 8
FFG = 256


def draw_live_count(key, part):
    base = jax.random.randint(jax.random.fold_in(key, 11), (MB, DATA_DEVS), 1, SL + 1)
    chosen = jax.random.randint(jax.random.fold_in(key, 12), (MB, 1), 0, DATA_DEVS)
    position = jnp.arange(DATA_DEVS)[None, :]
    base = jnp.where(position == chosen, SL, base)
    base = jnp.where(position == (chosen + 1) % DATA_DEVS, 1, base)
    return base.astype(jnp.int32)


def level_of(key, extent, cuts, least, largest):
    level, own = 1.0, jax.random.fold_in(key, 6)
    for dim, blocks in cuts:
        steps = jnp.exp(jax.random.uniform(jax.random.fold_in(own, dim), (blocks,), jnp.float32, least / len(cuts), largest / len(cuts)))
        level = level * jnp.repeat(steps, extent[dim] // blocks).reshape([-1 if axis == dim else 1 for axis in range(len(extent))])
    return level


def gaussian(rng, dims, width, most, split=(), kind=jnp.bfloat16):
    array = jax.random.normal(rng, dims, jnp.float32) * width
    if len(split) > 0:
        array = level_of(rng, dims, split, -0.22, 0.18) * array
    return jnp.clip(array, min=-most, max=most).astype(kind)


def setup_inputs(seed: int = 0) -> dict:
    key_list = jax.random.split(jax.random.key(seed), 16)
    images = gaussian(key_list[0], (MB, SLOTS, L, D), 1.0, 6.0, ((1, 8),))
    cotangent = gaussian(key_list[1], (MB, SLOTS, L, D), 1.0, 6.0, ((1, 8),))
    live_count = draw_live_count(jax.random.fold_in(key_list[15], 71), 0)
    ln1_gain = jnp.clip(1.0 + 0.18 * jax.random.normal(key_list[3], (SECTIONS, D), jnp.float32), 0.099609375, 1.8984375).astype(jnp.bfloat16)
    ln1_bias = gaussian(key_list[4], (SECTIONS, D), 0.5, 3.0, ((0, 2), (1, 8)))
    qkv_weight = gaussian(key_list[5], (SECTIONS, 3, D, D), D ** -0.5, 0.1875, ((0, 2), (2, 8), (3, 2)))
    qv_bias = gaussian(key_list[6], (SECTIONS, 2, H, HD), 0.5, 3.0, ((0, 2), (2, 2), (3, 8)))
    out_weight = gaussian(key_list[7], (SECTIONS, D, D), (D // HD) ** -0.5, 1.5, ((0, 2), (1, 2), (2, 8)))
    out_bias = gaussian(key_list[8], (SECTIONS, D), 0.5, 3.0, ((0, 2), (1, 8)))
    ln2_gain = jnp.clip(1.0 + 0.18 * jax.random.normal(key_list[9], (SECTIONS, D), jnp.float32), 0.099609375, 1.8984375).astype(jnp.bfloat16)
    ln2_bias = gaussian(key_list[10], (SECTIONS, D), 0.5, 3.0, ((0, 2), (1, 8)))
    up_weight = gaussian(key_list[11], (SECTIONS, D, FF), D ** -0.5, 0.1875, ((0, 2), (1, 8), (2, 2)))
    up_bias = gaussian(key_list[12], (SECTIONS, H, FFG), 0.5, 3.0, ((0, 2), (1, 2), (2, 8)))
    down_weight = gaussian(key_list[13], (SECTIONS, FF, D), FF ** -0.5, 0.09375, ((0, 2), (1, 2), (2, 8)))
    down_bias = gaussian(key_list[14], (SECTIONS, D), 0.5, 3.0, ((0, 2), (1, 8)))
    return dict(images=images, cotangent=cotangent, live_count=live_count, ln1_gain=ln1_gain, ln1_bias=ln1_bias, qkv_weight=qkv_weight, qv_bias=qv_bias, out_weight=out_weight, out_bias=out_bias, ln2_gain=ln2_gain, ln2_bias=ln2_bias, up_weight=up_weight, up_bias=up_bias, down_weight=down_weight, down_bias=down_bias)


epsilon = 1e-06
highest = lax.Precision.HIGHEST

@jax.custom_vjp
def low(v):
    return lax.optimization_barrier(v.astype(jnp.bfloat16)).astype(jnp.float32)

@jax.custom_vjp
def low_back(v):
    return v

def low_keep(v):
    return (low(v), None)

def low_pass(kept, grad):
    return (grad,)

def back_keep(v):
    return (v, None)

def back_low(kept, grad):
    return (low(grad),)
low.defvjp(low_keep, low_pass)
low_back.defvjp(back_keep, back_low)

def layer_norm(stream, gain, shift):
    centered = stream - lax.optimization_barrier(jnp.mean(stream, axis=-1, keepdims=True))
    inverse = lax.rsqrt(lax.optimization_barrier(jnp.mean(centered * centered, axis=-1, keepdims=True)) + epsilon)
    return centered * inverse * gain + shift

def block(stream, weights, rows):
    gain_one, shift_one, qkv_mat, qv_shift, out_mat, out_shift, gain_two, shift_two, up_mat, up_shift, down_mat, down_shift = weights
    batch_size, seq_len, model_width = stream.shape
    lowered = low(layer_norm(stream, gain_one, shift_one))
    projected = jnp.einsum('bld,cde->cble', lowered, qkv_mat, precision=highest)
    split_shape = (batch_size, seq_len, H, HD)
    queries = low(low_back(projected[0] + qv_shift[0])).reshape(split_shape)
    keys_low = low(low_back(projected[1])).reshape(split_shape)
    values_low = low(low_back(projected[2] + qv_shift[1])).reshape(split_shape)
    scores = low_back(jnp.einsum('blhe,bmhe->bhlm', queries, keys_low, precision=highest) * HD ** (-0.5))
    attn_probs = jax.nn.softmax(scores, axis=-1)
    mixed = low(low_back(jnp.einsum('bhlm,bmhe->blhe', low(attn_probs), values_low, precision=highest)))
    mixed = mixed.reshape(batch_size, seq_len, model_width)
    middle = stream + low_back(jnp.einsum('bld,de->ble', mixed, out_mat, precision=highest) + out_shift)
    lowered_two = low(layer_norm(middle, gain_two, shift_two))
    preact = low_back(jnp.einsum('bld,df->blf', lowered_two, up_mat, precision=highest) + up_shift)
    gelu_out = low(jax.nn.gelu(preact, approximate=False))
    result = middle + low_back(jnp.einsum('blf,fd->bld', gelu_out, down_mat, precision=highest) + down_shift)
    return result * rows

def section_weights(params, index):
    picked = [piece[index] for piece in params]
    picked[3] = picked[3].reshape(2, D)
    picked[9] = picked[9].reshape(FF)
    return tuple(picked)

def reference(images, cotangent, live_count, ln1_gain, ln1_bias, qkv_weight, qv_bias, out_weight, out_bias, ln2_gain, ln2_bias, up_weight, up_bias, down_weight, down_bias):
    params = tuple((piece.astype(jnp.float32) for piece in (ln1_gain, ln1_bias, qkv_weight, qv_bias, out_weight, out_bias, ln2_gain, ln2_bias, up_weight, up_bias, down_weight, down_bias)))
    count = MB * SLOTS
    group = math.gcd(count, 16)
    slot_of = jnp.arange(SLOTS).astype(jnp.int32) % SL
    live_rows = jnp.repeat(live_count, SL, axis=1)
    rows = (slot_of[None, :] < live_rows).astype(jnp.float32).reshape(count // group, group, 1, 1)
    entry = images.astype(jnp.float32).reshape(count, L, D)
    offset = jnp.zeros((count, L, D), jnp.float32)

    def apply_section(stream, weights):

        def one_group(pair):
            return block(pair[0], weights, pair[1])
        grouped = lax.map(jax.checkpoint(one_group), (stream.reshape(count // group, group, L, D), rows))
        return grouped.reshape(count, L, D)

    def whole(entry_in, offset_in, params_in):
        first_out = apply_section(entry_in, section_weights(params_in, 0))
        second_in = low(low_back(first_out + offset_in))
        second_out = apply_section(second_in, section_weights(params_in, 1))
        return (first_out, second_out)
    (first_out, second_out), pull = jax.vjp(whole, entry, offset, params)
    grad_entry, grad_offset, grad_params = pull((jnp.zeros_like(first_out), cotangent.astype(jnp.float32).reshape(count, L, D)))
    activations = jnp.stack([first_out, second_out]).astype(jnp.bfloat16).reshape(SECTIONS, MB, SLOTS, L, D)
    input_grads = jnp.stack([grad_entry, grad_offset]).astype(jnp.bfloat16).reshape(SECTIONS, MB, SLOTS, L, D)
    return (activations, input_grads, grad_params[0], grad_params[1], grad_params[2], grad_params[3], grad_params[4], grad_params[5], grad_params[6], grad_params[7], grad_params[8], grad_params[9], grad_params[10], grad_params[11])
```

```python
import math

import jax
import jax.numpy as jnp
from jax import lax
from jax.sharding import PartitionSpec as P

HD = 64


epsilon = 1e-06


def gather_all(small, big):
    flat = jnp.concatenate([piece.reshape(-1) for piece in small])
    packed = lax.all_gather(flat, "dp", axis=0, tiled=False)
    count = packed.shape[0]
    whole, offset = [], 0
    for piece, axis in zip(small, (1, 1, 3, 1, 1, 1, 2, 1)):
        part = packed[:, offset : offset + piece.size].reshape((count,) + piece.shape)
        offset += piece.size
        part = jnp.moveaxis(part, 0, axis)
        shape = list(piece.shape)
        shape[axis] *= count
        whole.append(part.reshape(shape))
    qkv, out, up, down = (
        lax.all_gather(piece, "dp", axis=axis, tiled=True) for piece, axis in zip(big, (2, 2, 1, 2))
    )
    return (
        whole[0],
        whole[1],
        qkv,
        whole[2],
        out,
        whole[3],
        whole[4],
        whole[5],
        up,
        whole[6],
        down,
        whole[7],
    )


def scatter_all(totals, shards):
    small_at = (0, 1, 3, 5, 6, 7, 9, 11)
    count = lax.axis_size("dp")
    rows = []
    for index, axis in zip(small_at, (1, 1, 3, 1, 1, 1, 2, 1)):
        piece = totals[index]
        shape = list(piece.shape)
        shape[axis : axis + 1] = [count, shape[axis] // count]
        rows.append(jnp.moveaxis(piece.reshape(shape), axis, 0).reshape(count, -1))
    packed = lax.psum_scatter(jnp.concatenate(rows, axis=1), "dp", scatter_dimension=0, tiled=False)
    owned, offset = [None] * 12, 0
    for index in small_at:
        size = shards[index].size
        owned[index] = packed[offset : offset + size].reshape(shards[index].shape)
        offset += size
    for index, axis in zip((2, 4, 8, 10), (2, 2, 1, 2)):
        owned[index] = lax.psum_scatter(
            totals[index].astype(jnp.bfloat16), "dp", scatter_dimension=axis, tiled=True
        ).astype(jnp.float32)
    return owned


def both_halves(partial):
    return lax.psum(partial.astype(jnp.bfloat16), "mp").astype(jnp.float32)


def from_behind(x, axis, by):
    length = lax.axis_size(axis)
    pairs = [(i, i + by) for i in range(length) if 0 <= i + by < length]
    return lax.ppermute(x, axis, pairs)


def norm_parts(stream):
    centered = stream - jnp.mean(stream, axis=-1, keepdims=True)
    inverse = lax.rsqrt(jnp.mean(centered * centered, axis=-1, keepdims=True) + epsilon)
    return (centered * inverse, inverse)


def norm_back(grad_normed, normed, inverse):
    first_mean = jnp.mean(grad_normed, axis=-1, keepdims=True)
    second_mean = jnp.mean(grad_normed * normed, axis=-1, keepdims=True)
    return inverse * (grad_normed - first_mean - normed * second_mean)


def gelu_slope(preact):
    cumul = 0.5 * (1.0 + lax.erf(preact * 2.0 ** (-0.5)))
    density = jnp.exp(-0.5 * preact * preact) * (2.0 * math.pi) ** (-0.5)
    return cumul + preact * density


def unpack_weights(whole):
    return (
        whole[0][0].astype(jnp.float32),
        whole[1][0].astype(jnp.float32),
        whole[2][0],
        whole[3][0].reshape(2, -1).astype(jnp.float32),
        whole[4][0],
        whole[5][0].astype(jnp.float32),
        whole[6][0].astype(jnp.float32),
        whole[7][0].astype(jnp.float32),
        whole[8][0],
        whole[9][0].reshape(-1).astype(jnp.float32),
        whole[10][0],
        whole[11][0].astype(jnp.float32),
    )


def forward(stream, params, rows):
    (
        gain_one,
        shift_one,
        qkv_mat,
        qv_shift,
        out_mat,
        out_shift,
        gain_two,
        shift_two,
        up_mat,
        up_shift,
        down_mat,
        down_shift,
    ) = params
    batch_size, seq_len, model_width = stream.shape
    head_count = qkv_mat.shape[2] // HD
    scale = HD ** (-0.5)
    normed, inverse = norm_parts(stream)
    lowered = (normed * gain_one + shift_one).astype(jnp.bfloat16)
    projected = jnp.einsum("bld,cde->cble", lowered, qkv_mat, preferred_element_type=jnp.float32)
    split_shape = (batch_size, seq_len, head_count, HD)
    queries = (projected[0] + qv_shift[0]).astype(jnp.bfloat16).reshape(split_shape)
    keys_low = projected[1].astype(jnp.bfloat16).reshape(split_shape)
    values_low = (projected[2] + qv_shift[1]).astype(jnp.bfloat16).reshape(split_shape)
    scores = (
        jnp.einsum("blhe,bmhe->bhlm", queries, keys_low, preferred_element_type=jnp.float32) * scale
    )
    row_max = jnp.max(scores, axis=-1, keepdims=True)
    log_total = row_max + jnp.log(jnp.sum(jnp.exp(scores - row_max), axis=-1, keepdims=True))
    attn_probs = jnp.exp(scores - log_total)
    mixed = jnp.einsum(
        "bhlm,bmhe->blhe",
        attn_probs.astype(jnp.bfloat16),
        values_low,
        preferred_element_type=jnp.float32,
    )
    mixed = mixed.astype(jnp.bfloat16).reshape(batch_size, seq_len, -1)
    partial_attn = jnp.einsum("bld,de->ble", mixed, out_mat, preferred_element_type=jnp.float32)
    middle = stream + both_halves(partial_attn) + out_shift
    normed_two, inverse_two = norm_parts(middle)
    lowered_two = (normed_two * gain_two + shift_two).astype(jnp.bfloat16)
    preact = (
        jnp.einsum("bld,df->blf", lowered_two, up_mat, preferred_element_type=jnp.float32)
        + up_shift
    )
    gelu_out = jax.nn.gelu(preact, approximate=False).astype(jnp.bfloat16)
    partial_mlp = jnp.einsum("blf,fd->bld", gelu_out, down_mat, preferred_element_type=jnp.float32)
    result = (middle + both_halves(partial_mlp) + down_shift) * rows
    return (result, (stream, middle, queries, keys_low, values_low, log_total, mixed, preact))


def backward(seed, saved, params, shapes):
    (
        gain_one,
        shift_one,
        qkv_mat,
        qv_shift,
        out_mat,
        out_shift,
        gain_two,
        shift_two,
        up_mat,
        up_shift,
        down_mat,
        down_shift,
    ) = params
    stream, middle, queries, keys_low, values_low, log_total, mixed, preact = saved
    batch_size, seq_len, head_count, head_dim = queries.shape
    scale = HD ** (-0.5)
    normed, inverse = norm_parts(stream)
    lowered = (normed * gain_one + shift_one).astype(jnp.bfloat16)
    normed_two, inverse_two = norm_parts(middle)
    lowered_two = (normed_two * gain_two + shift_two).astype(jnp.bfloat16)
    gelu_out = jax.nn.gelu(preact, approximate=False).astype(jnp.bfloat16)
    grad_mlp = seed.astype(jnp.bfloat16)
    grad_down_shift = jnp.sum(grad_mlp.astype(jnp.float32), axis=(0, 1))
    grad_down_mat = jnp.einsum(
        "blf,bld->fd", gelu_out, grad_mlp, preferred_element_type=jnp.float32
    )
    grad_gelu = jnp.einsum("bld,fd->blf", grad_mlp, down_mat, preferred_element_type=jnp.float32)
    grad_pre = (grad_gelu * gelu_slope(preact)).astype(jnp.bfloat16)
    grad_up_shift = jnp.sum(grad_pre.astype(jnp.float32), axis=(0, 1))
    grad_up_mat = jnp.einsum(
        "bld,blf->df", lowered_two, grad_pre, preferred_element_type=jnp.float32
    )
    grad_low_two = both_halves(
        jnp.einsum("blf,df->bld", grad_pre, up_mat, preferred_element_type=jnp.float32)
    )
    grad_gain_two = jnp.sum(grad_low_two * normed_two, axis=(0, 1))
    grad_shift_two = jnp.sum(grad_low_two, axis=(0, 1))
    grad_middle = seed + norm_back(grad_low_two * gain_two, normed_two, inverse_two)
    grad_attn = grad_middle.astype(jnp.bfloat16)
    grad_out_shift = jnp.sum(grad_attn.astype(jnp.float32), axis=(0, 1))
    grad_out_mat = jnp.einsum("bld,ble->de", mixed, grad_attn, preferred_element_type=jnp.float32)
    grad_mixed = jnp.einsum("ble,de->bld", grad_attn, out_mat, preferred_element_type=jnp.float32)
    grad_mixed = grad_mixed.astype(jnp.bfloat16).reshape(batch_size, seq_len, head_count, head_dim)
    scores = (
        jnp.einsum("blhe,bmhe->bhlm", queries, keys_low, preferred_element_type=jnp.float32) * scale
    )
    attn_probs = jnp.exp(scores - log_total)
    grad_probs = jnp.einsum(
        "blhe,bmhe->bhlm", grad_mixed, values_low, preferred_element_type=jnp.float32
    )
    grad_values = jnp.einsum(
        "bhlm,blhe->bmhe",
        attn_probs.astype(jnp.bfloat16),
        grad_mixed,
        preferred_element_type=jnp.float32,
    ).astype(jnp.bfloat16)
    grad_scores = (
        attn_probs * (grad_probs - jnp.sum(attn_probs * grad_probs, axis=-1, keepdims=True))
    ).astype(jnp.bfloat16)
    grad_queries = (
        jnp.einsum("bhlm,bmhe->blhe", grad_scores, keys_low, preferred_element_type=jnp.float32)
        * scale
    ).astype(jnp.bfloat16)
    grad_keys = (
        jnp.einsum("bhlm,blhe->bmhe", grad_scores, queries, preferred_element_type=jnp.float32)
        * scale
    ).astype(jnp.bfloat16)
    grad_proj = jnp.stack([grad_queries, grad_keys, grad_values]).reshape(
        3, batch_size, seq_len, -1
    )
    grad_qv_shift = jnp.stack(
        [
            jnp.sum(grad_queries.astype(jnp.float32), axis=(0, 1)),
            jnp.sum(grad_values.astype(jnp.float32), axis=(0, 1)),
        ]
    )
    grad_qkv_mat = jnp.einsum(
        "bld,cble->cde", lowered, grad_proj, preferred_element_type=jnp.float32
    )
    grad_lowered = both_halves(
        jnp.einsum("cble,cde->bld", grad_proj, qkv_mat, preferred_element_type=jnp.float32)
    )
    grad_gain_one = jnp.sum(grad_lowered * normed, axis=(0, 1))
    grad_shift_one = jnp.sum(grad_lowered, axis=(0, 1))
    grad_stream = grad_middle + norm_back(grad_lowered * gain_one, normed, inverse)
    terms = [
        grad_gain_one,
        grad_shift_one,
        grad_qkv_mat,
        grad_qv_shift,
        grad_out_mat,
        grad_out_shift,
        grad_gain_two,
        grad_shift_two,
        grad_up_mat,
        grad_up_shift,
        grad_down_mat,
        grad_down_shift,
    ]
    return (grad_stream, [term.reshape(shape) for term, shape in zip(terms, shapes)])


def local(
    images,
    cotangent,
    live_count,
    ln1_gain,
    ln1_bias,
    qkv_weight,
    qv_bias,
    out_weight,
    out_bias,
    ln2_gain,
    ln2_bias,
    up_weight,
    up_bias,
    down_weight,
    down_bias,
):
    first_section = lax.axis_index("section") == 0
    micro_count = images.shape[0]
    slot_count = images.shape[1]
    slot_ids = jnp.arange(slot_count)
    small = (ln1_gain, ln1_bias, qv_bias, out_bias, ln2_gain, ln2_bias, up_bias, down_bias)
    gathered = gather_all(small, (qkv_weight, out_weight, up_weight, down_weight))
    params = unpack_weights(gathered)
    shapes = [piece.shape for piece in gathered]

    def row_mask(batch_index, valid):
        alive = jnp.logical_and(slot_ids < live_count[batch_index, 0], valid)
        return alive.astype(jnp.float32).reshape(slot_count, 1, 1)

    def choose(for_first, for_second):
        return jnp.where(first_section, for_first, for_second)

    incoming = jnp.zeros(images.shape[1:], jnp.bfloat16)
    outputs = []
    kept = []
    for moment in range(micro_count + 1):
        own = images[min(moment, micro_count - 1)]
        source = choose(own, incoming).astype(jnp.float32)
        rows = choose(
            row_mask(min(moment, micro_count - 1), moment < micro_count),
            row_mask(max(moment - 1, 0), moment >= 1),
        )
        result, saved = forward(source, params, rows)
        result = result.astype(jnp.bfloat16)
        outputs.append(result)
        kept.append(saved)
        if moment < micro_count:
            incoming = from_behind(result, "section", 1)
    activations = jnp.stack(
        [choose(outputs[index], outputs[index + 1]) for index in range(micro_count)]
    )
    totals = [jnp.zeros(shape, jnp.float32) for shape in shapes]
    incoming = jnp.zeros(images.shape[1:], jnp.bfloat16)
    returned = []
    for moment in range(micro_count + 1):
        later_index = min(moment, micro_count - 1)
        rows = choose(
            row_mask(max(moment - 1, 0), moment >= 1), row_mask(later_index, moment < micro_count)
        )
        seed = choose(incoming, cotangent[later_index]).astype(jnp.float32) * rows
        saved = jax.tree.map(choose, kept[max(moment - 1, 0)], kept[min(moment + 1, micro_count)])
        grad_stream, terms = backward(seed, saved, params, shapes)
        grad_low = grad_stream.astype(jnp.bfloat16)
        returned.append(grad_low)
        if moment < micro_count:
            incoming = from_behind(grad_low, "section", -1)
        totals = [first_part + second_part for first_part, second_part in zip(totals, terms)]
    shards = (
        ln1_gain,
        ln1_bias,
        qkv_weight,
        qv_bias,
        out_weight,
        out_bias,
        ln2_gain,
        ln2_bias,
        up_weight,
        up_bias,
        down_weight,
        down_bias,
    )
    owned = scatter_all(totals, shards)
    input_grads = jnp.stack(
        [choose(returned[index + 1], returned[index]) for index in range(micro_count)]
    )
    return (
        activations[None],
        input_grads[None],
        owned[0],
        owned[1],
        owned[2],
        owned[3],
        owned[4],
        owned[5],
        owned[6],
        owned[7],
        owned[8],
        owned[9],
        owned[10],
        owned[11],
    )


def solution(mesh):
    return jax.shard_map(
        local,
        mesh=mesh,
        in_specs=(
            P(None, "dp", None, None),
            P(None, "dp", None, None),
            P(None, "dp"),
            P("section", "dp"),
            P("section", "dp"),
            P("section", None, "dp", "mp"),
            P("section", None, "mp", "dp"),
            P("section", "mp", "dp"),
            P("section", "dp"),
            P("section", "dp"),
            P("section", "dp"),
            P("section", "dp", "mp"),
            P("section", "mp", "dp"),
            P("section", "mp", "dp"),
            P("section", "dp"),
        ),
        out_specs=(
            P("section", None, "dp", None, None),
            P("section", None, "dp", None, None),
            P("section", "dp"),
            P("section", "dp"),
            P("section", None, "dp", "mp"),
            P("section", None, "mp", "dp"),
            P("section", "mp", "dp"),
            P("section", "dp"),
            P("section", "dp"),
            P("section", "dp"),
            P("section", "dp", "mp"),
            P("section", "mp", "dp"),
            P("section", "mp", "dp"),
            P("section", "dp"),
        ),
        check_vma=False,
    )
```

```python
import functools
import heapq
import math

import jax
import jax.numpy as jnp
from jax import lax
from jax.experimental import pallas as pl
from jax.experimental.pallas import tpu as pltpu
from jax.sharding import PartitionSpec as P

HD = 64


epsilon = 1e-06


def gather_all(small, big):
    flat = jnp.concatenate([piece.reshape(-1) for piece in small])
    packed = lax.all_gather(flat, "dp", axis=0, tiled=False)
    count = packed.shape[0]
    whole, offset = [], 0
    for piece, axis in zip(small, (1, 1, 3, 1, 1, 1, 2, 1)):
        part = packed[:, offset : offset + piece.size].reshape((count,) + piece.shape)
        offset += piece.size
        part = jnp.moveaxis(part, 0, axis)
        shape = list(piece.shape)
        shape[axis] *= count
        whole.append(part.reshape(shape))
    qkv, out, up, down = (
        lax.all_gather(piece, "dp", axis=axis, tiled=True) for piece, axis in zip(big, (2, 2, 1, 2))
    )
    return (
        whole[0],
        whole[1],
        qkv,
        whole[2],
        out,
        whole[3],
        whole[4],
        whole[5],
        up,
        whole[6],
        down,
        whole[7],
    )


def scatter_all(totals, shards):
    small_at = (0, 1, 3, 5, 6, 7, 9, 11)
    count = lax.axis_size("dp")
    rows = []
    for index, axis in zip(small_at, (1, 1, 3, 1, 1, 1, 2, 1)):
        piece = totals[index]
        shape = list(piece.shape)
        shape[axis : axis + 1] = [count, shape[axis] // count]
        rows.append(jnp.moveaxis(piece.reshape(shape), axis, 0).reshape(count, -1))
    packed = lax.psum_scatter(jnp.concatenate(rows, axis=1), "dp", scatter_dimension=0, tiled=False)
    owned, offset = [None] * 12, 0
    for index in small_at:
        size = shards[index].size
        owned[index] = packed[offset : offset + size].reshape(shards[index].shape)
        offset += size
    for index, axis in zip((2, 4, 8, 10), (2, 2, 1, 2)):
        owned[index] = lax.psum_scatter(
            totals[index].astype(jnp.bfloat16), "dp", scatter_dimension=axis, tiled=True
        ).astype(jnp.float32)
    return owned


def both_halves(partial):
    return lax.psum(partial.astype(jnp.bfloat16), "mp").astype(jnp.float32)


def from_behind(x, axis, by):
    length = lax.axis_size(axis)
    pairs = [(i, i + by) for i in range(length) if 0 <= i + by < length]
    return lax.ppermute(x, axis, pairs)


def norm_parts(stream):
    centered = stream - jnp.mean(stream, axis=-1, keepdims=True)
    inverse = lax.rsqrt(jnp.mean(centered * centered, axis=-1, keepdims=True) + epsilon)
    return (centered * inverse, inverse)


def norm_back(grad_normed, normed, inverse):
    first_mean = jnp.mean(grad_normed, axis=-1, keepdims=True)
    second_mean = jnp.mean(grad_normed * normed, axis=-1, keepdims=True)
    return inverse * (grad_normed - first_mean - normed * second_mean)


def gelu_slope(preact):
    cumul = 0.5 * (1.0 + lax.erf(preact * 2.0 ** (-0.5)))
    density = jnp.exp(-0.5 * preact * preact) * (2.0 * math.pi) ** (-0.5)
    return cumul + preact * density


def unpack_weights(whole):
    return (
        whole[0][0].astype(jnp.float32),
        whole[1][0].astype(jnp.float32),
        whole[2][0],
        whole[3][0].reshape(2, -1).astype(jnp.float32),
        whole[4][0],
        whole[5][0].astype(jnp.float32),
        whole[6][0].astype(jnp.float32),
        whole[7][0].astype(jnp.float32),
        whole[8][0],
        whole[9][0].reshape(-1).astype(jnp.float32),
        whole[10][0],
        whole[11][0].astype(jnp.float32),
    )


def forward(stream, params, rows):
    (
        gain_one,
        shift_one,
        qkv_mat,
        qv_shift,
        out_mat,
        out_shift,
        gain_two,
        shift_two,
        up_mat,
        up_shift,
        down_mat,
        down_shift,
    ) = params
    batch_size, seq_len, model_width = stream.shape
    head_count = qkv_mat.shape[2] // HD
    scale = HD ** (-0.5)
    normed, inverse = norm_parts(stream)
    lowered = (normed * gain_one + shift_one).astype(jnp.bfloat16)
    projected = jnp.einsum("bld,cde->cble", lowered, qkv_mat, preferred_element_type=jnp.float32)
    split_shape = (batch_size, seq_len, head_count, HD)
    queries = (projected[0] + qv_shift[0]).astype(jnp.bfloat16).reshape(split_shape)
    keys_low = projected[1].astype(jnp.bfloat16).reshape(split_shape)
    values_low = (projected[2] + qv_shift[1]).astype(jnp.bfloat16).reshape(split_shape)
    scores = (
        jnp.einsum("blhe,bmhe->bhlm", queries, keys_low, preferred_element_type=jnp.float32) * scale
    )
    row_max = jnp.max(scores, axis=-1, keepdims=True)
    log_total = row_max + jnp.log(jnp.sum(jnp.exp(scores - row_max), axis=-1, keepdims=True))
    attn_probs = jnp.exp(scores - log_total)
    mixed = jnp.einsum(
        "bhlm,bmhe->blhe",
        attn_probs.astype(jnp.bfloat16),
        values_low,
        preferred_element_type=jnp.float32,
    )
    mixed = mixed.astype(jnp.bfloat16).reshape(batch_size, seq_len, -1)
    partial_attn = jnp.einsum("bld,de->ble", mixed, out_mat, preferred_element_type=jnp.float32)
    middle = stream + both_halves(partial_attn) + out_shift
    normed_two, inverse_two = norm_parts(middle)
    lowered_two = (normed_two * gain_two + shift_two).astype(jnp.bfloat16)
    preact = (
        jnp.einsum("bld,df->blf", lowered_two, up_mat, preferred_element_type=jnp.float32)
        + up_shift
    )
    gelu_out = jax.nn.gelu(preact, approximate=False).astype(jnp.bfloat16)
    partial_mlp = jnp.einsum("blf,fd->bld", gelu_out, down_mat, preferred_element_type=jnp.float32)
    result = (middle + both_halves(partial_mlp) + down_shift) * rows
    return (result, (stream, middle, queries, keys_low, values_low, log_total, mixed, preact))


def backward(seed, saved, params, shapes):
    (
        gain_one,
        shift_one,
        qkv_mat,
        qv_shift,
        out_mat,
        out_shift,
        gain_two,
        shift_two,
        up_mat,
        up_shift,
        down_mat,
        down_shift,
    ) = params
    stream, middle, queries, keys_low, values_low, log_total, mixed, preact = saved
    batch_size, seq_len, head_count, head_dim = queries.shape
    scale = HD ** (-0.5)
    normed, inverse = norm_parts(stream)
    lowered = (normed * gain_one + shift_one).astype(jnp.bfloat16)
    normed_two, inverse_two = norm_parts(middle)
    lowered_two = (normed_two * gain_two + shift_two).astype(jnp.bfloat16)
    gelu_out = jax.nn.gelu(preact, approximate=False).astype(jnp.bfloat16)
    grad_mlp = seed.astype(jnp.bfloat16)
    grad_down_shift = jnp.sum(grad_mlp.astype(jnp.float32), axis=(0, 1))
    grad_down_mat = jnp.einsum(
        "blf,bld->fd", gelu_out, grad_mlp, preferred_element_type=jnp.float32
    )
    grad_gelu = jnp.einsum("bld,fd->blf", grad_mlp, down_mat, preferred_element_type=jnp.float32)
    grad_pre = (grad_gelu * gelu_slope(preact)).astype(jnp.bfloat16)
    grad_up_shift = jnp.sum(grad_pre.astype(jnp.float32), axis=(0, 1))
    grad_up_mat = jnp.einsum(
        "bld,blf->df", lowered_two, grad_pre, preferred_element_type=jnp.float32
    )
    grad_low_two = both_halves(
        jnp.einsum("blf,df->bld", grad_pre, up_mat, preferred_element_type=jnp.float32)
    )
    grad_gain_two = jnp.sum(grad_low_two * normed_two, axis=(0, 1))
    grad_shift_two = jnp.sum(grad_low_two, axis=(0, 1))
    grad_middle = seed + norm_back(grad_low_two * gain_two, normed_two, inverse_two)
    grad_attn = grad_middle.astype(jnp.bfloat16)
    grad_out_shift = jnp.sum(grad_attn.astype(jnp.float32), axis=(0, 1))
    grad_out_mat = jnp.einsum("bld,ble->de", mixed, grad_attn, preferred_element_type=jnp.float32)
    grad_mixed = jnp.einsum("ble,de->bld", grad_attn, out_mat, preferred_element_type=jnp.float32)
    grad_mixed = grad_mixed.astype(jnp.bfloat16).reshape(batch_size, seq_len, head_count, head_dim)
    scores = (
        jnp.einsum("blhe,bmhe->bhlm", queries, keys_low, preferred_element_type=jnp.float32) * scale
    )
    attn_probs = jnp.exp(scores - log_total)
    grad_probs = jnp.einsum(
        "blhe,bmhe->bhlm", grad_mixed, values_low, preferred_element_type=jnp.float32
    )
    grad_values = jnp.einsum(
        "bhlm,blhe->bmhe",
        attn_probs.astype(jnp.bfloat16),
        grad_mixed,
        preferred_element_type=jnp.float32,
    ).astype(jnp.bfloat16)
    grad_scores = (
        attn_probs * (grad_probs - jnp.sum(attn_probs * grad_probs, axis=-1, keepdims=True))
    ).astype(jnp.bfloat16)
    grad_queries = (
        jnp.einsum("bhlm,bmhe->blhe", grad_scores, keys_low, preferred_element_type=jnp.float32)
        * scale
    ).astype(jnp.bfloat16)
    grad_keys = (
        jnp.einsum("bhlm,blhe->bmhe", grad_scores, queries, preferred_element_type=jnp.float32)
        * scale
    ).astype(jnp.bfloat16)
    grad_proj = jnp.stack([grad_queries, grad_keys, grad_values]).reshape(
        3, batch_size, seq_len, -1
    )
    grad_qv_shift = jnp.stack(
        [
            jnp.sum(grad_queries.astype(jnp.float32), axis=(0, 1)),
            jnp.sum(grad_values.astype(jnp.float32), axis=(0, 1)),
        ]
    )
    grad_qkv_mat = jnp.einsum(
        "bld,cble->cde", lowered, grad_proj, preferred_element_type=jnp.float32
    )
    grad_lowered = both_halves(
        jnp.einsum("cble,cde->bld", grad_proj, qkv_mat, preferred_element_type=jnp.float32)
    )
    grad_gain_one = jnp.sum(grad_lowered * normed, axis=(0, 1))
    grad_shift_one = jnp.sum(grad_lowered, axis=(0, 1))
    grad_stream = grad_middle + norm_back(grad_lowered * gain_one, normed, inverse)
    terms = [
        grad_gain_one,
        grad_shift_one,
        grad_qkv_mat,
        grad_qv_shift,
        grad_out_mat,
        grad_out_shift,
        grad_gain_two,
        grad_shift_two,
        grad_up_mat,
        grad_up_shift,
        grad_down_mat,
        grad_down_shift,
    ]
    return (grad_stream, [term.reshape(shape) for term, shape in zip(terms, shapes)])


def local(
    images,
    cotangent,
    live_count,
    ln1_gain,
    ln1_bias,
    qkv_weight,
    qv_bias,
    out_weight,
    out_bias,
    ln2_gain,
    ln2_bias,
    up_weight,
    up_bias,
    down_weight,
    down_bias,
):
    first_section = lax.axis_index("section") == 0
    micro_count = images.shape[0]
    slot_count = images.shape[1]
    slot_ids = jnp.arange(slot_count)
    small = (ln1_gain, ln1_bias, qv_bias, out_bias, ln2_gain, ln2_bias, up_bias, down_bias)
    gathered = gather_all(small, (qkv_weight, out_weight, up_weight, down_weight))
    params = unpack_weights(gathered)
    shapes = [piece.shape for piece in gathered]

    def row_mask(batch_index, valid):
        alive = jnp.logical_and(slot_ids < live_count[batch_index, 0], valid)
        return alive.astype(jnp.float32).reshape(slot_count, 1, 1)

    def choose(for_first, for_second):
        return jnp.where(first_section, for_first, for_second)

    incoming = jnp.zeros(images.shape[1:], jnp.bfloat16)
    outputs = []
    kept = []
    for moment in range(micro_count + 1):
        own = images[min(moment, micro_count - 1)]
        source = choose(own, incoming).astype(jnp.float32)
        rows = choose(
            row_mask(min(moment, micro_count - 1), moment < micro_count),
            row_mask(max(moment - 1, 0), moment >= 1),
        )
        result, saved = forward(source, params, rows)
        result = result.astype(jnp.bfloat16)
        outputs.append(result)
        kept.append(saved)
        if moment < micro_count:
            incoming = from_behind(result, "section", 1)
    activations = jnp.stack(
        [choose(outputs[index], outputs[index + 1]) for index in range(micro_count)]
    )
    totals = [jnp.zeros(shape, jnp.float32) for shape in shapes]
    incoming = jnp.zeros(images.shape[1:], jnp.bfloat16)
    returned = []
    for moment in range(micro_count + 1):
        later_index = min(moment, micro_count - 1)
        rows = choose(
            row_mask(max(moment - 1, 0), moment >= 1), row_mask(later_index, moment < micro_count)
        )
        seed = choose(incoming, cotangent[later_index]).astype(jnp.float32) * rows
        saved = jax.tree.map(choose, kept[max(moment - 1, 0)], kept[min(moment + 1, micro_count)])
        grad_stream, terms = backward(seed, saved, params, shapes)
        grad_low = grad_stream.astype(jnp.bfloat16)
        returned.append(grad_low)
        if moment < micro_count:
            incoming = from_behind(grad_low, "section", -1)
        totals = [first_part + second_part for first_part, second_part in zip(totals, terms)]
    shards = (
        ln1_gain,
        ln1_bias,
        qkv_weight,
        qv_bias,
        out_weight,
        out_bias,
        ln2_gain,
        ln2_bias,
        up_weight,
        up_bias,
        down_weight,
        down_bias,
    )
    owned = scatter_all(totals, shards)
    input_grads = jnp.stack(
        [choose(returned[index + 1], returned[index]) for index in range(micro_count)]
    )
    return (
        activations[None],
        input_grads[None],
        owned[0],
        owned[1],
        owned[2],
        owned[3],
        owned[4],
        owned[5],
        owned[6],
        owned[7],
        owned[8],
        owned[9],
        owned[10],
        owned[11],
    )


MESH = pl.DeviceIdType.MESH
BF = jnp.bfloat16
F32 = jnp.float32
Z = 4
EPS = 1e-06
L = 197
LP = 208
R = 2 * LP
SMALL, Q, K, V, OUT, UP, DOWN = range(7)
MATS = (Q, K, V, OUT, UP, DOWN)
BY_ROWS = (Q, K, V, UP)
X_FIRST = (K, OUT)
WIDTH = {Q: 512, K: 512, V: 512, OUT: 512, UP: 2048, DOWN: 2048}
SELF, NEAR, INNER, FAR = range(4)


class Clock:
    def __init__(self):
        self.now, self.queue, self.count = 0.0, [], 0

    def add(self, ready, step, cost=0.2):
        heapq.heappush(self.queue, (ready, self.count, cost, step))
        self.count += 1

    def pop(self):
        ready, _, cost, step = heapq.heappop(self.queue)
        self.now = max(self.now, ready)
        step()
        self.now += cost

    def flush(self, until):
        while self.queue and self.queue[0][0] <= until:
            self.pop()

    def run(self, cost, step, *args):
        self.flush(self.now)
        step(*args)
        self.now += cost

    def wait(self, until, step, *args):
        self.flush(until)
        self.now = max(self.now, until)
        step(*args)

    def drain(self, done):
        while not done():
            self.pop()


def lanes(d, n=128):
    return pl.ds(pl.multiple_of(d * 128, 128), n)


def dot(a, b, ca, cb):
    return lax.dot_general(a, b, (((ca,), (cb,)), ((), ())), preferred_element_type=F32)


def half(m, ref, s, h):
    n = WIDTH[m] // 2
    at = pl.ds(pl.multiple_of(h * n, n), n)
    return ref.at[s, :, at] if m in BY_ROWS else ref.at[s, at, :]


def block(m, ref, s, d, h=None):
    if m == SMALL:
        return ref.at[s, d] if h is None else ref.at[s, d, pl.ds(h * 16, 16), :]
    own = pl.ds(pl.multiple_of(d * 128, 128), 128)
    n = WIDTH[m] // 2
    other = pl.ds(0, 2 * n) if h is None else pl.ds(pl.multiple_of(h * n, n), n)
    return ref.at[s, own, other] if m in BY_ROWS else ref.at[s, other, own]


def kernel(
    small_ref, qkv_ref, out_ref, up_ref, down_ref, x_ref, cot_ref, live_ref,
    act_out, gin_out, gqkv_out, gout_out, gup_out, gdown_out, gvec_out,
    wsmall, wq, wk, wv, wout, wup, wdown,
    rq, rk, rv, rout, rup, rdown, xq, xk, xv, xout, xup, xdown,
    zq, zk, zv, zout, zup, zdown, fq, fk, fv, fout, fup, fdown,
    xs, qkvs, mixs, nrm2s, gels, slps, inv2s,
    low, mid, gb, gpre, gqkv, ys, yr, acc, vec, sv, svc, svx, svz,
    asem_s, asem_c, asem_z, asem_x, rsem_cs, rsem_c, rsem_xs, rsem_x, rsem_zs, rsem_z, rsem_fs, rsem_f,
    ysem, ysem_s, osem, osem_r, osem_s, isem, vsem, vsem_s, free_c, free_x, free_z,
):
    shards = (small_ref, qkv_ref.at[0], qkv_ref.at[1], qkv_ref.at[2], out_ref, up_ref, down_ref)
    wqkv = (wq, wk, wv)
    w = (wsmall, wq, wk, wv, wout, wup, wdown)
    rbuf = (None, rq, rk, rv, rout, rup, rdown)
    xbuf = (None, xq, xk, xv, xout, xup, xdown)
    zbuf = (None, zq, zk, zv, zout, zup, zdown)
    fbuf = (None, fq, fk, fv, fout, fup, fdown)

    c = lax.axis_index("section")
    me = lax.axis_index("dp")
    y = lax.axis_index("mp")
    z, x = me // 2, lax.rem(me, 2)
    to_x = {"dp": z * 2 + 1 - x}
    to_c = {"section": 1 - c}
    to_y = {"mp": 1 - y}

    inner = jnp.logical_or(z == 1, z == 2)
    near = z + 1 - 2 * lax.rem(z, 2)
    lower = (z < 2).astype(jnp.int32)
    places = (z, near, 1 + lower, 3 * lower)
    inner_i = jnp.where(inner, 1, 0)

    def at_dp(k, col):
        return places[k] * 2 + (x if col == 0 else 1 - x)

    def to_z(zi):
        return {"dp": zi * 2 + x}

    def remote(a, b, ss, rs, dev):
        return pltpu.make_async_remote_copy(
            src_ref=a, dst_ref=b, send_sem=ss, recv_sem=rs, device_id=dev, device_id_type=MESH
        )

    barrier = pltpu.get_barrier_semaphore()
    for dev in [to_z(places[k]) for k in (NEAR, INNER, FAR)] + [to_x, to_c, to_y]:
        pl.semaphore_signal(barrier, inc=1, device_id=dev, device_id_type=MESH)
    pl.semaphore_wait(barrier, Z + 2)

    def number(per):
        table = {}
        for key, count in per:
            for i in range(count):
                table[key, i] = len(table)
        return table

    pieces = [(s, m) for s in range(2) for m in range(7)]
    az = number((p, 6 if p[1] in X_FIRST else 3) for p in pieces)
    ax = number((p, 1 if p[1] in X_FIRST else 4) for p in pieces)
    rz = number((p, 8 if p[1] in X_FIRST else 4) for p in pieces if p[1])
    rx = number((p, 1 if p[1] in X_FIRST else 4) for p in pieces if p[1])

    def wait_bytes(m, count, sem):
        if m == SMALL:
            v = inv2s.at[0, pl.ds(0, 8 * count), :]
        else:
            v = wdown.at[:, pl.ds(0, count * WIDTH[m] // 32), :]
        pltpu.make_async_copy(v, v, sem).wait()

    def ag_share(s, m):
        p = s * 7 + m

        @pl.when(c == s)
        def _():
            dst = block(m, w[m], s, me)
            remote(shards[m], dst, asem_s.at[p], asem_c.at[p, 0], to_c).start()
            pltpu.make_async_copy(shards[m], dst, asem_c.at[p, 0]).start()

    def ag_shared(s, m):
        whole = block(m, w[m], s, me)
        pltpu.make_async_copy(whole, whole, asem_c.at[s * 7 + m, 0]).wait()

    def ag_own_z(s, m, col):
        p, first = s * 7 + m, az[(s, m), col * 3]
        b = block(m, w[m], s, at_dp(SELF, col), c)
        slot = jnp.where(inner, INNER, FAR) - 1
        remote(b, b, asem_s.at[p], asem_z.at[first], to_z(near)).start()
        remote(b, b, asem_s.at[p], asem_z.at[first + slot], to_z(places[INNER])).start()

    def ag_to_x(s, m, k):
        b = block(m, w[m], s, at_dp(k, 0), c)
        remote(b, b, asem_s.at[s * 7 + m], asem_x.at[ax[(s, m), k]], to_x).start()

    def ag_to_c(s, m, k, col):
        p = s * 7 + m
        b = block(m, w[m], s, at_dp(k, col), c)
        remote(b, b, asem_s.at[p], asem_c.at[p, 1], to_c).start()

    def ag_z(s, m, k, col):
        b = block(m, w[m], s, at_dp(k, col), c)
        cp = remote(b, b, asem_s.at[s * 7 + m], asem_z.at[az[(s, m), col * 3 + k - 1]], to_z(near))
        cp.wait_recv()
        if k != NEAR:

            @pl.when(inner)
            def _():
                cp.start()

        if m not in X_FIRST:
            ag_to_x(s, m, k)
        ag_to_c(s, m, k, col)

    def ag_x(s, m, k):
        b = block(m, w[m], s, at_dp(k, 1), c)
        remote(b, b, asem_s.at[s * 7 + m], asem_x.at[ax[(s, m), k]], to_x).wait_recv()
        if m in X_FIRST:
            ag_own_z(s, m, 1)
        ag_to_c(s, m, k, 1)

    def ag_need(s, m):
        wait_bytes(m, 7, asem_c.at[s * 7 + m, 1])

    def ag_sent(s, m):
        count = 7 + (1 + 4 if m in X_FIRST else 4 + 2)
        extra = 4 if m in X_FIRST else 2
        for ins in range(2):
            for own in range(2):

                @pl.when(jnp.logical_and(inner_i == ins, jnp.where(c == s, 1, 0) == own))
                def _():
                    wait_bytes(m, count + extra * ins + 2 * own, asem_s.at[s * 7 + m])

    def rows_of(b):
        return pl.ds(b * LP, LP)

    def y_src(k):
        return slps.at[1, :, pl.ds(0, 1024)] if k == 7 else ys

    def y_start(k, b, n):
        cols = lanes(n * 2, 256)
        src = y_src(k).at[rows_of(b), cols]
        remote(src, yr.at[k % 2, rows_of(b), cols], ysem_s.at[k * 2 + b], ysem.at[k * 2 + b], to_y).start()

    def y_wait(k, b):
        src = y_src(k).at[rows_of(b), pl.ds(0, 1024)]
        cp = remote(src, yr.at[k % 2, rows_of(b), :], ysem_s.at[k * 2 + b], ysem.at[k * 2 + b], to_y)
        cp.wait_recv()
        cp.wait_send()

    def y_sum(k, rows):
        return y_src(k)[rows, :].astype(F32) + yr[k % 2, rows, :].astype(F32)

    def unpack_small(s):
        total = jnp.zeros((32, 128), F32)
        for d in range(2 * Z):
            piece = wsmall[s, d].astype(F32)
            total = total + piece
            for r in range(6):
                vec[s, r : r + 1, d * 128 : d * 128 + 128] = piece[r : r + 1, :]
        for k in range(8):
            vec[s, 6:7, k * 128 : k * 128 + 128] = total[6 + k : 7 + k, :]
            vec[s, 7:8, k * 128 : k * 128 + 128] = total[14 + k : 15 + k, :]
            vec[s, 8:9, k * 128 : k * 128 + 128] = total[22 + k : 23 + k, :]

    def row(s, r):
        return vec[s, r : r + 1, :]

    CH = 16

    def norm_chunk(v):
        mean = jnp.mean(v, axis=-1, keepdims=True)
        cen = v - mean
        inv = lax.rsqrt(jnp.mean(cen * cen, axis=-1, keepdims=True) + EPS)
        return cen * inv, inv

    def chunks(b):
        def wrap(body):
            @pl.loop(0, LP // CH)
            def _(i):
                body(pl.ds(pl.multiple_of(b * LP + i * CH, CH), CH))

        return wrap

    def ln1(s, b):
        gain, shift = row(s, 0), row(s, 1)

        @chunks(b)
        def _(rows):
            nrm, _ = norm_chunk(xs[s, rows, :].astype(F32))
            low[rows, :] = (nrm * gain + shift).astype(BF)

    def unweave(src, dst, b, alive):
        r = lax.broadcasted_iota(jnp.int32, (LP, R), 0)
        q = lax.broadcasted_iota(jnp.int32, (LP, R), 1)
        take = jnp.where(q == 2 * r + b, 1.0, 0.0)
        if alive is not None:
            take = take * alive
        take = take.astype(BF)

        @pl.loop(0, 4)
        def _(n):
            cols = lanes(n * 2, 256)
            dst[rows_of(b), cols] = dot(take, src[:, cols], 1, 0).astype(BF)

    def alive_of(b):
        return jnp.where(live_ref[c, 0] > b, 1.0, 0.0)

    def project(s, b):
        for t in range(3):
            @pl.loop(0, 2)
            def _(n):
                cols = lanes(n * 2, 256)
                a = dot(low[rows_of(b), :], wqkv[t][s, :, cols], 1, 0)
                if t != 1:
                    base = 0 if t == 0 else 512
                    a = a + vec[s, 6:7, pl.ds(pl.multiple_of(base + n * 256, 256), 256)]
                qkvs[s, t, rows_of(b), cols] = a.astype(BF)

    left = lax.broadcasted_iota(jnp.int32, (1, 128), 1) < 64
    live_col = lax.broadcasted_iota(jnp.int32, (1, LP), 1) < L

    def pick(h, v):
        return jnp.where(left if h == 0 else jnp.logical_not(left), v, jnp.zeros_like(v))

    def softmax(q, k):
        sc = dot(q, k, 1, 1) * (64.0 ** -0.5)
        sc = jnp.where(live_col, sc, -1e30)
        top = jnp.max(sc, axis=-1, keepdims=True)
        e = jnp.exp(sc - top)
        return e * (1.0 / jnp.sum(e, axis=-1, keepdims=True))

    def attention(s, b):
        rows = rows_of(b)

        @pl.loop(0, 4)
        def _(i):
            cols = lanes(i)
            q, k, v = (qkvs[s, t, rows, cols] for t in range(3))
            parts = [dot(softmax(pick(h, q), k).astype(BF), v, 1, 0) for h in range(2)]
            mixs[s, rows, cols] = jnp.where(left, parts[0], parts[1]).astype(BF)

    def out_project(s, b, k):
        @pl.loop(0, 4)
        def _(n):
            cols = lanes(n * 2, 256)
            ys[rows_of(b), cols] = dot(mixs[s, rows_of(b), :], wout[s, :, cols], 1, 0).astype(BF)
            y_start(k, b, n)

    def middle(s, b, k):
        shift, gain2, shift2 = row(s, 2), row(s, 3), row(s, 4)

        @chunks(b)
        def _(rows):
            v = xs[s, rows, :].astype(F32) + y_sum(k, rows) + shift
            if s == 0:
                mid[rows, :] = v
            else:
                gb[0, rows, :] = v.astype(BF)
            nrm, inv = norm_chunk(v)
            nrm2s[s, rows, :] = nrm.astype(BF)
            inv2s[s, rows, :] = jnp.broadcast_to(inv, (CH, 128))
            low[rows, :] = (nrm * gain2 + shift2).astype(BF)

    def up_project(s, b):
        @pl.loop(0, 8)
        def _(n):
            cols = lanes(n * 2, 256)
            acc[...] = dot(low[rows_of(b), :], wup[s, :, cols], 1, 0)
            at = pl.ds(pl.multiple_of(lax.rem(n, 4) * 256, 256), 256)
            bias = jnp.where(n < 4, vec[s, 7:8, at], vec[s, 8:9, at])

            @pl.loop(0, LP // 16)
            def _(i):
                rows = pl.ds(pl.multiple_of(b * LP + i * 16, 16), 16)
                a = acc[pl.ds(pl.multiple_of(i * 16, 16), 16), :] + bias
                phi = 0.5 * (1.0 + lax.erf(a * (2.0 ** -0.5)))
                dens = jnp.exp(-0.5 * a * a) * ((2.0 * math.pi) ** -0.5)
                gels[s, rows, cols] = (a * phi).astype(BF)
                slps[s, rows, cols] = (phi + a * dens).astype(BF)

    def down_project(s, b, k, send):
        @pl.loop(0, 4)
        def _(n):
            cols = lanes(n * 2, 256)
            y_src(k)[rows_of(b), cols] = dot(gels[s, rows_of(b), :], wdown[s, :, cols], 1, 0).astype(BF)
            if send:
                y_start(k, b, n)

    def finish(s, b, k, dst):
        shift, alive = row(s, 5), alive_of(b)

        @chunks(b)
        def _(rows):
            base = mid[rows, :] if s == 0 else slps[1, rows, 1024:2048].astype(F32)
            dst[rows, :] = ((base + y_sum(k, rows) + shift) * alive).astype(BF)

    def keep_middle(b):
        @chunks(b)
        def _(rows):
            slps[1, rows, 1024:2048] = gb[0, rows, :]

    def emit(which, s, src):
        target = (act_out, gin_out)[which].at[c]
        q = which * 2 + s

        @pl.when(c == s)
        def _():
            pltpu.make_async_copy(src, target, osem.at[q]).start()

        @pl.when(c != s)
        def _():
            remote(src, target, osem_s.at[q], osem_r.at[q], to_c).start()

    def emit_sent(which, s, src):
        target = (act_out, gin_out)[which].at[c]
        q = which * 2 + s

        @pl.when(c == s)
        def _():
            pltpu.make_async_copy(src, target, osem.at[q]).wait()

        @pl.when(c != s)
        def _():
            remote(src, target, osem_s.at[q], osem_r.at[q], to_c).wait_send()

    def emit_got(which, s, src):
        target = (act_out, gin_out)[which].at[1 - c]
        q = which * 2 + s

        @pl.when(c == s)
        def _():
            remote(src, target, osem_s.at[q], osem_r.at[q], to_c).wait_recv()

    def relower(s, b):
        gain2, shift2 = row(s, 3), row(s, 4)

        @chunks(b)
        def _(rows):
            low[rows, :] = (nrm2s[s, rows, :].astype(F32) * gain2 + shift2).astype(BF)

    def colsum(v):
        return jnp.sum(v, axis=0, keepdims=True)

    def sum_rows(ref_slice, width):
        def step(i, tot):
            rows = pl.ds(pl.multiple_of(i * CH, CH), CH)
            return tot + colsum(ref_slice(rows).astype(F32))

        return lax.fori_loop(0, R // CH, step, jnp.zeros((1, width), F32))

    def total(s, r, b, v):
        sv[s, r : r + 1, :] = v if b == 0 else sv[s, r : r + 1, :] + v

    def grad_gelu(s, b):
        @pl.loop(0, 8)
        def _(n):
            cols = lanes(n * 2, 256)
            rows_w = pl.ds(pl.multiple_of(n * 256, 256), 256)
            a = dot(gb[s, rows_of(b), :], wdown[s, rows_w, :], 1, 1)
            gpre[rows_of(b), cols] = (a * slps[s, rows_of(b), cols].astype(F32)).astype(BF)

    def grad_mlp_biases(s):
        sv[s, 5:6, :] = sum_rows(lambda r: gb[s, r, :], 1024)
        sv[s, 7:8, :] = sum_rows(lambda r: gpre[r, 0:1024], 1024)
        sv[s, 8:9, :] = sum_rows(lambda r: gpre[r, 1024:2048], 1024)

    def grad_down(s):
        @pl.loop(0, 8)
        def _(i):
            cols = lanes(i * 2, 256)
            rows_w = pl.ds(pl.multiple_of(i * 256, 256), 256)
            wdown[s, rows_w, :] = dot(gels[s, :, cols], gb[s], 0, 0).astype(BF)

    def grad_low_two(s, b, k):
        @pl.loop(0, 4)
        def _(n):
            cols = lanes(n * 2, 256)
            rows_w = pl.ds(pl.multiple_of(n * 256, 256), 256)
            ys[rows_of(b), cols] = dot(gpre[rows_of(b), :], wup[s, rows_w, :], 1, 1).astype(BF)
            y_start(k, b, n)

    def grad_up(s):
        @pl.loop(0, 4)
        def _(i):
            cols = lanes(i * 2, 256)
            rows_w = pl.ds(pl.multiple_of(i * 256, 256), 256)
            for q in range(2):
                wup[s, rows_w, q * 1024 : q * 1024 + 1024] = dot(
                    low[:, cols], gpre[:, q * 1024 : q * 1024 + 1024], 0, 0
                ).astype(BF)

    def loop_sums(b, count, step):
        zero = jnp.zeros((1, 1024), F32)

        def body(i, tots):
            return step(pl.ds(pl.multiple_of(b * LP + i * CH, CH), CH), tots)

        return lax.fori_loop(0, LP // CH, body, (zero,) * count)

    def grad_middle(s, b, k):
        gain = row(s, 3)

        def step(rows, tots):
            t_gain, t_shift, t_out = tots
            g2 = y_sum(k, rows)
            nrm = nrm2s[s, rows, :].astype(F32)
            t = g2 * gain
            m1 = jnp.mean(t, axis=-1, keepdims=True)
            m2 = jnp.mean(t * nrm, axis=-1, keepdims=True)
            inv = inv2s[s, rows, :][:, 0:1]
            gm = gb[s, rows, :].astype(F32) + inv * (t - m1 - nrm * m2)
            mid[rows, :] = gm
            ga = gm.astype(BF)
            low[rows, :] = ga
            return (t_gain + colsum(g2 * nrm), t_shift + colsum(g2), t_out + colsum(ga.astype(F32)))

        for r, v in zip((3, 4, 2), loop_sums(b, 3, step)):
            total(s, r, b, v)

    def grad_mixed(s, b):
        @pl.loop(0, 2)
        def _(n):
            cols = lanes(n * 2, 256)
            rows_w = pl.ds(pl.multiple_of(n * 256, 256), 256)
            gpre[rows_of(b), cols] = dot(low[rows_of(b), :], wout[s, rows_w, :], 1, 1).astype(BF)

    def grad_out(s):
        @pl.loop(0, 2)
        def _(i):
            cols = lanes(i * 2, 256)
            rows_w = pl.ds(pl.multiple_of(i * 256, 256), 256)
            wout[s, rows_w, :] = dot(mixs[s, :, cols], low[...], 0, 0).astype(BF)

    def grad_attention(s, b):
        rows = rows_of(b)

        @pl.loop(0, 4)
        def _(i):
            cols = lanes(i)
            q, k, v = (qkvs[s, t, rows, cols] for t in range(3))
            gm = gpre[rows, cols]
            res = []
            for h in range(2):
                probs = softmax(pick(h, q), k)
                gp = dot(pick(h, gm), v, 1, 1)
                gv = dot(probs.astype(BF), gm, 0, 0)
                gs = (probs * (gp - jnp.sum(probs * gp, axis=-1, keepdims=True))).astype(BF)
                gq = dot(gs, k, 1, 0) * (64.0 ** -0.5)
                gk = dot(gs, q, 0, 0) * (64.0 ** -0.5)
                res.append((gq, gk, gv))
            for t in range(3):
                gqkv[t, rows, cols] = jnp.where(left, res[0][t], res[1][t]).astype(BF)

    def grad_qv_bias(s):
        sv[s, 6:7, 0:512] = sum_rows(lambda r: gqkv[0, r, :], 512)
        sv[s, 6:7, 512:1024] = sum_rows(lambda r: gqkv[2, r, :], 512)

    def grad_lowered(s, b, k):
        rows = rows_of(b)

        @pl.loop(0, 4)
        def _(n):
            cols = lanes(n * 2, 256)
            rows_w = pl.ds(pl.multiple_of(n * 256, 256), 256)
            a = dot(gqkv[0, rows, :], wqkv[0][s, rows_w, :], 1, 1)
            a = a + dot(gqkv[1, rows, :], wqkv[1][s, rows_w, :], 1, 1)
            a = a + dot(gqkv[2, rows, :], wqkv[2][s, rows_w, :], 1, 1)
            ys[rows, cols] = a.astype(BF)
            y_start(k, b, n)

    def grad_qkv(s, t):
        @pl.loop(0, 4)
        def _(i):
            cols = lanes(i * 2, 256)
            rows_w = pl.ds(pl.multiple_of(i * 256, 256), 256)
            wqkv[t][s, rows_w, :] = dot(low[:, cols], gqkv[t], 0, 0).astype(BF)

    def grad_stream(s, b, k, dst):
        gain = row(s, 0)

        def step(rows, tots):
            t_gain, t_shift = tots
            g1 = y_sum(k, rows)
            nrm, inv = norm_chunk(xs[s, rows, :].astype(F32))
            t = g1 * gain
            m1 = jnp.mean(t, axis=-1, keepdims=True)
            m2 = jnp.mean(t * nrm, axis=-1, keepdims=True)
            dst[rows, :] = (mid[rows, :] + inv * (t - m1 - nrm * m2)).astype(BF)
            return (t_gain + colsum(g1 * nrm), t_shift + colsum(g1))

        for r, v in zip((0, 1), loop_sums(b, 2, step)):
            total(s, r, b, v)

    def add_rows(dst, src, count, chunk):
        @pl.loop(0, count // chunk)
        def _(i):
            rows = pl.ds(pl.multiple_of(i * chunk, chunk), chunk)
            dst[rows, :] = dst[rows, :] + src[rows, :]

    def shape_of(m):
        if m in BY_ROWS:
            return 128, (16 if m == UP else 64)
        return WIDTH[m] // 2, 128

    def add_block(m, dst, src):
        add_rows(dst, src, *shape_of(m))

    def r_view(s, m, h):
        return rbuf[m] if s == 1 else half(m, w[m], 1, h)

    def x_view(s, m, k, col):
        if m in X_FIRST:
            return xbuf[m].at[s]
        if s == 0:
            return block(m, w[m], 1, at_dp(k, col), c)
        at = pl.ds(k * 128, 128)
        return xbuf[m].at[at, :] if m in BY_ROWS else xbuf[m].at[:, at]

    def z_view(s, m, slot, col, place):
        if s == 0:
            return block(m, w[m], 1, place * 2 + (x if col == 0 else 1 - x), c)
        return zbuf[m].at[col * 4 + slot]

    def rs_c(s, m):
        q = s * 6 + m - 1
        if s == 0:
            pl.semaphore_wait(free_c.at[m - 1], 1)
        remote(half(m, w[m], s, 1 - c), r_view(s, m, c), rsem_cs.at[q], rsem_c.at[q], to_c).start()

    def rs_sum(s, m):
        q = s * 6 + m - 1
        mine, got = half(m, w[m], s, c), r_view(s, m, 1 - c)
        cp = remote(mine, got, rsem_cs.at[q], rsem_c.at[q], to_c)
        cp.wait_recv()
        cp.wait_send()
        if s == 1:
            pl.semaphore_signal(free_c.at[m - 1], inc=1, device_id=to_c, device_id_type=MESH)
        rows = 1024 if m in BY_ROWS else WIDTH[m] // 2
        add_rows(mine, got, rows, 16 if m not in (Q, K, V) else 64)

    def rs_to_x(s, m):
        if s == 0:
            pl.semaphore_wait(free_x.at[m - 1], 1)
        for k in (INNER, FAR, NEAR, SELF):
            q = s * 6 + m - 1
            b = block(m, w[m], s, at_dp(k, 1), c)
            remote(b, x_view(s, m, k, 0), rsem_xs.at[q], rsem_x.at[rx[(s, m), k]], to_x).start()

    def rs_from_x(s, m, k):
        q = s * 6 + m - 1
        b = block(m, w[m], s, at_dp(k, 0), c)
        got = x_view(s, m, k, 1)
        remote(b, got, rsem_xs.at[q], rsem_x.at[rx[(s, m), k]], to_x).wait_recv()
        if k == SELF:
            wait_bytes(m, 4, rsem_xs.at[q])
        add_block(m, b, got)

    def x_freed(m):
        pl.semaphore_signal(free_x.at[m - 1], inc=1, device_id=to_x, device_id_type=MESH)

    def z_ready(m):
        @pl.when(inner)
        def _():
            pl.semaphore_wait(free_z.at[m - 1], 3)

        @pl.when(jnp.logical_not(inner))
        def _():
            pl.semaphore_wait(free_z.at[m - 1], 1)

    def rs_to_z(s, m, k, col):
        q = s * 6 + m - 1
        b = block(m, w[m], s, at_dp(k, col), c)
        if k == NEAR:
            remote(b, z_view(s, m, 0, col, z), rsem_zs.at[q, col], rsem_z.at[rz[(s, m), col * 4]], to_z(near)).start()
        else:

            @pl.when(jnp.logical_not(inner))
            def _():
                remote(b, z_view(s, m, k, col, places[k]), rsem_zs.at[q, col], rsem_z.at[rz[(s, m), col * 4 + k]], to_z(near)).start()

    def rs_pass(s, m, k, col):
        q = s * 6 + m - 1

        @pl.when(inner)
        def _():
            b = block(m, w[m], s, at_dp(k, col), c)
            got = z_view(s, m, k, col, places[k])
            remote(b, got, rsem_zs.at[q, col], rsem_z.at[rz[(s, m), col * 4 + k]], to_z(near)).wait_recv()
            add_block(m, b, got)
            remote(b, z_view(s, m, 1, col, places[k]), rsem_zs.at[q, col], rsem_z.at[rz[(s, m), col * 4 + 1]], to_z(places[k])).start()

    def z_arrived(s, m, col):
        q = s * 6 + m - 1
        got = [z_view(s, m, 0, col, near), z_view(s, m, 1, col, z)]
        for slot in range(2):
            remote(got[slot], got[slot], rsem_zs.at[q, col], rsem_z.at[rz[(s, m), col * 4 + slot]], to_z(near)).wait_recv()
        return got

    def z_sent(s, m, col):
        wait_bytes(m, 3, rsem_zs.at[s * 6 + m - 1, col])

    def z_freed(m):
        for k in (NEAR, INNER):
            pl.semaphore_signal(free_z.at[m - 1], inc=1, device_id=to_z(places[k]), device_id_type=MESH)

    def rs_fold(s, m):
        q = s * 6 + m - 1
        b = block(m, w[m], s, at_dp(SELF, 1), c)
        for got in z_arrived(s, m, 1):
            add_block(m, b, got)
        remote(b, xbuf[m].at[s], rsem_xs.at[q], rsem_x.at[rx[(s, m), 0]], to_x).start()

    def f_target(m):
        n = WIDTH[m] // 2
        at = pl.ds(pl.multiple_of(c * n, n), n)
        if m in (Q, K, V):
            return gqkv_out.at[m - 1, :, at]
        if m == UP:
            return gup_out.at[:, at]
        return (gout_out if m == OUT else gdown_out).at[at, :]

    def rs_f(s, m):
        q = s * 6 + m - 1
        mine = block(m, w[m], s, me, c)
        parts = [mine] + z_arrived(s, m, 0)
        if m in X_FIRST:
            cp = remote(mine, xbuf[m].at[s], rsem_xs.at[q], rsem_x.at[rx[(s, m), 0]], to_x)
            cp.wait_recv()
            cp.wait_send()
            parts.append(xbuf[m].at[s])
        count, chunk = shape_of(m)
        chunk = min(chunk, 64)

        @pl.loop(0, count // chunk)
        def _(i):
            rows = pl.ds(pl.multiple_of(i * chunk, chunk), chunk)
            a = parts[0][rows, :].astype(F32)
            for part in parts[1:]:
                a = a + part[rows, :].astype(F32)
            fbuf[m][rows, :] = a

        for col in range(2) if m in X_FIRST else (0,):
            z_sent(s, m, col)
        if s == 1:
            z_freed(m)

        @pl.when(c == s)
        def _():
            pltpu.make_async_copy(fbuf[m], f_target(m), rsem_fs.at[q]).start()

        @pl.when(c != s)
        def _():
            remote(fbuf[m], f_target(m), rsem_fs.at[q], rsem_f.at[q], to_c).start()

    def rs_f_sent(s, m):
        q = s * 6 + m - 1

        @pl.when(c == s)
        def _():
            pltpu.make_async_copy(fbuf[m], f_target(m), rsem_fs.at[q]).wait()

        @pl.when(c != s)
        def _():
            remote(fbuf[m], f_target(m), rsem_fs.at[q], rsem_f.at[q], to_c).wait_send()

    def rs_end(s, m):
        q = s * 6 + m - 1

        @pl.when(c == s)
        def _():
            remote(fbuf[m], fbuf[m], rsem_fs.at[q], rsem_f.at[q], to_c).wait_recv()

    def vec_copies(i):
        if i == 0:
            return [remote(sv.at[1 - c], svc, vsem_s.at[0], vsem.at[0], to_c)]
        if i == 1:
            return [remote(sv.at[c], svx, vsem_s.at[1], vsem.at[1], to_x)]
        if i == 2:
            return [
                remote(svc, svz.at[j - 1], vsem_s.at[1 + j], vsem.at[1 + j], to_z(lax.rem(z + j, Z)))
                for j in range(1, Z)
            ]
        return [pltpu.make_async_copy(sv.at[c], gvec_out, isem.at[2])]

    def vec_step(i):
        if i:
            for cp in vec_copies(i - 1):
                cp.wait_recv()
                cp.wait_send()
        if i == 1:
            sv[c] = sv[c] + svc[...]
        if i == 2:
            svc[...] = sv[c] + svx[...]
        if i == 3:
            sv[c] = svc[...] + svz[0] + svz[1] + svz[2]
        for cp in vec_copies(i):
            cp.start()

    clock = Clock()
    size = {SMALL: 8e3, Q: 131e3, K: 131e3, V: 131e3, OUT: 131e3, UP: 524e3, DOWN: 524e3}
    RATE = 88e3
    HOP = 1.8
    free = {"x": 0.0, "z": 0.0, "y": 0.0}
    got = {}

    def link(name, nbytes):
        free[name] = max(free[name], clock.now) + nbytes / RATE
        return free[name] + HOP

    in_x = pltpu.make_async_copy(x_ref.at[c], ys, isem.at[0])
    in_g = pltpu.make_async_copy(cot_ref.at[c], gpre.at[:, pl.ds(0, 1024)], isem.at[1])
    in_x.start()
    in_g.start()

    order = (SMALL, Q, K, V, OUT, UP, DOWN)
    for s in range(2):
        for m in order:
            ag_share(s, m)
    clock.now = 2.0

    def plan_gather(s, m):
        x_first = m in X_FIRST

        def at_x(k):
            ag_x(s, m, k)
            got[s, m] = got.get((s, m), 0) + 1
            if x_first:
                along_z(1)

        def at_z(k, col):
            ag_z(s, m, k, col)
            if x_first:
                got[s, m] = got.get((s, m), 0) + 1
            else:
                clock.add(link("x", size[m]), functools.partial(at_x, k))

        def along_z(col):
            begin = max(free["z"], clock.now)
            t = size[m] / RATE
            free["z"] = begin + 3 * t
            for k in (NEAR, INNER, FAR):
                clock.add(begin + k * t + (HOP if k == NEAR else 2 * HOP), functools.partial(at_z, k, col))

        def own():
            if not x_first:
                ag_shared(s, m)
            ag_own_z(s, m, 0)
            along_z(0)
            if not x_first:
                ag_to_x(s, m, SELF)
                clock.add(link("x", size[m]), functools.partial(at_x, SELF))

        def early():
            ag_shared(s, m)
            ag_to_x(s, m, SELF)
            clock.add(max(link("x", size[m]), z_begin[s, m] - LEAD + 0.1), functools.partial(at_x, SELF))

        if x_first:
            clock.add(x_begin[s, m], early)
        clock.add(max(z_begin[s, m] - LEAD, 2.0), own)

    LEAD = 5.0
    z_begin, x_begin, at = {}, {}, 3.0
    for s in range(2):
        for m in order:
            z_begin[s, m] = at
            at += size[m] / RATE * (6 if m in X_FIRST else 3)
            x_begin[s, m] = max(2.0, z_begin[s, m] - 14.0)
    for s in range(2):
        for m in order:
            plan_gather(s, m)

    def need(s, m):
        clock.drain(lambda: got.get((s, m), 0) == (7 if m in X_FIRST else 4))
        clock.now += 1.5
        ag_need(s, m)

    def y_sent():
        return link("y", 426e3 * 2) + 1.0

    passed = set()

    def reduce(s, m):
        x_first = m in X_FIRST
        t = size[m] / RATE
        order = (INNER, FAR, NEAR)

        def z_start(k, col):
            rs_to_z(s, m, k, col)
            ready = link("z", size[m])
            if k != NEAR:
                clock.add(ready, functools.partial(z_pass, k, col), 0.4)

        def z_pass(k, col):
            rs_pass(s, m, k, col)
            done.append((k, col))
            if len([d for d in done if d[1] == col]) == 2:
                ready = max(clock.now, free["z"] - 2 * t) + 2 * t + 2 * HOP
                if x_first and col == 1:
                    clock.add(ready, fold, 0.4)
                elif not x_first:
                    clock.add(ready, finish_sum, 0.6)

        done = []

        def fold():
            rs_fold(s, m)
            clock.add(max(link("x", size[m]), clock.now + 2.0), finish_sum, 0.6)

        def sum_step():
            rs_sum(s, m)
            passed.add(("c", s, m))
            if x_first:
                if s == 0:
                    clock.drain(lambda: ("z", m) in passed)
                    z_ready(m)
                for col in (1, 0):
                    for k in order:
                        z_start(k, col)
            else:
                if s == 0:
                    clock.drain(lambda: ("x", m) in passed)
                rs_to_x(s, m)
                for k in order + (SELF,):
                    clock.add(link("x", size[m]), functools.partial(from_x, k), 0.3)

        def from_x(k):
            rs_from_x(s, m, k)
            if k == SELF:
                done.append((SELF, -1))
                if s == 1:
                    x_freed(m)
                    passed.add(("x", m))
                return
            if k == INNER and s == 0:
                clock.drain(lambda: ("z", m) in passed)
                z_ready(m)
            z_start(k, 0)

        def finish_sum():
            clock.drain(lambda: ready_to_finish())
            if s == 0:
                rs_f_sent(1, m)
            rs_f(s, m)
            if s == 1:
                passed.add(("z", m))

        def ready_to_finish():
            return x_first or (SELF, -1) in done

        if s == 0:
            clock.drain(lambda: ("c", 1, m) in passed)
        rs_c(s, m)
        clock.add(clock.now + 4 * size[m] / 500e3 + 2.0, sum_step, 0.8)

    for i in range(5):
        clock.flush(clock.now)
        clock.now += 0.4
    in_x.wait()
    in_g.wait()
    for b in range(2):
        clock.run(0.6, unweave, ys, xs.at[0], b, None)
    for b in range(2):
        clock.run(0.6, unweave, gpre, gb.at[1], b, alive_of(b))
    y_at = {}
    for s in range(2):
        last = s == 1
        need(s, SMALL)
        unpack_small(s)
        for b in range(2):
            if last:
                clock.wait(y_at[1, b], y_wait, 1, b)
                clock.run(1.0, finish, 0, b, 1, xs.at[1])
                if b == 1:
                    emit(0, 0, xs.at[1])
            clock.run(2.3, ln1, s, b)
            if b == 0:
                for m in (Q, K, V):
                    need(s, m)
            clock.run(1.4, project, s, b)
            clock.run(3.6, attention, s, b)
            if b == 0:
                need(s, OUT)
            clock.run(0.7, out_project, s, b, s * 2)
            y_at[s * 2, b] = y_sent()
        for b in range(2):
            clock.wait(y_at[s * 2, b], y_wait, s * 2, b)
            clock.run(2.5, middle, s, b, s * 2)
            if b == 0:
                need(s, UP)
            clock.run(2.7, up_project, s, b)
        need(s, DOWN)
        if not last:
            for b in range(2):
                clock.run(1.5, down_project, 0, b, 1, True)
                y_at[1, b] = y_sent()

    for s in range(2):
        for m in order:
            ag_sent(s, m)
    for s in (1, 0):
        k = 3 if s == 1 else 5
        for b in range(2):
            if s == 0:
                clock.wait(y_at[4, b], y_wait, 4, b)
                clock.run(3.5, grad_stream, 1, b, 4, gb.at[0])
                if b == 1:
                    emit(1, 1, gb.at[0])
            clock.run(2.2, grad_gelu, s, b)
            clock.run(1.5, grad_low_two, s, b, k)
            y_at[k, b] = y_sent()
        if s == 0:
            for b in range(2):
                clock.run(0.5, relower, 0, b)
        clock.run(3.0, grad_up, s)
        reduce(s, UP)
        if s == 1:
            for b in range(2):
                clock.run(0.3, keep_middle, b)
                clock.run(1.5, down_project, 1, b, 7, False)
        clock.run(3.8, grad_down, s)
        reduce(s, DOWN)
        clock.run(1.0, grad_mlp_biases, s)
        for b in range(2):
            clock.wait(y_at[k, b], y_wait, k, b)
            clock.run(1.6, grad_middle, s, b, k)
            clock.run(0.5, grad_mixed, s, b)
            if b == 1:
                clock.run(0.9, grad_out, s)
                reduce(s, OUT)
            clock.run(5.1, grad_attention, s, b)
            clock.run(1.2, grad_lowered, s, b, k + 1)
            y_at[k + 1, b] = y_sent()
        for b in range(2):
            clock.run(2.3, ln1, s, b)
        for t in range(3):
            clock.run(1.4, grad_qkv, s, t)
            reduce(s, Q + t)
        clock.run(0.5, grad_qv_bias, s)
    for b in range(2):
        clock.wait(y_at[6, b], y_wait, 6, b)
        clock.run(3.5, grad_stream, 0, b, 6, low)
    emit(1, 0, low)
    for i in range(4):
        clock.add(clock.now + 3.0 * i, functools.partial(vec_step, i), 0.5)
    for b in range(2):
        for n in range(4):
            y_start(7, b, n)
        y_at[7, b] = y_sent()
    for b in range(2):
        clock.wait(y_at[7, b], y_wait, 7, b)
        clock.run(1.0, finish, 1, b, 7, gb.at[1])
    emit(0, 1, gb.at[1])
    clock.drain(lambda: not clock.queue)
    for cp in vec_copies(3):
        cp.wait()
    for m in MATS:
        rs_f_sent(0, m)
    for s in range(2):
        for m in MATS:
            rs_end(s, m)
    emit_sent(0, 0, xs.at[1])
    emit_sent(0, 1, gb.at[1])
    emit_sent(1, 1, gb.at[0])
    emit_sent(1, 0, low)
    for which in range(2):
        for s in range(2):
            emit_got(which, s, low)


def run_kernel(small, qkv, out, up, down, xin, cot, live):
    any_spec = pl.BlockSpec(memory_space=pl.ANY)
    V = pltpu.VMEM
    D_ = pltpu.SemaphoreType.DMA
    REG = pltpu.SemaphoreType.REGULAR
    S = jax.ShapeDtypeStruct
    mats = ((1024, 512), (1024, 512), (1024, 512), (512, 1024), (1024, 2048), (2048, 1024))
    by_rows = (True, True, True, False, True, False)
    first = (False, True, False, True, False, False)

    def halved(shape, rows, cut):
        return (shape[0] // cut, shape[1] // 2) if rows else (shape[0] // 2, shape[1] // cut)

    scratch = [V((2, 8, 32, 128), BF)]
    scratch += [V((2,) + shape, BF) for shape in mats]
    scratch += [V(halved(shape, rows, 1), BF) for shape, rows in zip(mats, by_rows)]
    scratch += [
        V((2,) + halved(shape, rows, 8) if f else halved(shape, rows, 2), BF)
        for shape, rows, f in zip(mats, by_rows, first)
    ]
    scratch += [V((8 if f else 4,) + halved(shape, rows, 8), BF) for shape, rows, f in zip(mats, by_rows, first)]
    scratch += [V(halved(shape, rows, 8), F32) for shape, rows in zip(mats, by_rows)]
    scratch += [
        V((2, R, 1024), BF), V((2, 3, R, 512), BF), V((2, R, 512), BF), V((2, R, 1024), BF),
        V((2, R, 2048), BF), V((2, R, 2048), BF), V((2, R, 128), F32),
        V((R, 1024), BF), V((R, 1024), F32), V((2, R, 1024), BF), V((R, 2048), BF), V((3, R, 512), BF),
        V((R, 1024), BF), V((2, R, 1024), BF), V((LP, 256), F32),
        V((2, 16, 1024), F32), V((2, 16, 1024), F32), V((16, 1024), F32), V((16, 1024), F32), V((3, 16, 1024), F32),
        D_((14,)), D_((14, 2)), D_((54,)), D_((44,)),
        D_((12,)), D_((12,)), D_((12,)), D_((36,)), D_((12, 2)), D_((64,)), D_((12,)), D_((12,)),
        D_((16,)), D_((16,)), D_((4,)), D_((4,)), D_((4,)), D_((3,)), D_((5,)), D_((5,)),
        REG((6,)), REG((6,)), REG((6,)),
    ]
    return pl.pallas_call(
        kernel,
        out_shape=[
            S((2, R, 1024), BF), S((2, R, 1024), BF), S((3, 128, 512), F32), S((512, 128), F32),
            S((128, 2048), F32), S((2048, 128), F32), S((16, 1024), F32),
        ],
        in_specs=[any_spec] * 7 + [pl.BlockSpec(memory_space=pltpu.SMEM)],
        out_specs=[any_spec] * 7,
        scratch_shapes=scratch,
        compiler_params=pltpu.CompilerParams(
            collective_id=1, has_side_effects=True, vmem_limit_bytes=67043328
        ),
        name="sections",
    )(small, qkv, out, up, down, xin, cot, live)


def local_fast(images, cotangent, live_count, ln1_gain, ln1_bias, qkv_weight, qv_bias, out_weight, out_bias,
               ln2_gain, ln2_bias, up_weight, up_bias, down_weight, down_bias):
    d = lax.axis_index("dp")

    def woven(a):
        a = jnp.transpose(a, (0, 2, 1, 3)).reshape(2, 2 * L, 1024)
        return jnp.pad(a, ((0, 0), (0, R - 2 * L), (0, 0)))

    def spread(a, width):
        n = a.shape[-1]
        z8 = jnp.where((jnp.arange(8) == d)[:, None], a[..., None, :], jnp.zeros_like(a[..., None, :]))
        return z8.reshape(a.shape[:-1] + (8 * n,))

    at = lax.broadcasted_iota(jnp.int32, (32, 128), 0)
    small = jnp.pad(spread(qv_bias[0], 64).reshape(8, 128), ((6, 18), (0, 0)))
    small = small + jnp.pad(spread(up_bias[0], 256).reshape(16, 128), ((14, 2), (0, 0)))
    for i, v in enumerate((ln1_gain, ln1_bias, out_bias, ln2_gain, ln2_bias, down_bias)):
        small = jnp.where(at == i, v, small)
    act, gin, gqkv, gout, gup, gdown, gvec = run_kernel(
        small, qkv_weight[0], out_weight[0], up_weight[0], down_weight[0], woven(images), woven(cotangent), live_count
    )

    def cut(v, axis, n):
        return lax.dynamic_slice_in_dim(v, d * n, n, axis=axis)

    act = act.reshape(2, 2, LP, 1024)[None, :, :, :L]
    gin = gin.reshape(2, 2, LP, 1024)[None, :, :, :L]
    vecs = cut(gvec[:6], 1, 128)
    qv = cut(gvec[6].reshape(2, 8, 64), 2, 8)
    upb = cut(gvec[7:9].reshape(8, 256), 1, 32)
    return (
        act, gin, vecs[0:1], vecs[1:2], gqkv[None], qv[None], gout[None], vecs[2:3], vecs[3:4], vecs[4:5],
        gup[None], upb[None], gdown[None], vecs[5:6],
    )


def solution(mesh):
    fast = dict(mesh.shape) == {"section": 2, "dp": 8, "mp": 2}
    return jax.shard_map(
        local_fast if fast else local,
        mesh=mesh,
        in_specs=(
            P(None, "dp", None, None),
            P(None, "dp", None, None),
            P(None, "dp"),
            P("section", "dp"),
            P("section", "dp"),
            P("section", None, "dp", "mp"),
            P("section", None, "mp", "dp"),
            P("section", "mp", "dp"),
            P("section", "dp"),
            P("section", "dp"),
            P("section", "dp"),
            P("section", "dp", "mp"),
            P("section", "mp", "dp"),
            P("section", "mp", "dp"),
            P("section", "dp"),
        ),
        out_specs=(
            P("section", None, "dp", None, None),
            P("section", None, "dp", None, None),
            P("section", "dp"),
            P("section", "dp"),
            P("section", None, "dp", "mp"),
            P("section", None, "mp", "dp"),
            P("section", "mp", "dp"),
            P("section", "dp"),
            P("section", "dp"),
            P("section", "dp"),
            P("section", "dp", "mp"),
            P("section", "mp", "dp"),
            P("section", "mp", "dp"),
            P("section", "dp"),
        ),
        check_vma=False,
    )
```

```python
import functools
import heapq
import math

import jax
import jax.numpy as jnp
from jax import lax
from jax.experimental import pallas as pl
from jax.experimental.pallas import tpu as pltpu
from jax.sharding import PartitionSpec as P

HD = 64


epsilon = 1e-06


def gather_all(small, big):
    flat = jnp.concatenate([piece.reshape(-1) for piece in small])
    packed = lax.all_gather(flat, "dp", axis=0, tiled=False)
    count = packed.shape[0]
    whole, offset = [], 0
    for piece, axis in zip(small, (1, 1, 3, 1, 1, 1, 2, 1)):
        part = packed[:, offset : offset + piece.size].reshape((count,) + piece.shape)
        offset += piece.size
        part = jnp.moveaxis(part, 0, axis)
        shape = list(piece.shape)
        shape[axis] *= count
        whole.append(part.reshape(shape))
    qkv, out, up, down = (
        lax.all_gather(piece, "dp", axis=axis, tiled=True) for piece, axis in zip(big, (2, 2, 1, 2))
    )
    return (
        whole[0],
        whole[1],
        qkv,
        whole[2],
        out,
        whole[3],
        whole[4],
        whole[5],
        up,
        whole[6],
        down,
        whole[7],
    )


def scatter_all(totals, shards):
    small_at = (0, 1, 3, 5, 6, 7, 9, 11)
    count = lax.axis_size("dp")
    rows = []
    for index, axis in zip(small_at, (1, 1, 3, 1, 1, 1, 2, 1)):
        piece = totals[index]
        shape = list(piece.shape)
        shape[axis : axis + 1] = [count, shape[axis] // count]
        rows.append(jnp.moveaxis(piece.reshape(shape), axis, 0).reshape(count, -1))
    packed = lax.psum_scatter(jnp.concatenate(rows, axis=1), "dp", scatter_dimension=0, tiled=False)
    owned, offset = [None] * 12, 0
    for index in small_at:
        size = shards[index].size
        owned[index] = packed[offset : offset + size].reshape(shards[index].shape)
        offset += size
    for index, axis in zip((2, 4, 8, 10), (2, 2, 1, 2)):
        owned[index] = lax.psum_scatter(
            totals[index].astype(jnp.bfloat16), "dp", scatter_dimension=axis, tiled=True
        ).astype(jnp.float32)
    return owned


def both_halves(partial):
    return lax.psum(partial.astype(jnp.bfloat16), "mp").astype(jnp.float32)


def from_behind(x, axis, by):
    length = lax.axis_size(axis)
    pairs = [(i, i + by) for i in range(length) if 0 <= i + by < length]
    return lax.ppermute(x, axis, pairs)


def norm_parts(stream):
    centered = stream - jnp.mean(stream, axis=-1, keepdims=True)
    inverse = lax.rsqrt(jnp.mean(centered * centered, axis=-1, keepdims=True) + epsilon)
    return (centered * inverse, inverse)


def norm_back(grad_normed, normed, inverse):
    first_mean = jnp.mean(grad_normed, axis=-1, keepdims=True)
    second_mean = jnp.mean(grad_normed * normed, axis=-1, keepdims=True)
    return inverse * (grad_normed - first_mean - normed * second_mean)


def gelu_slope(preact):
    cumul = 0.5 * (1.0 + lax.erf(preact * 2.0 ** (-0.5)))
    density = jnp.exp(-0.5 * preact * preact) * (2.0 * math.pi) ** (-0.5)
    return cumul + preact * density


def unpack_weights(whole):
    return (
        whole[0][0].astype(jnp.float32),
        whole[1][0].astype(jnp.float32),
        whole[2][0],
        whole[3][0].reshape(2, -1).astype(jnp.float32),
        whole[4][0],
        whole[5][0].astype(jnp.float32),
        whole[6][0].astype(jnp.float32),
        whole[7][0].astype(jnp.float32),
        whole[8][0],
        whole[9][0].reshape(-1).astype(jnp.float32),
        whole[10][0],
        whole[11][0].astype(jnp.float32),
    )


def forward(stream, params, rows):
    (
        gain_one,
        shift_one,
        qkv_mat,
        qv_shift,
        out_mat,
        out_shift,
        gain_two,
        shift_two,
        up_mat,
        up_shift,
        down_mat,
        down_shift,
    ) = params
    batch_size, seq_len, model_width = stream.shape
    head_count = qkv_mat.shape[2] // HD
    scale = HD ** (-0.5)
    normed, inverse = norm_parts(stream)
    lowered = (normed * gain_one + shift_one).astype(jnp.bfloat16)
    projected = jnp.einsum("bld,cde->cble", lowered, qkv_mat, preferred_element_type=jnp.float32)
    split_shape = (batch_size, seq_len, head_count, HD)
    queries = (projected[0] + qv_shift[0]).astype(jnp.bfloat16).reshape(split_shape)
    keys_low = projected[1].astype(jnp.bfloat16).reshape(split_shape)
    values_low = (projected[2] + qv_shift[1]).astype(jnp.bfloat16).reshape(split_shape)
    scores = (
        jnp.einsum("blhe,bmhe->bhlm", queries, keys_low, preferred_element_type=jnp.float32) * scale
    )
    row_max = jnp.max(scores, axis=-1, keepdims=True)
    log_total = row_max + jnp.log(jnp.sum(jnp.exp(scores - row_max), axis=-1, keepdims=True))
    attn_probs = jnp.exp(scores - log_total)
    mixed = jnp.einsum(
        "bhlm,bmhe->blhe",
        attn_probs.astype(jnp.bfloat16),
        values_low,
        preferred_element_type=jnp.float32,
    )
    mixed = mixed.astype(jnp.bfloat16).reshape(batch_size, seq_len, -1)
    partial_attn = jnp.einsum("bld,de->ble", mixed, out_mat, preferred_element_type=jnp.float32)
    middle = stream + both_halves(partial_attn) + out_shift
    normed_two, inverse_two = norm_parts(middle)
    lowered_two = (normed_two * gain_two + shift_two).astype(jnp.bfloat16)
    preact = (
        jnp.einsum("bld,df->blf", lowered_two, up_mat, preferred_element_type=jnp.float32)
        + up_shift
    )
    gelu_out = jax.nn.gelu(preact, approximate=False).astype(jnp.bfloat16)
    partial_mlp = jnp.einsum("blf,fd->bld", gelu_out, down_mat, preferred_element_type=jnp.float32)
    result = (middle + both_halves(partial_mlp) + down_shift) * rows
    return (result, (stream, middle, queries, keys_low, values_low, log_total, mixed, preact))


def backward(seed, saved, params, shapes):
    (
        gain_one,
        shift_one,
        qkv_mat,
        qv_shift,
        out_mat,
        out_shift,
        gain_two,
        shift_two,
        up_mat,
        up_shift,
        down_mat,
        down_shift,
    ) = params
    stream, middle, queries, keys_low, values_low, log_total, mixed, preact = saved
    batch_size, seq_len, head_count, head_dim = queries.shape
    scale = HD ** (-0.5)
    normed, inverse = norm_parts(stream)
    lowered = (normed * gain_one + shift_one).astype(jnp.bfloat16)
    normed_two, inverse_two = norm_parts(middle)
    lowered_two = (normed_two * gain_two + shift_two).astype(jnp.bfloat16)
    gelu_out = jax.nn.gelu(preact, approximate=False).astype(jnp.bfloat16)
    grad_mlp = seed.astype(jnp.bfloat16)
    grad_down_shift = jnp.sum(grad_mlp.astype(jnp.float32), axis=(0, 1))
    grad_down_mat = jnp.einsum(
        "blf,bld->fd", gelu_out, grad_mlp, preferred_element_type=jnp.float32
    )
    grad_gelu = jnp.einsum("bld,fd->blf", grad_mlp, down_mat, preferred_element_type=jnp.float32)
    grad_pre = (grad_gelu * gelu_slope(preact)).astype(jnp.bfloat16)
    grad_up_shift = jnp.sum(grad_pre.astype(jnp.float32), axis=(0, 1))
    grad_up_mat = jnp.einsum(
        "bld,blf->df", lowered_two, grad_pre, preferred_element_type=jnp.float32
    )
    grad_low_two = both_halves(
        jnp.einsum("blf,df->bld", grad_pre, up_mat, preferred_element_type=jnp.float32)
    )
    grad_gain_two = jnp.sum(grad_low_two * normed_two, axis=(0, 1))
    grad_shift_two = jnp.sum(grad_low_two, axis=(0, 1))
    grad_middle = seed + norm_back(grad_low_two * gain_two, normed_two, inverse_two)
    grad_attn = grad_middle.astype(jnp.bfloat16)
    grad_out_shift = jnp.sum(grad_attn.astype(jnp.float32), axis=(0, 1))
    grad_out_mat = jnp.einsum("bld,ble->de", mixed, grad_attn, preferred_element_type=jnp.float32)
    grad_mixed = jnp.einsum("ble,de->bld", grad_attn, out_mat, preferred_element_type=jnp.float32)
    grad_mixed = grad_mixed.astype(jnp.bfloat16).reshape(batch_size, seq_len, head_count, head_dim)
    scores = (
        jnp.einsum("blhe,bmhe->bhlm", queries, keys_low, preferred_element_type=jnp.float32) * scale
    )
    attn_probs = jnp.exp(scores - log_total)
    grad_probs = jnp.einsum(
        "blhe,bmhe->bhlm", grad_mixed, values_low, preferred_element_type=jnp.float32
    )
    grad_values = jnp.einsum(
        "bhlm,blhe->bmhe",
        attn_probs.astype(jnp.bfloat16),
        grad_mixed,
        preferred_element_type=jnp.float32,
    ).astype(jnp.bfloat16)
    grad_scores = (
        attn_probs * (grad_probs - jnp.sum(attn_probs * grad_probs, axis=-1, keepdims=True))
    ).astype(jnp.bfloat16)
    grad_queries = (
        jnp.einsum("bhlm,bmhe->blhe", grad_scores, keys_low, preferred_element_type=jnp.float32)
        * scale
    ).astype(jnp.bfloat16)
    grad_keys = (
        jnp.einsum("bhlm,blhe->bmhe", grad_scores, queries, preferred_element_type=jnp.float32)
        * scale
    ).astype(jnp.bfloat16)
    grad_proj = jnp.stack([grad_queries, grad_keys, grad_values]).reshape(
        3, batch_size, seq_len, -1
    )
    grad_qv_shift = jnp.stack(
        [
            jnp.sum(grad_queries.astype(jnp.float32), axis=(0, 1)),
            jnp.sum(grad_values.astype(jnp.float32), axis=(0, 1)),
        ]
    )
    grad_qkv_mat = jnp.einsum(
        "bld,cble->cde", lowered, grad_proj, preferred_element_type=jnp.float32
    )
    grad_lowered = both_halves(
        jnp.einsum("cble,cde->bld", grad_proj, qkv_mat, preferred_element_type=jnp.float32)
    )
    grad_gain_one = jnp.sum(grad_lowered * normed, axis=(0, 1))
    grad_shift_one = jnp.sum(grad_lowered, axis=(0, 1))
    grad_stream = grad_middle + norm_back(grad_lowered * gain_one, normed, inverse)
    terms = [
        grad_gain_one,
        grad_shift_one,
        grad_qkv_mat,
        grad_qv_shift,
        grad_out_mat,
        grad_out_shift,
        grad_gain_two,
        grad_shift_two,
        grad_up_mat,
        grad_up_shift,
        grad_down_mat,
        grad_down_shift,
    ]
    return (grad_stream, [term.reshape(shape) for term, shape in zip(terms, shapes)])


def local(
    images,
    cotangent,
    live_count,
    ln1_gain,
    ln1_bias,
    qkv_weight,
    qv_bias,
    out_weight,
    out_bias,
    ln2_gain,
    ln2_bias,
    up_weight,
    up_bias,
    down_weight,
    down_bias,
):
    first_section = lax.axis_index("section") == 0
    micro_count = images.shape[0]
    slot_count = images.shape[1]
    slot_ids = jnp.arange(slot_count)
    small = (ln1_gain, ln1_bias, qv_bias, out_bias, ln2_gain, ln2_bias, up_bias, down_bias)
    gathered = gather_all(small, (qkv_weight, out_weight, up_weight, down_weight))
    params = unpack_weights(gathered)
    shapes = [piece.shape for piece in gathered]

    def row_mask(batch_index, valid):
        alive = jnp.logical_and(slot_ids < live_count[batch_index, 0], valid)
        return alive.astype(jnp.float32).reshape(slot_count, 1, 1)

    def choose(for_first, for_second):
        return jnp.where(first_section, for_first, for_second)

    incoming = jnp.zeros(images.shape[1:], jnp.bfloat16)
    outputs = []
    kept = []
    for moment in range(micro_count + 1):
        own = images[min(moment, micro_count - 1)]
        source = choose(own, incoming).astype(jnp.float32)
        rows = choose(
            row_mask(min(moment, micro_count - 1), moment < micro_count),
            row_mask(max(moment - 1, 0), moment >= 1),
        )
        result, saved = forward(source, params, rows)
        result = result.astype(jnp.bfloat16)
        outputs.append(result)
        kept.append(saved)
        if moment < micro_count:
            incoming = from_behind(result, "section", 1)
    activations = jnp.stack(
        [choose(outputs[index], outputs[index + 1]) for index in range(micro_count)]
    )
    totals = [jnp.zeros(shape, jnp.float32) for shape in shapes]
    incoming = jnp.zeros(images.shape[1:], jnp.bfloat16)
    returned = []
    for moment in range(micro_count + 1):
        later_index = min(moment, micro_count - 1)
        rows = choose(
            row_mask(max(moment - 1, 0), moment >= 1), row_mask(later_index, moment < micro_count)
        )
        seed = choose(incoming, cotangent[later_index]).astype(jnp.float32) * rows
        saved = jax.tree.map(choose, kept[max(moment - 1, 0)], kept[min(moment + 1, micro_count)])
        grad_stream, terms = backward(seed, saved, params, shapes)
        grad_low = grad_stream.astype(jnp.bfloat16)
        returned.append(grad_low)
        if moment < micro_count:
            incoming = from_behind(grad_low, "section", -1)
        totals = [first_part + second_part for first_part, second_part in zip(totals, terms)]
    shards = (
        ln1_gain,
        ln1_bias,
        qkv_weight,
        qv_bias,
        out_weight,
        out_bias,
        ln2_gain,
        ln2_bias,
        up_weight,
        up_bias,
        down_weight,
        down_bias,
    )
    owned = scatter_all(totals, shards)
    input_grads = jnp.stack(
        [choose(returned[index + 1], returned[index]) for index in range(micro_count)]
    )
    return (
        activations[None],
        input_grads[None],
        owned[0],
        owned[1],
        owned[2],
        owned[3],
        owned[4],
        owned[5],
        owned[6],
        owned[7],
        owned[8],
        owned[9],
        owned[10],
        owned[11],
    )


MESH = pl.DeviceIdType.MESH
BF = jnp.bfloat16
F32 = jnp.float32
Z = 4
EPS = 1e-06
L = 197
LP = 208
R = 2 * LP
SMALL, Q, K, V, OUT, UP, DOWN = range(7)
MATS = (Q, K, V, OUT, UP, DOWN)
BY_ROWS = (Q, K, V, UP)
X_FIRST = (K, OUT)
WIDTH = {Q: 512, K: 512, V: 512, OUT: 512, UP: 2048, DOWN: 2048}
SELF, NEAR, INNER, FAR = range(4)


class Clock:
    def __init__(self):
        self.now, self.queue, self.count = 0.0, [], 0

    def add(self, ready, step, cost=0.2):
        heapq.heappush(self.queue, (ready, self.count, cost, step))
        self.count += 1

    def pop(self):
        ready, _, cost, step = heapq.heappop(self.queue)
        self.now = max(self.now, ready)
        step()
        self.now += cost

    def flush(self, until):
        while self.queue and self.queue[0][0] <= until:
            self.pop()

    def run(self, cost, step, *args):
        self.flush(self.now)
        step(*args)
        self.now += cost

    def wait(self, until, step, *args):
        self.flush(until)
        self.now = max(self.now, until)
        step(*args)

    def drain(self, done):
        while not done():
            self.pop()


def lanes(d, n=128):
    return pl.ds(pl.multiple_of(d * 128, 128), n)


def dot(a, b, ca, cb):
    return lax.dot_general(a, b, (((ca,), (cb,)), ((), ())), preferred_element_type=F32)


def half(m, ref, s, h):
    n = WIDTH[m] // 2
    at = pl.ds(pl.multiple_of(h * n, n), n)
    return ref.at[s, :, at] if m in BY_ROWS else ref.at[s, at, :]


def block(m, ref, s, d, h=None):
    if m == SMALL:
        return ref.at[s, d] if h is None else ref.at[s, d, pl.ds(h * 16, 16), :]
    own = pl.ds(pl.multiple_of(d * 128, 128), 128)
    n = WIDTH[m] // 2
    other = pl.ds(0, 2 * n) if h is None else pl.ds(pl.multiple_of(h * n, n), n)
    return ref.at[s, own, other] if m in BY_ROWS else ref.at[s, other, own]


def kernel(
    gain1_ref, shift1_ref, bias_o_ref, gain2_ref, shift2_ref, bias_d_ref, qv_ref, upb_ref,
    qkv_ref, out_ref, up_ref, down_ref, x_ref, cot_ref, live_ref,
    act_out, gin_out, gqkv_out, gout_out, gup_out, gdown_out, gvec_out,
    wsmall, wq, wk, wv, wout, wup, wdown,
    rq, rk, rv, rout, rup, rdown, xq, xk, xv, xout, xup, xdown,
    zq, zk, zv, zout, fq, fk, fv, fout, fup, fdown,
    xs, qkvs, mixs, nrm2s, gels, slps, stats,
    low, mid, gb, gpre, gqkv, ys, yr, acc, vec, sv, svc, svx, svz, woven, stage, pack, raw, rawq, rawu,
    asem_s, asem_c, asem_z, asem_x, rsem_cs, rsem_c, rsem_xs, rsem_x, rsem_zs, rsem_z, rsem_fs, rsem_f,
    ysem, ysem_s, osem, osem_r, osem_s, isem, vsem, vsem_s, free_c, free_x, free_z, free_up, free_r, free_y,
):
    shards = (pack, qkv_ref.at[0], qkv_ref.at[1], qkv_ref.at[2], out_ref, up_ref, down_ref)
    wqkv = (wq, wk, wv)
    w = (wsmall, wq, wk, wv, wout, wup, wdown)
    rbuf = (None, rq, rk, rv, rout, rup, rdown)
    xbuf = (None, xq, xk, xv, xout, xup, xdown)
    zbuf = (None, zq, zk, zv, zout)
    fbuf = (None, fq, fk, fv, fout, fup, fdown)

    c = lax.axis_index("section")
    me = lax.axis_index("dp")
    y = lax.axis_index("mp")
    z, x = me // 2, lax.rem(me, 2)
    to_x = {"dp": z * 2 + 1 - x}
    to_c = {"section": 1 - c}
    to_y = {"mp": 1 - y}

    inner = jnp.logical_or(z == 1, z == 2)
    near = z + 1 - 2 * lax.rem(z, 2)
    lower = (z < 2).astype(jnp.int32)
    places = (z, near, 1 + lower, 3 * lower)
    inner_i = jnp.where(inner, 1, 0)

    def at_dp(k, col):
        return places[k] * 2 + (x if col == 0 else 1 - x)

    def to_z(zi):
        return {"dp": zi * 2 + x}

    def remote(a, b, ss, rs, dev):
        return pltpu.make_async_remote_copy(
            src_ref=a, dst_ref=b, send_sem=ss, recv_sem=rs, device_id=dev, device_id_type=MESH
        )

    barrier = pltpu.get_barrier_semaphore()
    for dev in [to_z(places[k]) for k in (NEAR, INNER, FAR)] + [to_x, to_c, to_y]:
        pl.semaphore_signal(barrier, inc=1, device_id=dev, device_id_type=MESH)
    pl.semaphore_wait(barrier, Z + 2)

    def number(per):
        table = {}
        for key, count in per:
            for i in range(count):
                table[key, i] = len(table)
        return table

    pieces = [(s, m) for s in range(2) for m in range(7)]
    az = number((p, 6 if p[1] in X_FIRST else 3) for p in pieces)
    ax = number((p, 1 if p[1] in X_FIRST else 4) for p in pieces)
    rz = number((p, 8 if p[1] in X_FIRST else 4) for p in pieces if p[1])
    rx = number((p, 1 if p[1] in X_FIRST else 4) for p in pieces if p[1])

    def wait_bytes(m, count, sem):
        if m == SMALL:
            v = stats.at[pl.ds(0, 8 * count), :]
        else:
            v = wdown.at[:, pl.ds(0, count * WIDTH[m] // 32), :]
        pltpu.make_async_copy(v, v, sem).wait()

    def ag_share(s, m):
        p = s * 7 + m

        @pl.when(c == s)
        def _():
            dst = block(m, w[m], s, me)
            remote(shards[m], dst, asem_s.at[p], asem_c.at[p, 0], to_c).start()
            pltpu.make_async_copy(shards[m], dst, asem_c.at[p, 0]).start()

    def ag_shared(s, m):
        whole = block(m, w[m], s, me)
        pltpu.make_async_copy(whole, whole, asem_c.at[s * 7 + m, 0]).wait()

    def ag_own_z(s, m, col):
        p, first = s * 7 + m, az[(s, m), col * 3]
        b = block(m, w[m], s, at_dp(SELF, col), c)
        slot = jnp.where(inner, INNER, FAR) - 1
        remote(b, b, asem_s.at[p], asem_z.at[first], to_z(near)).start()
        remote(b, b, asem_s.at[p], asem_z.at[first + slot], to_z(places[INNER])).start()

    def ag_to_x(s, m, k):
        b = block(m, w[m], s, at_dp(k, 0), c)
        remote(b, b, asem_s.at[s * 7 + m], asem_x.at[ax[(s, m), k]], to_x).start()

    def ag_to_c(s, m, k, col):
        p = s * 7 + m
        b = block(m, w[m], s, at_dp(k, col), c)
        remote(b, b, asem_s.at[p], asem_c.at[p, 1], to_c).start()

    def ag_z(s, m, k, col):
        b = block(m, w[m], s, at_dp(k, col), c)
        cp = remote(b, b, asem_s.at[s * 7 + m], asem_z.at[az[(s, m), col * 3 + k - 1]], to_z(near))
        cp.wait_recv()
        if k != NEAR:

            @pl.when(inner)
            def _():
                cp.start()

        if m not in X_FIRST:
            ag_to_x(s, m, k)
        ag_to_c(s, m, k, col)

    def ag_x(s, m, k):
        b = block(m, w[m], s, at_dp(k, 1), c)
        remote(b, b, asem_s.at[s * 7 + m], asem_x.at[ax[(s, m), k]], to_x).wait_recv()
        if m in X_FIRST:
            ag_own_z(s, m, 1)
        ag_to_c(s, m, k, 1)

    def ag_need(s, m):
        wait_bytes(m, 7, asem_c.at[s * 7 + m, 1])

    def ag_sent(s, m):
        count = 7 + (1 + 4 if m in X_FIRST else 4 + 2)
        extra = 4 if m in X_FIRST else 2
        for ins in range(2):
            for own in range(2):

                @pl.when(jnp.logical_and(inner_i == ins, jnp.where(c == s, 1, 0) == own))
                def _():
                    wait_bytes(m, count + extra * ins + 2 * own, asem_s.at[s * 7 + m])

    def rows_of(b):
        return pl.ds(b * LP, LP)

    def y_src(k):
        return slps.at[1, :, pl.ds(0, 1024)] if k == 7 else ys

    def y_start(k, b, n):
        cols = lanes(n * 2, 256)
        src = y_src(k).at[rows_of(b), cols]
        remote(src, yr.at[k % 2, rows_of(b), cols], ysem_s.at[k * 2 + b], ysem.at[k * 2 + b], to_y).start()

    def y_wait(k, b):
        src = y_src(k).at[rows_of(b), pl.ds(0, 1024)]
        cp = remote(src, yr.at[k % 2, rows_of(b), :], ysem_s.at[k * 2 + b], ysem.at[k * 2 + b], to_y)
        cp.wait_recv()
        cp.wait_send()

    def y_sum(k, rows):
        return y_src(k)[rows, :].astype(F32) + yr[k % 2, rows, :].astype(F32)

    small_in = [
        pltpu.make_async_copy(ref, raw.at[i], isem.at[2 + i])
        for i, ref in enumerate((gain1_ref, shift1_ref, bias_o_ref, gain2_ref, shift2_ref, bias_d_ref))
    ] + [pltpu.make_async_copy(qv_ref, rawq, isem.at[8]), pltpu.make_async_copy(upb_ref, rawu, isem.at[9])]

    def pack_small():
        for cp in small_in:
            cp.wait()

        def iota(shape, axis):
            return lax.broadcasted_iota(jnp.int32, shape, axis)

        def hot(test):
            return jnp.where(test, 1.0, 0.0).astype(BF)

        r = iota((32, 128), 0)
        v = jnp.zeros((32, 128), F32)
        for i in range(6):
            v = jnp.where(r == i, raw[i].astype(F32), v)
        for t in range(2):
            for e in range(2):
                pick_rows = hot(iota((32, 8), 1) == 2 * (iota((32, 8), 0) - 6 - 4 * t) + e)
                spread = hot(iota((8, 128), 1) == e * 64 + me * 8 + iota((8, 128), 0))
                rows = dot(pick_rows, rawq[t], 1, 0).astype(BF)
                v = v + dot(rows, spread, 1, 0)
        odd = me // 4
        pick_rows = hot(2 * iota((32, 8), 1) + odd == iota((32, 8), 0) - 14)
        spread = hot(iota((32, 128), 1) == lax.rem(me, 4) * 32 + iota((32, 128), 0))
        v = v + dot(dot(pick_rows, rawu[...], 1, 0).astype(BF), spread, 1, 0)
        pack[...] = v.astype(BF)

    def unpack_small(s):
        total = jnp.zeros((32, 128), F32)
        for d in range(2 * Z):
            piece = wsmall[s, d].astype(F32)
            total = total + piece
            for r in range(6):
                vec[s, r : r + 1, d * 128 : d * 128 + 128] = piece[r : r + 1, :]
        for k in range(8):
            vec[s, 6:7, k * 128 : k * 128 + 128] = total[6 + k : 7 + k, :]
            vec[s, 7:8, k * 128 : k * 128 + 128] = total[14 + k : 15 + k, :]
            vec[s, 8:9, k * 128 : k * 128 + 128] = total[22 + k : 23 + k, :]

    def row(s, r):
        return vec[s, r : r + 1, :]

    CH = 16

    lane = lax.broadcasted_iota(jnp.int32, (1, 128), 1)
    left = lane < 64
    live_col = lax.broadcasted_iota(jnp.int32, (1, LP), 1) < L
    INV2, MEAN1, INV1 = range(3)

    def stat_at(s, which):
        return 16 + 4 * s + which

    def put_stats(rows, *pairs):
        v = stats[rows, :]
        for at, value in pairs:
            v = jnp.where(lane == at, value, v)
        stats[rows, :] = v

    def stat(s, which, rows):
        at = stat_at(s, which)
        return stats[rows, :][:, at : at + 1]

    def norm_chunk(v):
        mean = jnp.mean(v, axis=-1, keepdims=True)
        cen = v - mean
        inv = lax.rsqrt(jnp.mean(cen * cen, axis=-1, keepdims=True) + EPS)
        return cen * inv, mean, inv

    def chunks(b, pair=1):
        def at(i):
            return pl.ds(pl.multiple_of(b * LP + i * CH, CH), CH)

        def wrap(body):
            count = LP // CH

            @pl.loop(0, count // pair)
            def _(i):
                for j in range(pair):
                    body(at(i * pair + j))

            for j in range(count % pair):
                body(at(count - 1 - j))

        return wrap

    def ln1(s, b):
        gain, shift = row(s, 0), row(s, 1)

        @chunks(b, 2)
        def _(rows):
            nrm, mean, inv = norm_chunk(xs[s, rows, :].astype(F32))
            put_stats(rows, (stat_at(s, MEAN1), mean), (stat_at(s, INV1), inv))
            low[rows, :] = (nrm * gain + shift).astype(BF)

    def norm1(s, rows):
        return (xs[s, rows, :].astype(F32) - stat(s, MEAN1, rows)) * stat(s, INV1, rows)

    def relow1(s, b, dst):
        gain, shift = row(s, 0), row(s, 1)

        @chunks(b)
        def _(rows):
            dst[rows, :] = (norm1(s, rows) * gain + shift).astype(BF)

    def load_woven(ref, sem, dst):
        cp = pltpu.make_async_copy(ref.at[c], woven.at[pl.ds(0, L)], sem)
        cp.start()
        cp.wait()
        woven[L:LP] = jnp.zeros((LP - L, 2, 1024), BF)

        @pl.loop(0, LP // 16)
        def _(i):
            dst[pl.ds(pl.multiple_of(i * 32, 32), 32), 0:1024] = woven[pl.ds(i * 16, 16)].reshape(32, 1024)

    def unweave(src, dst, b, alive):
        r = lax.broadcasted_iota(jnp.int32, (LP, R), 0)
        q = lax.broadcasted_iota(jnp.int32, (LP, R), 1)
        take = jnp.where(q == 2 * r + b, 1.0, 0.0)
        if alive is not None:
            take = take * alive
        take = take.astype(BF)

        @pl.loop(0, 4)
        def _(n):
            cols = lanes(n * 2, 256)
            dst[rows_of(b), cols] = dot(take, src[:, cols], 1, 0).astype(BF)

    def weave(src, tmp):
        r = lax.broadcasted_iota(jnp.int32, (R, R), 0)
        q = lax.broadcasted_iota(jnp.int32, (R, R), 1)
        put = jnp.where(q == lax.rem(r, 2) * LP + r // 2, 1.0, 0.0).astype(BF)

        @pl.loop(0, 4)
        def _(n):
            cols = lanes(n * 2, 256)
            tmp[:, cols] = dot(put, src[:, cols], 1, 0).astype(BF)

        @pl.loop(0, LP // 16)
        def _(i):
            woven[pl.ds(i * 16, 16)] = tmp[pl.ds(pl.multiple_of(i * 32, 32), 32), 0:1024].reshape(16, 2, 1024)

    def alive_of(b):
        return jnp.where(live_ref[c] > b, 1.0, 0.0)

    def project(s, b):
        for t in range(3):
            @pl.loop(0, 2)
            def _(n):
                cols = lanes(n * 2, 256)
                a = dot(low[rows_of(b), :], wqkv[t][s, :, cols], 1, 0)
                if t != 1:
                    base = 0 if t == 0 else 512
                    a = a + vec[s, 6:7, pl.ds(pl.multiple_of(base + n * 256, 256), 256)]
                qkvs[s, t, rows_of(b), cols] = a.astype(BF)

    def pick(h, v):
        return jnp.where(left if h == 0 else jnp.logical_not(left), v, jnp.zeros_like(v))

    def scores(q, k):
        return jnp.where(live_col, dot(q, k, 1, 1), -1e30)

    def attention(s, b):
        rows = rows_of(b)

        @pl.loop(0, 4)
        def _(i):
            cols = lanes(i)
            q, k, v = (qkvs[s, t, rows, cols] for t in range(3))
            q = q * jnp.asarray(0.125, BF)
            ones = jnp.ones_like(v)
            tops, parts = [], []
            for h in range(2):
                sc = scores(pick(h, q), k)
                tops.append(jnp.max(sc, axis=-1, keepdims=True))
                e = jnp.exp(sc - tops[h]).astype(BF)
                parts.append(dot(e, jnp.where(left, v, ones) if h == 0 else jnp.where(left, ones, v), 1, 0))
            den = pltpu.roll(jnp.where(left, parts[1], parts[0]), 64, 1)
            mixs[s, rows, cols] = (jnp.where(left, parts[0], parts[1]) / den).astype(BF)
            lse = jnp.where(left, tops[0], tops[1]) + jnp.log(den)
            stats[rows, :] = jnp.where(lax.rem(lane, 64) == 8 * s + i, lse, stats[rows, :])

    def out_project(s, b, k):
        @pl.loop(0, 4)
        def _(n):
            cols = lanes(n * 2, 256)
            ys[rows_of(b), cols] = dot(mixs[s, rows_of(b), :], wout[s, :, cols], 1, 0).astype(BF)
            y_start(k, b, n)

    def middle(s, b, k):
        shift, gain2, shift2 = row(s, 2), row(s, 3), row(s, 4)

        @chunks(b, 2)
        def _(rows):
            v = xs[s, rows, :].astype(F32) + y_sum(k, rows) + shift
            if s == 0:
                mid[rows, :] = v
            else:
                gb[0, rows, :] = v.astype(BF)
            nrm, _, inv = norm_chunk(v)
            nrm2s[s, rows, :] = nrm.astype(BF)
            put_stats(rows, (stat_at(s, INV2), inv))
            low[rows, :] = (nrm * gain2 + shift2).astype(BF)

    def up_project(s, b):
        @pl.loop(0, 8)
        def _(n):
            cols = lanes(n * 2, 256)
            acc[...] = dot(low[rows_of(b), :], wup[s, :, cols], 1, 0)
            at = pl.ds(pl.multiple_of(lax.rem(n, 4) * 256, 256), 256)
            bias = jnp.where(n < 4, vec[s, 7:8, at], vec[s, 8:9, at])

            @pl.loop(0, LP // 16)
            def _(i):
                rows = pl.ds(pl.multiple_of(b * LP + i * 16, 16), 16)
                a = acc[pl.ds(pl.multiple_of(i * 16, 16), 16), :] + bias
                phi = 0.5 * (1.0 + lax.erf(a * (2.0 ** -0.5)))
                dens = jnp.exp(-0.5 * a * a) * ((2.0 * math.pi) ** -0.5)
                gels[s, rows, cols] = (a * phi).astype(BF)
                slps[s, rows, cols] = (phi + a * dens).astype(BF)

    def down_project(s, b, k, send):
        @pl.loop(0, 4)
        def _(n):
            cols = lanes(n * 2, 256)
            y_src(k)[rows_of(b), cols] = dot(gels[s, rows_of(b), :], wdown[s, :, cols], 1, 0).astype(BF)
            if send:
                y_start(k, b, n)

    def finish(s, b, k, dst):
        shift, alive = row(s, 5), alive_of(b)

        @chunks(b)
        def _(rows):
            base = mid[rows, :] if s == 0 else slps[1, rows, 1024:2048].astype(F32)
            dst[rows, :] = ((base + y_sum(k, rows) + shift) * alive).astype(BF)

    def keep_middle(b):
        @chunks(b)
        def _(rows):
            slps[1, rows, 1024:2048] = gb[0, rows, :]

    def emit_copies(which, s):
        target = (act_out, gin_out)[which].at[c]
        src, q = woven.at[pl.ds(0, L)], which * 2 + s
        return pltpu.make_async_copy(src, target, osem.at[q]), remote(src, target, osem_s.at[q], osem_r.at[q], to_c)

    def emit(which, s):
        here, there = emit_copies(which, s)

        @pl.when(c == s)
        def _():
            here.start()

        @pl.when(c != s)
        def _():
            there.start()

    def emit_sent(which, s):
        here, there = emit_copies(which, s)

        @pl.when(c == s)
        def _():
            here.wait()

        @pl.when(c != s)
        def _():
            there.wait_send()

    def emit_got(which, s):
        @pl.when(c == s)
        def _():
            remote(
                woven.at[pl.ds(0, L)], (act_out, gin_out)[which].at[1 - c], osem_s.at[which * 2 + s], osem_r.at[which * 2 + s], to_c
            ).wait_recv()

    def relower(s, b, dst):
        gain2, shift2 = row(s, 3), row(s, 4)

        @chunks(b)
        def _(rows):
            dst[rows, :] = (nrm2s[s, rows, :].astype(F32) * gain2 + shift2).astype(BF)

    def fold8(v):
        return jnp.sum(v.reshape(v.shape[0] // 8, 8, v.shape[1]), axis=0)

    def colsum(v):
        return jnp.sum(v, axis=0, keepdims=True)

    def sum_rows(ref_slice, width):
        def step(i, tot):
            rows = pl.ds(pl.multiple_of(i * 32, 32), 32)
            return tot + fold8(ref_slice(rows).astype(F32))

        return colsum(lax.fori_loop(0, R // 32, step, jnp.zeros((8, width), F32)))

    def total(s, r, b, v):
        sv[s, r : r + 1, :] = v if b == 0 else sv[s, r : r + 1, :] + v

    def grad_gelu(s, b):
        @pl.loop(0, 8)
        def _(n):
            cols = lanes(n * 2, 256)
            rows_w = pl.ds(pl.multiple_of(n * 256, 256), 256)
            a = dot(gb[s, rows_of(b), :], wdown[s, rows_w, :], 1, 1)
            gpre[rows_of(b), cols] = (a * slps[s, rows_of(b), cols].astype(F32)).astype(BF)

    def grad_mlp_biases(s):
        sv[s, 5:6, :] = sum_rows(lambda r: gb[s, r, :], 1024)
        sv[s, 7:8, :] = sum_rows(lambda r: gpre[r, 0:1024], 1024)
        sv[s, 8:9, :] = sum_rows(lambda r: gpre[r, 1024:2048], 1024)

    def grad_down(s, h, dst):
        @pl.loop(0, 4)
        def _(i):
            first = h * 1024 + i * 256
            cols = pl.ds(pl.multiple_of(first, 256), 256)
            rows_w = pl.ds(pl.multiple_of(i * 256 if s == 1 else first, 256), 256)
            dst[rows_w, :] = dot(gels[s, :, cols], gb[s], 0, 0).astype(BF)

    def grad_low_two(s, b, k):
        @pl.loop(0, 4)
        def _(n):
            cols = lanes(n * 2, 256)
            rows_w = pl.ds(pl.multiple_of(n * 256, 256), 256)
            ys[rows_of(b), cols] = dot(gpre[rows_of(b), :], wup[s, rows_w, :], 1, 1).astype(BF)
            y_start(k, b, n)

    def grad_up(s, low2):
        @pl.loop(0, 4)
        def _(i):
            cols = lanes(i * 2, 256)
            rows_w = pl.ds(pl.multiple_of(i * 256, 256), 256)
            for q in range(2):
                wup[s, rows_w, q * 1024 : q * 1024 + 1024] = dot(
                    low2[:, cols], gpre[:, q * 1024 : q * 1024 + 1024], 0, 0
                ).astype(BF)

    def loop_sums(b, count, step):
        zero = jnp.zeros((8, 1024), F32)

        def body(i, tots):
            new = step(pl.ds(pl.multiple_of(b * LP + i * CH, CH), CH))
            return tuple(t + fold8(v) for t, v in zip(tots, new))

        return [colsum(t) for t in lax.fori_loop(0, LP // CH, body, (zero,) * count)]

    def grad_middle(s, b, k):
        gain = row(s, 3)

        def step(rows):
            g2 = y_sum(k, rows)
            nrm = nrm2s[s, rows, :].astype(F32)
            t = g2 * gain
            m1 = jnp.mean(t, axis=-1, keepdims=True)
            m2 = jnp.mean(t * nrm, axis=-1, keepdims=True)
            gm = gb[s, rows, :].astype(F32) + stat(s, INV2, rows) * (t - m1 - nrm * m2)
            mid[rows, :] = gm
            ga = gm.astype(BF)
            low[rows, :] = ga
            return g2 * nrm, g2, ga.astype(F32)

        for r, v in zip((3, 4, 2), loop_sums(b, 3, step)):
            total(s, r, b, v)

    def grad_mixed(s, b):
        @pl.loop(0, 2)
        def _(n):
            cols = lanes(n * 2, 256)
            rows_w = pl.ds(pl.multiple_of(n * 256, 256), 256)
            gpre[rows_of(b), cols] = dot(low[rows_of(b), :], wout[s, rows_w, :], 1, 1).astype(BF)

    def grad_out(s):
        @pl.loop(0, 2)
        def _(i):
            cols = lanes(i * 2, 256)
            rows_w = pl.ds(pl.multiple_of(i * 256, 256), 256)
            wout[s, rows_w, :] = dot(mixs[s, :, cols], low[...], 0, 0).astype(BF)

    def grad_attention(s, b):
        rows = rows_of(b)

        @pl.loop(0, 4)
        def _(i):
            cols = lanes(i)
            q, k, v = (qkvs[s, t, rows, cols] for t in range(3))
            q, k_low = q * jnp.asarray(0.125, BF), k * jnp.asarray(0.125, BF)
            gm = gpre[rows, cols]
            kept = stats[rows, :]
            res = []
            for h in range(2):
                lse = jnp.sum(jnp.where(lane == 64 * h + 8 * s + i, kept, 0.0), axis=-1, keepdims=True)
                probs = jnp.exp(scores(pick(h, q), k) - lse)
                gp = dot(pick(h, gm), v, 1, 1)
                gv = dot(probs.astype(BF), gm, 0, 0)
                gs = (probs * (gp - jnp.sum(probs * gp, axis=-1, keepdims=True))).astype(BF)
                res.append((dot(gs, k_low, 1, 0), dot(gs, q, 0, 0), gv))
            for t in range(3):
                gqkv[t, rows, cols] = jnp.where(left, res[0][t], res[1][t]).astype(BF)

    def grad_qv_bias(s):
        sv[s, 6:7, 0:512] = sum_rows(lambda r: gqkv[0, r, :], 512)
        sv[s, 6:7, 512:1024] = sum_rows(lambda r: gqkv[2, r, :], 512)

    def grad_lowered(s, b, k):
        rows = rows_of(b)

        @pl.loop(0, 4)
        def _(n):
            cols = lanes(n * 2, 256)
            rows_w = pl.ds(pl.multiple_of(n * 256, 256), 256)
            a = dot(gqkv[0, rows, :], wqkv[0][s, rows_w, :], 1, 1)
            a = a + dot(gqkv[1, rows, :], wqkv[1][s, rows_w, :], 1, 1)
            a = a + dot(gqkv[2, rows, :], wqkv[2][s, rows_w, :], 1, 1)
            ys[rows, cols] = a.astype(BF)
            y_start(k, b, n)

    def grad_qkv(s, t, low1):
        @pl.loop(0, 4)
        def _(i):
            cols = lanes(i * 2, 256)
            rows_w = pl.ds(pl.multiple_of(i * 256, 256), 256)
            wqkv[t][s, rows_w, :] = dot(low1[:, cols], gqkv[t], 0, 0).astype(BF)

    def grad_stream(s, b, k, dst):
        gain = row(s, 0)

        def step(rows):
            g1 = y_sum(k, rows)
            nrm = norm1(s, rows)
            t = g1 * gain
            m1 = jnp.mean(t, axis=-1, keepdims=True)
            m2 = jnp.mean(t * nrm, axis=-1, keepdims=True)
            dst[rows, :] = (mid[rows, :] + stat(s, INV1, rows) * (t - m1 - nrm * m2)).astype(BF)
            if s == 1:
                low[rows, :] = (nrm * gain + row(s, 1)).astype(BF)
            return g1 * nrm, g1

        for r, v in zip((0, 1), loop_sums(b, 2, step)):
            total(s, r, b, v)

    def add_rows(dst, src, count, chunk):
        @pl.loop(0, count // chunk)
        def _(i):
            rows = pl.ds(pl.multiple_of(i * chunk, chunk), chunk)
            dst[rows, :] = dst[rows, :] + src[rows, :]

    def shape_of(m):
        if m in BY_ROWS:
            return 128, (16 if m == UP else 64)
        return WIDTH[m] // 2, 128

    def add_block(m, dst, src):
        add_rows(dst, src, *shape_of(m))

    def g_half(s, m):
        return stage if (s, m) == (1, DOWN) else half(m, w[m], s, c)

    def g_block(s, m, d):
        if (s, m) == (1, DOWN):
            return stage.at[:, pl.ds(pl.multiple_of(d * 128, 128), 128)]
        return block(m, w[m], s, d, c)

    def r_view(s, m, h):
        return rbuf[m] if s == 1 else half(m, w[m], 1, h)

    def x_view(s, m, k, col):
        if m in X_FIRST:
            return xbuf[m].at[s]
        if s == 0 and m in (Q, V):
            return gels.at[1, pl.ds((m - Q) * 128, 128), pl.ds(k * 256, 256)]
        if s == 0:
            return block(m, w[m], 1, at_dp(k, col), c)
        at = pl.ds(k * 128, 128)
        return xbuf[m].at[at, :] if m in BY_ROWS else xbuf[m].at[:, at]

    def z_view(s, m, slot, col, place):
        if s == 0 and m in (Q, K, V):
            i = col * 4 + slot if m == K else 4 + slot
            return gels.at[1, pl.ds((m - Q) * 128, 128), pl.ds(i * 256, 256)]
        if s == 0:
            return block(m, w[m], 1, place * 2 + (x if col == 0 else 1 - x), c)
        if m in (UP, DOWN):
            at = pl.ds(slot * 128, 128)
            return rbuf[m].at[at, :] if m == UP else rbuf[m].at[:, at]
        return zbuf[m].at[col * 4 + slot]

    def rs_c(s, m):
        q = s * 6 + m - 1
        if s == 0:
            pl.semaphore_wait(free_c.at[m - 1], 1)
        if (s, m) == (1, UP):
            pl.semaphore_wait(free_up, 1)
        src = rup if (s, m) == (1, DOWN) else half(m, w[m], s, 1 - c)
        remote(src, r_view(s, m, c), rsem_cs.at[q], rsem_c.at[q], to_c).start()

    def rs_sum(s, m):
        q = s * 6 + m - 1
        mine, got = g_half(s, m), r_view(s, m, 1 - c)
        cp = remote(mine, got, rsem_cs.at[q], rsem_c.at[q], to_c)
        cp.wait_recv()
        cp.wait_send()
        if (s, m) == (1, DOWN):
            pl.semaphore_signal(free_up, inc=1, device_id=to_c, device_id_type=MESH)
        elif s == 1:
            pl.semaphore_signal(free_c.at[m - 1], inc=1, device_id=to_c, device_id_type=MESH)
        rows = 1024 if m in BY_ROWS else WIDTH[m] // 2
        add_rows(mine, got, rows, 16 if m not in (Q, K, V) else 64)
        if s == 1 and m in (UP, DOWN):
            z_credit(free_r.at[m - UP])

    def rs_to_x(s, m):
        if s == 0:
            pl.semaphore_wait(free_x.at[m - 1], 1)
        for k in (INNER, FAR, NEAR, SELF):
            q = s * 6 + m - 1
            b = g_block(s, m, at_dp(k, 1))
            remote(b, x_view(s, m, k, 0), rsem_xs.at[q], rsem_x.at[rx[(s, m), k]], to_x).start()

    def rs_from_x(s, m, k):
        q = s * 6 + m - 1
        b = g_block(s, m, at_dp(k, 0))
        got = x_view(s, m, k, 1)
        remote(b, got, rsem_xs.at[q], rsem_x.at[rx[(s, m), k]], to_x).wait_recv()
        if k == SELF:
            wait_bytes(m, 4, rsem_xs.at[q])
        add_block(m, b, got)

    def down_freed():
        pl.semaphore_signal(free_c.at[DOWN - 1], inc=1, device_id=to_c, device_id_type=MESH)
        x_freed(DOWN)
        z_freed(DOWN)

    def gelu_freed():
        for m in (Q, V):
            x_freed(m)
        for m in (Q, K, V):
            z_freed(m)

    def x_freed(m):
        pl.semaphore_signal(free_x.at[m - 1], inc=1, device_id=to_x, device_id_type=MESH)

    def z_wait_credits(sem):
        @pl.when(inner)
        def _():
            pl.semaphore_wait(sem, 3)

        @pl.when(jnp.logical_not(inner))
        def _():
            pl.semaphore_wait(sem, 1)

    def z_credit(sem):
        for k in (NEAR, INNER):
            pl.semaphore_signal(sem, inc=1, device_id=to_z(places[k]), device_id_type=MESH)

    def z_ready(s, m):
        if s == 0:
            z_wait_credits(free_z.at[m - 1])
        elif m in (UP, DOWN):
            z_wait_credits(free_r.at[m - UP])

    def rs_to_z(s, m, k, col):
        q = s * 6 + m - 1
        b = g_block(s, m, at_dp(k, col))
        if k == NEAR:
            remote(b, z_view(s, m, 0, col, z), rsem_zs.at[q, col], rsem_z.at[rz[(s, m), col * 4]], to_z(near)).start()
        else:

            @pl.when(jnp.logical_not(inner))
            def _():
                remote(b, z_view(s, m, k, col, places[k]), rsem_zs.at[q, col], rsem_z.at[rz[(s, m), col * 4 + k]], to_z(near)).start()

    def rs_pass(s, m, k, col):
        q = s * 6 + m - 1

        @pl.when(inner)
        def _():
            b = g_block(s, m, at_dp(k, col))
            got = z_view(s, m, k, col, places[k])
            remote(b, got, rsem_zs.at[q, col], rsem_z.at[rz[(s, m), col * 4 + k]], to_z(near)).wait_recv()
            add_block(m, b, got)
            remote(b, z_view(s, m, 1, col, places[k]), rsem_zs.at[q, col], rsem_z.at[rz[(s, m), col * 4 + 1]], to_z(places[k])).start()

    def z_arrived(s, m, col):
        q = s * 6 + m - 1
        got = [z_view(s, m, 0, col, near), z_view(s, m, 1, col, z)]
        for slot in range(2):
            remote(got[slot], got[slot], rsem_zs.at[q, col], rsem_z.at[rz[(s, m), col * 4 + slot]], to_z(near)).wait_recv()
        return got

    def z_sent(s, m, col):
        wait_bytes(m, 3, rsem_zs.at[s * 6 + m - 1, col])

    def z_freed(m):
        z_credit(free_z.at[m - 1])

    def rs_fold(s, m):
        q = s * 6 + m - 1
        b = g_block(s, m, at_dp(SELF, 1))
        for got in z_arrived(s, m, 1):
            add_block(m, b, got)
        remote(b, xbuf[m].at[s], rsem_xs.at[q], rsem_x.at[rx[(s, m), 0]], to_x).start()

    def f_target(m):
        n = WIDTH[m] // 2
        at = pl.ds(pl.multiple_of(c * n, n), n)
        if m in (Q, K, V):
            return gqkv_out.at[m - 1, :, at]
        if m == UP:
            return gup_out.at[:, at]
        return (gout_out if m == OUT else gdown_out).at[at, :]

    def rs_f(s, m):
        q = s * 6 + m - 1
        mine = g_block(s, m, me)
        parts = [mine] + z_arrived(s, m, 0)
        if m in X_FIRST:
            cp = remote(mine, xbuf[m].at[s], rsem_xs.at[q], rsem_x.at[rx[(s, m), 0]], to_x)
            cp.wait_recv()
            cp.wait_send()
            parts.append(xbuf[m].at[s])
        count, chunk = shape_of(m)
        chunk = min(chunk, 64)

        @pl.loop(0, count // chunk)
        def _(i):
            rows = pl.ds(pl.multiple_of(i * chunk, chunk), chunk)
            a = parts[0][rows, :].astype(F32)
            for part in parts[1:]:
                a = a + part[rows, :].astype(F32)
            fbuf[m][rows, :] = a

        for col in range(2) if m in X_FIRST else (0,):
            z_sent(s, m, col)
        if s == 1 and m in (UP, OUT):
            z_freed(m)

        @pl.when(c == s)
        def _():
            pltpu.make_async_copy(fbuf[m], f_target(m), rsem_fs.at[q]).start()

        @pl.when(c != s)
        def _():
            remote(fbuf[m], f_target(m), rsem_fs.at[q], rsem_f.at[q], to_c).start()

    def rs_f_sent(s, m):
        q = s * 6 + m - 1

        @pl.when(c == s)
        def _():
            pltpu.make_async_copy(fbuf[m], f_target(m), rsem_fs.at[q]).wait()

        @pl.when(c != s)
        def _():
            remote(fbuf[m], f_target(m), rsem_fs.at[q], rsem_f.at[q], to_c).wait_send()

    def rs_end(s, m):
        q = s * 6 + m - 1

        @pl.when(c == s)
        def _():
            remote(fbuf[m], fbuf[m], rsem_fs.at[q], rsem_f.at[q], to_c).wait_recv()

    def vec_copies(i):
        if i == 0:
            return [remote(sv.at[1 - c], svc, vsem_s.at[0], vsem.at[0], to_c)]
        if i == 1:
            return [remote(sv.at[c], svx, vsem_s.at[1], vsem.at[1], to_x)]
        if i == 2:
            return [
                remote(svc, svz.at[j - 1], vsem_s.at[1 + j], vsem.at[1 + j], to_z(lax.rem(z + j, Z)))
                for j in range(1, Z)
            ]
        return [pltpu.make_async_copy(sv.at[c], gvec_out, isem.at[0])]

    def vec_step(i):
        if i:
            for cp in vec_copies(i - 1):
                cp.wait_recv()
                cp.wait_send()
        if i == 1:
            sv[c] = sv[c] + svc[...]
        if i == 2:
            svc[...] = sv[c] + svx[...]
        if i == 3:
            sv[c] = svc[...] + svz[0] + svz[1] + svz[2]
        for cp in vec_copies(i):
            cp.start()

    clock = Clock()
    size = {SMALL: 8e3, Q: 131e3, K: 131e3, V: 131e3, OUT: 131e3, UP: 524e3, DOWN: 524e3}
    RATE = 82e3
    HOP = 1.8
    free = {"x": 0.0, "z": 0.0, "y": 0.0}
    got = {}

    def link(name, nbytes):
        free[name] = max(free[name], clock.now) + nbytes / RATE
        return free[name] + HOP

    order = (SMALL, Q, K, V, OUT, UP, DOWN)
    for cp in small_in:
        cp.start()
    for s in range(2):
        for m in order[1:]:
            ag_share(s, m)
    pack_small()
    for s in range(2):
        ag_share(s, SMALL)
    clock.now = 6.5

    def plan_gather(s, m):
        x_first = m in X_FIRST

        def at_x(k):
            ag_x(s, m, k)
            got[s, m] = got.get((s, m), 0) + 1
            if x_first:
                along_z(1)

        def at_z(k, col):
            ag_z(s, m, k, col)
            if x_first:
                got[s, m] = got.get((s, m), 0) + 1
            else:
                clock.add(link("x", size[m]), functools.partial(at_x, k))

        def along_z(col):
            begin = max(free["z"], clock.now)
            t = size[m] / RATE
            free["z"] = begin + 3 * t
            for k in (NEAR, INNER, FAR):
                late = HOP if k == NEAR else 2 * HOP
                clock.add(begin + k * t + late, functools.partial(at_z, k, col))

        def own():
            if not x_first:
                ag_shared(s, m)
            ag_own_z(s, m, 0)
            along_z(0)
            if not x_first:
                ag_to_x(s, m, SELF)
                clock.add(link("x", size[m]), functools.partial(at_x, SELF))

        def early():
            ag_shared(s, m)
            ag_to_x(s, m, SELF)
            clock.add(max(link("x", size[m]), z_begin[s, m] - LEAD + 0.1), functools.partial(at_x, SELF))

        if x_first:
            clock.add(x_begin[s, m], early)
        clock.add(max(z_begin[s, m] - LEAD, clock.now), own)

    LEAD, AHEAD = 23.0, 2.0
    z_begin, x_begin, at = {}, {}, 7.0
    for s in range(2):
        for m in order:
            z_begin[s, m] = at
            at += size[m] / RATE * (6 if m in X_FIRST else 3)
            x_begin[s, m] = max(clock.now, z_begin[s, m] - LEAD - AHEAD)
    for s in range(2):
        for m in order:
            plan_gather(s, m)

    def need(s, m):
        clock.drain(lambda: got.get((s, m), 0) == (7 if m in X_FIRST else 4))
        clock.now += 1.5
        ag_need(s, m)

    def y_sent():
        return link("y", 426e3 * 2) + 1.0

    passed = set()

    def reduce(s, m):
        x_first = m in X_FIRST
        t = size[m] / RATE
        order = (INNER, FAR, NEAR)

        def z_start(k, col):
            rs_to_z(s, m, k, col)
            ready = link("z", size[m])
            if k != NEAR:
                clock.add(ready, functools.partial(z_pass, k, col), 0.4)

        def z_pass(k, col):
            rs_pass(s, m, k, col)
            done.append((k, col))
            if len([d for d in done if d[1] == col]) == 2:
                ready = clock.now + t + 2 * HOP + 4.0
                if x_first and col == 1:
                    clock.add(ready, fold, 0.4)
                elif not x_first:
                    clock.add(ready, finish_sum, 0.6)

        done = []

        def fold():
            rs_fold(s, m)
            clock.add(max(link("x", size[m]), clock.now + 2.0), finish_sum, 0.6)

        def sum_step():
            rs_sum(s, m)
            passed.add(("c", s, m))
            if x_first:
                if s == 0:
                    clock.drain(lambda: ("z", m) in passed)
                z_ready(s, m)
                for col in (1, 0):
                    for k in order:
                        z_start(k, col)
            else:
                if s == 0:
                    clock.drain(lambda: ("x", m) in passed)
                rs_to_x(s, m)
                for k in order + (SELF,):
                    clock.add(link("x", size[m]) + 1.5, functools.partial(from_x, k), 0.3)

        def from_x(k):
            rs_from_x(s, m, k)
            if k == SELF:
                done.append((SELF, -1))
                if s == 1:
                    if m == UP:
                        x_freed(m)
                        passed.add(("x", m))
                return
            if k == INNER:
                if s == 0:
                    clock.drain(lambda: ("z", m) in passed)
                z_ready(s, m)
            z_start(k, 0)

        def finish_sum():
            clock.drain(lambda: ready_to_finish())
            if s == 0:
                clock.drain(lambda: ("f", m) in passed)
                rs_f_sent(1, m)
            rs_f(s, m)
            if s == 1:
                passed.add(("f", m))
                if m in (UP, OUT):
                    passed.add(("z", m))

        def ready_to_finish():
            return x_first or (SELF, -1) in done

        if s == 0:
            clock.drain(lambda: ("c", 1, m) in passed)
        elif m == UP:
            clock.drain(lambda: ("c", 1, DOWN) in passed)
        rs_c(s, m)
        clock.add(clock.now + 4 * size[m] / 500e3 + 2.0, sum_step, 0.8)

    clock.run(2.0, load_woven, x_ref, isem.at[0], gpre)
    for b in range(2):
        clock.run(0.6, unweave, gpre, xs.at[0], b, None)
    y_at = {}
    for s in range(2):
        last = s == 1
        need(s, SMALL)
        unpack_small(s)
        for b in range(2):
            if last:
                clock.wait(y_at[1, b], y_wait, 1, b)
                clock.run(1.0, finish, 0, b, 1, xs.at[1])
            clock.run(1.7, ln1, s, b)
            if b == 0:
                for m in (Q, K, V):
                    need(s, m)
            clock.run(1.7, project, s, b)
            clock.run(3.0, attention, s, b)
            if b == 0:
                need(s, OUT)
            clock.run(0.9, out_project, s, b, s * 2)
            y_at[s * 2, b] = y_sent()
        if last:
            clock.run(1.5, weave, xs.at[1], gpre)
            emit(0, 0)
        for b in range(2):
            clock.wait(y_at[s * 2, b], y_wait, s * 2, b)
            clock.run(1.5, middle, s, b, s * 2)
            if b == 0:
                need(s, UP)
            clock.run(4.0, up_project, s, b)
        if not last:
            need(0, DOWN)
            for b in range(2):
                clock.run(1.5, down_project, 0, b, 1, True)
                y_at[1, b] = y_sent()
            clock.run(2.0, load_woven, cot_ref, isem.at[1], gpre)
            for b in range(2):
                clock.run(0.6, unweave, gpre, gb.at[1], b, alive_of(b))

    clock.run(1.9, grad_down, 1, 1 - c, rup)
    reduce(1, DOWN)
    clock.run(1.9, grad_down, 1, c, stage)
    need(1, DOWN)
    for b in range(2):
        clock.run(2.7, grad_gelu, 1, b)
        clock.run(2.0, grad_low_two, 1, b, 3)
        y_at[3, b] = y_sent()
    for q in range(2):
        for m in order:
            ag_sent(q, m)
    for s in (1, 0):
        k = 3 if s == 1 else 5
        clock.run(3.0, grad_up, s, low if s == 1 else gb.at[1])
        reduce(s, UP)
        if s == 0:
            for b in range(2):
                clock.run(1.7, down_project, 1, b, 7, False)
            down_freed()
            gelu_freed()
            passed.update({("c", 1, DOWN), ("x", DOWN), ("z", DOWN), ("x", Q), ("x", V), ("z", Q), ("z", K), ("z", V)})
            clock.run(1.9, grad_down, 0, 1 - c, wdown.at[0])
            reduce(0, DOWN)
            clock.run(1.9, grad_down, 0, c, wdown.at[0])
            for t in range(3):
                clock.run(1.4, grad_qkv, 1, t, low)
                reduce(1, Q + t)
            clock.run(0.5, grad_qv_bias, 1)
        clock.run(0.6, grad_mlp_biases, s)
        if s == 1:
            for b in range(2):
                clock.run(0.3, keep_middle, b)
        if s == 0:
            emit_sent(0, 0)
            clock.run(1.5, weave, gb.at[0], gpre)
            emit(1, 1)
        if s == 0:
            for b in range(2):
                clock.run(0.8, relow1, 0, b, gb.at[1])
        for b in range(2):
            clock.wait(y_at[k, b], y_wait, k, b)
            clock.run(1.9, grad_middle, s, b, k)
            clock.run(0.5, grad_mixed, s, b)
            if b == 1:
                clock.run(0.9, grad_out, s)
                reduce(s, OUT)
            clock.run(3.8, grad_attention, s, b)
            clock.run(1.6, grad_lowered, s, b, k + 1)
            y_at[k + 1, b] = y_sent()
        if s == 1:
            for b in range(2):
                clock.wait(y_at[4, b], y_wait, 4, b)
                clock.run(2.2, grad_stream, 1, b, 4, gb.at[0])
                clock.run(2.7, grad_gelu, 0, b)
                clock.run(2.0, grad_low_two, 0, b, 5)
                y_at[5, b] = y_sent()
                if b == 0:
                    for q in range(2):
                        clock.run(0.5, relower, 0, q, gb.at[1])
        else:
            pl.semaphore_signal(free_y, inc=1, device_id=to_y, device_id_type=MESH)
            pl.semaphore_wait(free_y, 1)
            for b in range(2):
                for n in range(4):
                    y_start(7, b, n)
                y_at[7, b] = y_sent()
            for t in range(3):
                clock.run(1.4, grad_qkv, 0, t, gb.at[1])
                reduce(0, Q + t)
            clock.run(0.5, grad_qv_bias, 0)
    for b in range(2):
        clock.wait(y_at[6, b], y_wait, 6, b)
        clock.run(2.2, grad_stream, 0, b, 6, low)
    def vec_chain(i):
        vec_step(i)
        if i < 3:
            ready = (clock.now + 3.0, link("x", 131e3) + 1.0, link("z", 262e3) + 4.0)[i]
            clock.add(ready, functools.partial(vec_chain, i + 1), 0.5)

    vec_chain(0)
    emit_sent(1, 1)
    clock.run(2.0, weave, low, gpre)
    emit(1, 0)
    for b in range(2):
        clock.wait(y_at[7, b], y_wait, 7, b)
        clock.run(1.0, finish, 1, b, 7, gb.at[1])
    emit_sent(1, 0)
    clock.run(2.0, weave, gb.at[1], gpre)
    emit(0, 1)
    clock.drain(lambda: not clock.queue)
    for cp in vec_copies(3):
        cp.wait()
    for m in MATS:
        rs_f_sent(0, m)
    for s in range(2):
        for m in MATS:
            rs_end(s, m)
    emit_sent(0, 1)
    for which in range(2):
        for s in range(2):
            emit_got(which, s)


def run_kernel(*args):
    any_spec = pl.BlockSpec(memory_space=pl.ANY)
    V = pltpu.VMEM
    D_ = pltpu.SemaphoreType.DMA
    REG = pltpu.SemaphoreType.REGULAR
    S = jax.ShapeDtypeStruct
    mats = ((1024, 512), (1024, 512), (1024, 512), (512, 1024), (1024, 2048), (2048, 1024))
    by_rows = (True, True, True, False, True, False)
    first = (False, True, False, True, False, False)

    def halved(shape, rows, cut):
        return (shape[0] // cut, shape[1] // 2) if rows else (shape[0] // 2, shape[1] // cut)

    scratch = [V((2, 8, 32, 128), BF)]
    scratch += [V((2,) + shape, BF) for shape in mats]
    scratch += [V(halved(shape, rows, 1), BF) for shape, rows in zip(mats, by_rows)]
    scratch += [
        V((2,) + halved(shape, rows, 8) if f else halved(shape, rows, 2), BF)
        for shape, rows, f in zip(mats, by_rows, first)
    ]
    scratch += [V((8 if f else 4,) + halved(shape, rows, 8), BF) for shape, rows, f in zip(mats[:4], by_rows, first)]
    scratch += [V(halved(shape, rows, 8), F32) for shape, rows in zip(mats, by_rows)]
    scratch += [
        V((2, R, 1024), BF), V((2, 3, R, 512), BF), V((2, R, 512), BF), V((2, R, 1024), BF),
        V((2, R, 2048), BF), V((2, R, 2048), BF), V((R, 128), F32),
        V((R, 1024), BF), V((R, 1024), F32), V((2, R, 1024), BF), V((R, 2048), BF), V((3, R, 512), BF),
        V((R, 1024), BF), V((2, R, 1024), BF), V((LP, 256), F32),
        V((2, 16, 1024), F32), V((2, 16, 1024), F32), V((16, 1024), F32), V((16, 1024), F32), V((3, 16, 1024), F32),
        V((LP, 2, 1024), BF), V((1024, 1024), BF), V((32, 128), BF), V((6, 1, 128), BF), V((2, 8, 8), BF), V((8, 32), BF),
        D_((14,)), D_((14, 2)), D_((54,)), D_((44,)),
        D_((12,)), D_((12,)), D_((12,)), D_((36,)), D_((12, 2)), D_((64,)), D_((12,)), D_((12,)),
        D_((16,)), D_((16,)), D_((4,)), D_((4,)), D_((4,)), D_((10,)), D_((5,)), D_((5,)),
        REG((6,)), REG((6,)), REG((6,)), REG, REG((2,)), REG,
    ]
    return pl.pallas_call(
        kernel,
        out_shape=[
            S((2, L, 2, 1024), BF), S((2, L, 2, 1024), BF), S((3, 128, 512), F32), S((512, 128), F32),
            S((128, 2048), F32), S((2048, 128), F32), S((16, 1024), F32),
        ],
        in_specs=[any_spec] * 14 + [pl.BlockSpec(memory_space=pltpu.SMEM)],
        out_specs=[any_spec] * 7,
        scratch_shapes=scratch,
        compiler_params=pltpu.CompilerParams(
            collective_id=1, has_side_effects=True, vmem_limit_bytes=67043328
        ),
        name="sections",
    )(*args)


def local_fast(images, cotangent, live_count, ln1_gain, ln1_bias, qkv_weight, qv_bias, out_weight, out_bias,
               ln2_gain, ln2_bias, up_weight, up_bias, down_weight, down_bias):
    d = lax.axis_index("dp")

    def woven(a):
        return jnp.transpose(a, (0, 2, 1, 3))

    act, gin, gqkv, gout, gup, gdown, gvec = run_kernel(
        ln1_gain, ln1_bias, out_bias, ln2_gain, ln2_bias, down_bias, qv_bias[0], up_bias[0],
        qkv_weight[0], out_weight[0], up_weight[0], down_weight[0], woven(images), woven(cotangent), live_count.reshape(2),
    )

    def cut(v, axis, n):
        return lax.dynamic_slice_in_dim(v, d * n, n, axis=axis)

    act, gin = woven(act)[None], woven(gin)[None]
    vecs = cut(gvec[:6], 1, 128)
    qv = cut(gvec[6].reshape(2, 8, 64), 2, 8)
    upb = cut(gvec[7:9].reshape(8, 256), 1, 32)
    return (
        act, gin, vecs[0:1], vecs[1:2], gqkv[None], qv[None], gout[None], vecs[2:3], vecs[3:4], vecs[4:5],
        gup[None], upb[None], gdown[None], vecs[5:6],
    )


def solution(mesh):
    fast = dict(mesh.shape) == {"section": 2, "dp": 8, "mp": 2}
    return jax.shard_map(
        local_fast if fast else local,
        mesh=mesh,
        in_specs=(
            P(None, "dp", None, None),
            P(None, "dp", None, None),
            P(None, "dp"),
            P("section", "dp"),
            P("section", "dp"),
            P("section", None, "dp", "mp"),
            P("section", None, "mp", "dp"),
            P("section", "mp", "dp"),
            P("section", "dp"),
            P("section", "dp"),
            P("section", "dp"),
            P("section", "dp", "mp"),
            P("section", "mp", "dp"),
            P("section", "mp", "dp"),
            P("section", "dp"),
        ),
        out_specs=(
            P("section", None, "dp", None, None),
            P("section", None, "dp", None, None),
            P("section", "dp"),
            P("section", "dp"),
            P("section", None, "dp", "mp"),
            P("section", None, "mp", "dp"),
            P("section", "mp", "dp"),
            P("section", "dp"),
            P("section", "dp"),
            P("section", "dp"),
            P("section", "dp", "mp"),
            P("section", "mp", "dp"),
            P("section", "mp", "dp"),
            P("section", "dp"),
        ),
        check_vma=False,
    )
```

```python
import functools
import heapq
import math

import jax
import jax.numpy as jnp
from jax import lax
from jax.experimental import pallas as pl
from jax.experimental.pallas import tpu as pltpu
from jax.sharding import PartitionSpec as P

HD = 64


epsilon = 1e-06


def gather_all(small, big):
    flat = jnp.concatenate([piece.reshape(-1) for piece in small])
    packed = lax.all_gather(flat, "dp", axis=0, tiled=False)
    count = packed.shape[0]
    whole, offset = [], 0
    for piece, axis in zip(small, (1, 1, 3, 1, 1, 1, 2, 1)):
        part = packed[:, offset : offset + piece.size].reshape((count,) + piece.shape)
        offset += piece.size
        part = jnp.moveaxis(part, 0, axis)
        shape = list(piece.shape)
        shape[axis] *= count
        whole.append(part.reshape(shape))
    qkv, out, up, down = (
        lax.all_gather(piece, "dp", axis=axis, tiled=True) for piece, axis in zip(big, (2, 2, 1, 2))
    )
    return (
        whole[0],
        whole[1],
        qkv,
        whole[2],
        out,
        whole[3],
        whole[4],
        whole[5],
        up,
        whole[6],
        down,
        whole[7],
    )


def scatter_all(totals, shards):
    small_at = (0, 1, 3, 5, 6, 7, 9, 11)
    count = lax.axis_size("dp")
    rows = []
    for index, axis in zip(small_at, (1, 1, 3, 1, 1, 1, 2, 1)):
        piece = totals[index]
        shape = list(piece.shape)
        shape[axis : axis + 1] = [count, shape[axis] // count]
        rows.append(jnp.moveaxis(piece.reshape(shape), axis, 0).reshape(count, -1))
    packed = lax.psum_scatter(jnp.concatenate(rows, axis=1), "dp", scatter_dimension=0, tiled=False)
    owned, offset = [None] * 12, 0
    for index in small_at:
        size = shards[index].size
        owned[index] = packed[offset : offset + size].reshape(shards[index].shape)
        offset += size
    for index, axis in zip((2, 4, 8, 10), (2, 2, 1, 2)):
        owned[index] = lax.psum_scatter(
            totals[index].astype(jnp.bfloat16), "dp", scatter_dimension=axis, tiled=True
        ).astype(jnp.float32)
    return owned


def both_halves(partial):
    return lax.psum(partial.astype(jnp.bfloat16), "mp").astype(jnp.float32)


def from_behind(x, axis, by):
    length = lax.axis_size(axis)
    pairs = [(i, i + by) for i in range(length) if 0 <= i + by < length]
    return lax.ppermute(x, axis, pairs)


def norm_parts(stream):
    centered = stream - jnp.mean(stream, axis=-1, keepdims=True)
    inverse = lax.rsqrt(jnp.mean(centered * centered, axis=-1, keepdims=True) + epsilon)
    return (centered * inverse, inverse)


def norm_back(grad_normed, normed, inverse):
    first_mean = jnp.mean(grad_normed, axis=-1, keepdims=True)
    second_mean = jnp.mean(grad_normed * normed, axis=-1, keepdims=True)
    return inverse * (grad_normed - first_mean - normed * second_mean)


def gelu_slope(preact):
    cumul = 0.5 * (1.0 + lax.erf(preact * 2.0 ** (-0.5)))
    density = jnp.exp(-0.5 * preact * preact) * (2.0 * math.pi) ** (-0.5)
    return cumul + preact * density


def unpack_weights(whole):
    return (
        whole[0][0].astype(jnp.float32),
        whole[1][0].astype(jnp.float32),
        whole[2][0],
        whole[3][0].reshape(2, -1).astype(jnp.float32),
        whole[4][0],
        whole[5][0].astype(jnp.float32),
        whole[6][0].astype(jnp.float32),
        whole[7][0].astype(jnp.float32),
        whole[8][0],
        whole[9][0].reshape(-1).astype(jnp.float32),
        whole[10][0],
        whole[11][0].astype(jnp.float32),
    )


def forward(stream, params, rows):
    (
        gain_one,
        shift_one,
        qkv_mat,
        qv_shift,
        out_mat,
        out_shift,
        gain_two,
        shift_two,
        up_mat,
        up_shift,
        down_mat,
        down_shift,
    ) = params
    batch_size, seq_len, model_width = stream.shape
    head_count = qkv_mat.shape[2] // HD
    scale = HD ** (-0.5)
    normed, inverse = norm_parts(stream)
    lowered = (normed * gain_one + shift_one).astype(jnp.bfloat16)
    projected = jnp.einsum("bld,cde->cble", lowered, qkv_mat, preferred_element_type=jnp.float32)
    split_shape = (batch_size, seq_len, head_count, HD)
    queries = (projected[0] + qv_shift[0]).astype(jnp.bfloat16).reshape(split_shape)
    keys_low = projected[1].astype(jnp.bfloat16).reshape(split_shape)
    values_low = (projected[2] + qv_shift[1]).astype(jnp.bfloat16).reshape(split_shape)
    scores = (
        jnp.einsum("blhe,bmhe->bhlm", queries, keys_low, preferred_element_type=jnp.float32) * scale
    )
    row_max = jnp.max(scores, axis=-1, keepdims=True)
    log_total = row_max + jnp.log(jnp.sum(jnp.exp(scores - row_max), axis=-1, keepdims=True))
    attn_probs = jnp.exp(scores - log_total)
    mixed = jnp.einsum(
        "bhlm,bmhe->blhe",
        attn_probs.astype(jnp.bfloat16),
        values_low,
        preferred_element_type=jnp.float32,
    )
    mixed = mixed.astype(jnp.bfloat16).reshape(batch_size, seq_len, -1)
    partial_attn = jnp.einsum("bld,de->ble", mixed, out_mat, preferred_element_type=jnp.float32)
    middle = stream + both_halves(partial_attn) + out_shift
    normed_two, inverse_two = norm_parts(middle)
    lowered_two = (normed_two * gain_two + shift_two).astype(jnp.bfloat16)
    preact = (
        jnp.einsum("bld,df->blf", lowered_two, up_mat, preferred_element_type=jnp.float32)
        + up_shift
    )
    gelu_out = jax.nn.gelu(preact, approximate=False).astype(jnp.bfloat16)
    partial_mlp = jnp.einsum("blf,fd->bld", gelu_out, down_mat, preferred_element_type=jnp.float32)
    result = (middle + both_halves(partial_mlp) + down_shift) * rows
    return (result, (stream, middle, queries, keys_low, values_low, log_total, mixed, preact))


def backward(seed, saved, params, shapes):
    (
        gain_one,
        shift_one,
        qkv_mat,
        qv_shift,
        out_mat,
        out_shift,
        gain_two,
        shift_two,
        up_mat,
        up_shift,
        down_mat,
        down_shift,
    ) = params
    stream, middle, queries, keys_low, values_low, log_total, mixed, preact = saved
    batch_size, seq_len, head_count, head_dim = queries.shape
    scale = HD ** (-0.5)
    normed, inverse = norm_parts(stream)
    lowered = (normed * gain_one + shift_one).astype(jnp.bfloat16)
    normed_two, inverse_two = norm_parts(middle)
    lowered_two = (normed_two * gain_two + shift_two).astype(jnp.bfloat16)
    gelu_out = jax.nn.gelu(preact, approximate=False).astype(jnp.bfloat16)
    grad_mlp = seed.astype(jnp.bfloat16)
    grad_down_shift = jnp.sum(grad_mlp.astype(jnp.float32), axis=(0, 1))
    grad_down_mat = jnp.einsum(
        "blf,bld->fd", gelu_out, grad_mlp, preferred_element_type=jnp.float32
    )
    grad_gelu = jnp.einsum("bld,fd->blf", grad_mlp, down_mat, preferred_element_type=jnp.float32)
    grad_pre = (grad_gelu * gelu_slope(preact)).astype(jnp.bfloat16)
    grad_up_shift = jnp.sum(grad_pre.astype(jnp.float32), axis=(0, 1))
    grad_up_mat = jnp.einsum(
        "bld,blf->df", lowered_two, grad_pre, preferred_element_type=jnp.float32
    )
    grad_low_two = both_halves(
        jnp.einsum("blf,df->bld", grad_pre, up_mat, preferred_element_type=jnp.float32)
    )
    grad_gain_two = jnp.sum(grad_low_two * normed_two, axis=(0, 1))
    grad_shift_two = jnp.sum(grad_low_two, axis=(0, 1))
    grad_middle = seed + norm_back(grad_low_two * gain_two, normed_two, inverse_two)
    grad_attn = grad_middle.astype(jnp.bfloat16)
    grad_out_shift = jnp.sum(grad_attn.astype(jnp.float32), axis=(0, 1))
    grad_out_mat = jnp.einsum("bld,ble->de", mixed, grad_attn, preferred_element_type=jnp.float32)
    grad_mixed = jnp.einsum("ble,de->bld", grad_attn, out_mat, preferred_element_type=jnp.float32)
    grad_mixed = grad_mixed.astype(jnp.bfloat16).reshape(batch_size, seq_len, head_count, head_dim)
    scores = (
        jnp.einsum("blhe,bmhe->bhlm", queries, keys_low, preferred_element_type=jnp.float32) * scale
    )
    attn_probs = jnp.exp(scores - log_total)
    grad_probs = jnp.einsum(
        "blhe,bmhe->bhlm", grad_mixed, values_low, preferred_element_type=jnp.float32
    )
    grad_values = jnp.einsum(
        "bhlm,blhe->bmhe",
        attn_probs.astype(jnp.bfloat16),
        grad_mixed,
        preferred_element_type=jnp.float32,
    ).astype(jnp.bfloat16)
    grad_scores = (
        attn_probs * (grad_probs - jnp.sum(attn_probs * grad_probs, axis=-1, keepdims=True))
    ).astype(jnp.bfloat16)
    grad_queries = (
        jnp.einsum("bhlm,bmhe->blhe", grad_scores, keys_low, preferred_element_type=jnp.float32)
        * scale
    ).astype(jnp.bfloat16)
    grad_keys = (
        jnp.einsum("bhlm,blhe->bmhe", grad_scores, queries, preferred_element_type=jnp.float32)
        * scale
    ).astype(jnp.bfloat16)
    grad_proj = jnp.stack([grad_queries, grad_keys, grad_values]).reshape(
        3, batch_size, seq_len, -1
    )
    grad_qv_shift = jnp.stack(
        [
            jnp.sum(grad_queries.astype(jnp.float32), axis=(0, 1)),
            jnp.sum(grad_values.astype(jnp.float32), axis=(0, 1)),
        ]
    )
    grad_qkv_mat = jnp.einsum(
        "bld,cble->cde", lowered, grad_proj, preferred_element_type=jnp.float32
    )
    grad_lowered = both_halves(
        jnp.einsum("cble,cde->bld", grad_proj, qkv_mat, preferred_element_type=jnp.float32)
    )
    grad_gain_one = jnp.sum(grad_lowered * normed, axis=(0, 1))
    grad_shift_one = jnp.sum(grad_lowered, axis=(0, 1))
    grad_stream = grad_middle + norm_back(grad_lowered * gain_one, normed, inverse)
    terms = [
        grad_gain_one,
        grad_shift_one,
        grad_qkv_mat,
        grad_qv_shift,
        grad_out_mat,
        grad_out_shift,
        grad_gain_two,
        grad_shift_two,
        grad_up_mat,
        grad_up_shift,
        grad_down_mat,
        grad_down_shift,
    ]
    return (grad_stream, [term.reshape(shape) for term, shape in zip(terms, shapes)])


def local(
    images,
    cotangent,
    live_count,
    ln1_gain,
    ln1_bias,
    qkv_weight,
    qv_bias,
    out_weight,
    out_bias,
    ln2_gain,
    ln2_bias,
    up_weight,
    up_bias,
    down_weight,
    down_bias,
):
    first_section = lax.axis_index("section") == 0
    micro_count = images.shape[0]
    slot_count = images.shape[1]
    slot_ids = jnp.arange(slot_count)
    small = (ln1_gain, ln1_bias, qv_bias, out_bias, ln2_gain, ln2_bias, up_bias, down_bias)
    gathered = gather_all(small, (qkv_weight, out_weight, up_weight, down_weight))
    params = unpack_weights(gathered)
    shapes = [piece.shape for piece in gathered]

    def row_mask(batch_index, valid):
        alive = jnp.logical_and(slot_ids < live_count[batch_index, 0], valid)
        return alive.astype(jnp.float32).reshape(slot_count, 1, 1)

    def choose(for_first, for_second):
        return jnp.where(first_section, for_first, for_second)

    incoming = jnp.zeros(images.shape[1:], jnp.bfloat16)
    outputs = []
    kept = []
    for moment in range(micro_count + 1):
        own = images[min(moment, micro_count - 1)]
        source = choose(own, incoming).astype(jnp.float32)
        rows = choose(
            row_mask(min(moment, micro_count - 1), moment < micro_count),
            row_mask(max(moment - 1, 0), moment >= 1),
        )
        result, saved = forward(source, params, rows)
        result = result.astype(jnp.bfloat16)
        outputs.append(result)
        kept.append(saved)
        if moment < micro_count:
            incoming = from_behind(result, "section", 1)
    activations = jnp.stack(
        [choose(outputs[index], outputs[index + 1]) for index in range(micro_count)]
    )
    totals = [jnp.zeros(shape, jnp.float32) for shape in shapes]
    incoming = jnp.zeros(images.shape[1:], jnp.bfloat16)
    returned = []
    for moment in range(micro_count + 1):
        later_index = min(moment, micro_count - 1)
        rows = choose(
            row_mask(max(moment - 1, 0), moment >= 1), row_mask(later_index, moment < micro_count)
        )
        seed = choose(incoming, cotangent[later_index]).astype(jnp.float32) * rows
        saved = jax.tree.map(choose, kept[max(moment - 1, 0)], kept[min(moment + 1, micro_count)])
        grad_stream, terms = backward(seed, saved, params, shapes)
        grad_low = grad_stream.astype(jnp.bfloat16)
        returned.append(grad_low)
        if moment < micro_count:
            incoming = from_behind(grad_low, "section", -1)
        totals = [first_part + second_part for first_part, second_part in zip(totals, terms)]
    shards = (
        ln1_gain,
        ln1_bias,
        qkv_weight,
        qv_bias,
        out_weight,
        out_bias,
        ln2_gain,
        ln2_bias,
        up_weight,
        up_bias,
        down_weight,
        down_bias,
    )
    owned = scatter_all(totals, shards)
    input_grads = jnp.stack(
        [choose(returned[index + 1], returned[index]) for index in range(micro_count)]
    )
    return (
        activations[None],
        input_grads[None],
        owned[0],
        owned[1],
        owned[2],
        owned[3],
        owned[4],
        owned[5],
        owned[6],
        owned[7],
        owned[8],
        owned[9],
        owned[10],
        owned[11],
    )


MESH = pl.DeviceIdType.MESH
BF = jnp.bfloat16
F32 = jnp.float32
Z = 4
EPS = 1e-06
L = 197
LP = 208
R = 2 * LP
SMALL, Q, K, V, OUT, UP, DOWN = range(7)
MATS = (Q, K, V, OUT, UP, DOWN)
BY_ROWS = (Q, K, V, UP)
X_FIRST = (K, OUT)
Z_FIRST = ((1, K), (1, OUT), (0, OUT))
WIDTH = {Q: 512, K: 512, V: 512, OUT: 512, UP: 2048, DOWN: 2048}
SELF, NEAR, INNER, FAR = range(4)


class Clock:
    def __init__(self):
        self.now, self.queue, self.count = 0.0, [], 0

    def add(self, ready, step, cost=0.2):
        heapq.heappush(self.queue, (ready, self.count, cost, step))
        self.count += 1

    def pop(self):
        ready, _, cost, step = heapq.heappop(self.queue)
        self.now = max(self.now, ready)
        step()
        self.now += cost

    def flush(self, until):
        while self.queue and self.queue[0][0] <= until:
            self.pop()

    def run(self, cost, step, *args):
        self.flush(self.now)
        step(*args)
        self.now += cost

    def wait(self, until, step, *args):
        self.flush(until)
        self.now = max(self.now, until)
        step(*args)

    def drain(self, done):
        while not done():
            self.pop()


def lanes(d, n=128):
    return pl.ds(pl.multiple_of(d * 128, 128), n)


def dot(a, b, ca, cb):
    return lax.dot_general(a, b, (((ca,), (cb,)), ((), ())), preferred_element_type=F32)


def half(m, ref, s, h):
    n = WIDTH[m] // 2
    at = pl.ds(pl.multiple_of(h * n, n), n)
    return ref.at[s, :, at] if m in BY_ROWS else ref.at[s, at, :]


def block(m, ref, s, d, h=None):
    if m == SMALL:
        return ref.at[s, d] if h is None else ref.at[s, d, pl.ds(h * 16, 16), :]
    own = pl.ds(pl.multiple_of(d * 128, 128), 128)
    n = WIDTH[m] // 2
    other = pl.ds(0, 2 * n) if h is None else pl.ds(pl.multiple_of(h * n, n), n)
    return ref.at[s, own, other] if m in BY_ROWS else ref.at[s, other, own]


def kernel(
    gain1_ref, shift1_ref, bias_o_ref, gain2_ref, shift2_ref, bias_d_ref, qv_ref, upb_ref,
    qkv_ref, out_ref, up_ref, down_ref, x_ref, cot_ref, live_ref,
    act_out, gin_out, gqkv_out, gout_out, gup_out, gdown_out, gvec_out, gqv_out, gupb_out,
    wsmall, wq, wk, wv, wout, wup, wdown,
    rq, rk, rv, rout, rup, rdown, xq, xk, xv, xout, xup, xdown,
    zq, zk, zv, zout, fq, fk, fv, fout, fup, fdown,
    xs, qkvs, mixs, nrm2s, gels, slps, stats,
    low, mid, gb, gpre, gqkv, ys, yr, acc, vec, sv, svc, svx, svz, woven, stage, pack, raw, rawq, rawu, vq, vu,
    asem_s, asem_c, asem_z, asem_x, rsem_cs, rsem_c, rsem_xs, rsem_x, rsem_zs, rsem_z, rsem_fs, rsem_f,
    ysem, ysem_s, osem, osem_r, osem_s, isem, vsem, vsem_s, free_c, free_x, free_z, free_up, free_r, free_y,
):
    shards = (pack, qkv_ref.at[0], qkv_ref.at[1], qkv_ref.at[2], out_ref, up_ref, down_ref)
    wqkv = (wq, wk, wv)
    w = (wsmall, wq, wk, wv, wout, wup, wdown)
    rbuf = (None, rq, rk, rv, rout, rup, rdown)
    xbuf = (None, xq, xk, xv, xout, xup, xdown)
    zbuf = (None, zq, zk, zv, zout)
    fbuf = (None, fq, fk, fv, fout, fup, fdown)

    c = lax.axis_index("section")
    me = lax.axis_index("dp")
    y = lax.axis_index("mp")
    z, x = me // 2, lax.rem(me, 2)
    to_x = {"dp": z * 2 + 1 - x}
    to_c = {"section": 1 - c}
    to_y = {"mp": 1 - y}

    inner = jnp.logical_or(z == 1, z == 2)
    near = z + 1 - 2 * lax.rem(z, 2)
    lower = (z < 2).astype(jnp.int32)
    places = (z, near, 1 + lower, 3 * lower)
    inner_i = jnp.where(inner, 1, 0)

    def at_dp(k, col):
        return places[k] * 2 + (x if col == 0 else 1 - x)

    def to_z(zi):
        return {"dp": zi * 2 + x}

    def remote(a, b, ss, rs, dev):
        return pltpu.make_async_remote_copy(
            src_ref=a, dst_ref=b, send_sem=ss, recv_sem=rs, device_id=dev, device_id_type=MESH
        )

    barrier = pltpu.get_barrier_semaphore()
    for dev in [to_z(places[k]) for k in (NEAR, INNER, FAR)] + [to_x, to_c, to_y]:
        pl.semaphore_signal(barrier, inc=1, device_id=dev, device_id_type=MESH)
    pl.semaphore_wait(barrier, Z + 2)

    def number(per):
        table = {}
        for key, count in per:
            for i in range(count):
                table[key, i] = len(table)
        return table

    pieces = [(s, m) for s in range(2) for m in range(7)]
    az = number((p, 6 if p[1] in X_FIRST else 3) for p in pieces)
    ax = number((p, 1 if p[1] in X_FIRST else 4) for p in pieces)
    rz = number((p, 8 if p in Z_FIRST else 4) for p in pieces if p[1])
    rx = number((p, 1 if p in Z_FIRST else 4) for p in pieces if p[1])

    def wait_bytes(m, count, sem):
        if m == SMALL:
            v = stats.at[pl.ds(0, 8 * count), :]
        else:
            v = wdown.at[:, pl.ds(0, count * WIDTH[m] // 32), :]
        pltpu.make_async_copy(v, v, sem).wait()

    def ag_share(s, m):
        p = s * 7 + m

        @pl.when(c == s)
        def _():
            dst = block(m, w[m], s, me)
            remote(shards[m], dst, asem_s.at[p], asem_c.at[p, 0], to_c).start()
            pltpu.make_async_copy(shards[m], dst, asem_c.at[p, 0]).start()

    def ag_shared(s, m):
        whole = block(m, w[m], s, me)
        pltpu.make_async_copy(whole, whole, asem_c.at[s * 7 + m, 0]).wait()

    def ag_own_z(s, m, col):
        p, first = s * 7 + m, az[(s, m), col * 3]
        b = block(m, w[m], s, at_dp(SELF, col), c)
        slot = jnp.where(inner, INNER, FAR) - 1
        remote(b, b, asem_s.at[p], asem_z.at[first], to_z(near)).start()
        remote(b, b, asem_s.at[p], asem_z.at[first + slot], to_z(places[INNER])).start()

    def ag_to_x(s, m, k):
        b = block(m, w[m], s, at_dp(k, 0), c)
        remote(b, b, asem_s.at[s * 7 + m], asem_x.at[ax[(s, m), k]], to_x).start()

    def ag_to_c(s, m, k, col):
        p = s * 7 + m
        b = block(m, w[m], s, at_dp(k, col), c)
        remote(b, b, asem_s.at[p], asem_c.at[p, 1], to_c).start()

    def ag_z(s, m, k, col):
        b = block(m, w[m], s, at_dp(k, col), c)
        cp = remote(b, b, asem_s.at[s * 7 + m], asem_z.at[az[(s, m), col * 3 + k - 1]], to_z(near))
        cp.wait_recv()
        if k != NEAR:

            @pl.when(inner)
            def _():
                cp.start()

        if m not in X_FIRST:
            ag_to_x(s, m, k)
        ag_to_c(s, m, k, col)

    def ag_x(s, m, k):
        b = block(m, w[m], s, at_dp(k, 1), c)
        remote(b, b, asem_s.at[s * 7 + m], asem_x.at[ax[(s, m), k]], to_x).wait_recv()
        if m in X_FIRST:
            ag_own_z(s, m, 1)
        ag_to_c(s, m, k, 1)

    def ag_need(s, m):
        wait_bytes(m, 7, asem_c.at[s * 7 + m, 1])

    def ag_sent(s, m):
        count = 7 + (1 + 4 if m in X_FIRST else 4 + 2)
        extra = 4 if m in X_FIRST else 2
        for ins in range(2):
            for own in range(2):

                @pl.when(jnp.logical_and(inner_i == ins, jnp.where(c == s, 1, 0) == own))
                def _():
                    wait_bytes(m, count + extra * ins + 2 * own, asem_s.at[s * 7 + m])

    def rows_of(b):
        return pl.ds(b * LP, LP)

    def y_src(k):
        return slps.at[1, :, pl.ds(0, 1024)] if k == 7 else ys

    def y_start(k, b, n):
        cols = lanes(n * 2, 256)
        src = y_src(k).at[rows_of(b), cols]
        remote(src, yr.at[k % 2, rows_of(b), cols], ysem_s.at[k * 2 + b], ysem.at[k * 2 + b], to_y).start()

    def y_wait(k, b):
        src = y_src(k).at[rows_of(b), pl.ds(0, 1024)]
        cp = remote(src, yr.at[k % 2, rows_of(b), :], ysem_s.at[k * 2 + b], ysem.at[k * 2 + b], to_y)
        cp.wait_recv()
        cp.wait_send()

    def y_sum(k, rows):
        return y_src(k)[rows, :].astype(F32) + yr[k % 2, rows, :].astype(F32)

    small_in = [
        pltpu.make_async_copy(ref, raw.at[i], isem.at[2 + i])
        for i, ref in enumerate((gain1_ref, shift1_ref, bias_o_ref, gain2_ref, shift2_ref, bias_d_ref))
    ] + [pltpu.make_async_copy(qv_ref, rawq, isem.at[8]), pltpu.make_async_copy(upb_ref, rawu, isem.at[9])]

    def pack_small():
        for cp in small_in:
            cp.wait()

        def iota(shape, axis):
            return lax.broadcasted_iota(jnp.int32, shape, axis)

        def hot(test):
            return jnp.where(test, 1.0, 0.0).astype(BF)

        r = iota((32, 128), 0)
        v = jnp.zeros((32, 128), F32)
        for i in range(6):
            v = jnp.where(r == i, raw[i].astype(F32), v)
        for t in range(2):
            for e in range(2):
                pick_rows = hot(iota((32, 8), 1) == 2 * (iota((32, 8), 0) - 6 - 4 * t) + e)
                spread = hot(iota((8, 128), 1) == e * 64 + me * 8 + iota((8, 128), 0))
                rows = dot(pick_rows, rawq[t], 1, 0).astype(BF)
                v = v + dot(rows, spread, 1, 0)
        odd = me // 4
        pick_rows = hot(2 * iota((32, 8), 1) + odd == iota((32, 8), 0) - 14)
        spread = hot(iota((32, 128), 1) == lax.rem(me, 4) * 32 + iota((32, 128), 0))
        v = v + dot(dot(pick_rows, rawu[...], 1, 0).astype(BF), spread, 1, 0)
        pack[...] = v.astype(BF)

    def unpack_small(s):
        total = jnp.zeros((32, 128), F32)
        for d in range(2 * Z):
            piece = wsmall[s, d].astype(F32)
            total = total + piece
            for r in range(6):
                vec[s, r : r + 1, d * 128 : d * 128 + 128] = piece[r : r + 1, :]
        for k in range(8):
            vec[s, 6:7, k * 128 : k * 128 + 128] = total[6 + k : 7 + k, :]
            vec[s, 7:8, k * 128 : k * 128 + 128] = total[14 + k : 15 + k, :]
            vec[s, 8:9, k * 128 : k * 128 + 128] = total[22 + k : 23 + k, :]

    def row(s, r):
        return vec[s, r : r + 1, :]

    CH = 16

    lane = lax.broadcasted_iota(jnp.int32, (1, 128), 1)
    left = lane < 64
    live_col = lax.broadcasted_iota(jnp.int32, (1, LP), 1) < L
    INV2, MEAN1, INV1 = range(3)

    def stat_at(s, which):
        return 16 + 4 * s + which

    def put_stats(rows, *pairs):
        v = stats[rows, :]
        for at, value in pairs:
            v = jnp.where(lane == at, value, v)
        stats[rows, :] = v

    def stat(s, which, rows):
        at = stat_at(s, which)
        return stats[rows, :][:, at : at + 1]

    def norm_chunk(v):
        mean = jnp.mean(v, axis=-1, keepdims=True)
        cen = v - mean
        inv = lax.rsqrt(jnp.mean(cen * cen, axis=-1, keepdims=True) + EPS)
        return cen * inv, mean, inv

    def chunks(b, pair=1):
        def at(i):
            return pl.ds(pl.multiple_of(b * LP + i * CH, CH), CH)

        def wrap(body):
            count = LP // CH

            @pl.loop(0, count // pair)
            def _(i):
                for j in range(pair):
                    body(at(i * pair + j))

            for j in range(count % pair):
                body(at(count - 1 - j))

        return wrap

    def ln1(s, b):
        gain, shift = row(s, 0), row(s, 1)

        @chunks(b, 2)
        def _(rows):
            nrm, mean, inv = norm_chunk(xs[s, rows, :].astype(F32))
            put_stats(rows, (stat_at(s, MEAN1), mean), (stat_at(s, INV1), inv))
            low[rows, :] = (nrm * gain + shift).astype(BF)

    def norm1(s, rows):
        return (xs[s, rows, :].astype(F32) - stat(s, MEAN1, rows)) * stat(s, INV1, rows)

    def relow1(s, b, dst):
        gain, shift = row(s, 0), row(s, 1)

        @chunks(b)
        def _(rows):
            dst[rows, :] = (norm1(s, rows) * gain + shift).astype(BF)

    def load_woven(ref, sem, dst):
        cp = pltpu.make_async_copy(ref.at[c], woven.at[pl.ds(0, L)], sem)
        cp.start()
        cp.wait()
        woven[L:LP] = jnp.zeros((LP - L, 2, 1024), BF)

        @pl.loop(0, LP // 16)
        def _(i):
            dst[pl.ds(pl.multiple_of(i * 32, 32), 32), 0:1024] = woven[pl.ds(i * 16, 16)].reshape(32, 1024)

    def unweave(src, dst, b, alive):
        r = lax.broadcasted_iota(jnp.int32, (LP, R), 0)
        q = lax.broadcasted_iota(jnp.int32, (LP, R), 1)
        take = jnp.where(q == 2 * r + b, 1.0, 0.0)
        if alive is not None:
            take = take * alive
        take = take.astype(BF)

        @pl.loop(0, 4)
        def _(n):
            cols = lanes(n * 2, 256)
            dst[rows_of(b), cols] = dot(take, src[:, cols], 1, 0).astype(BF)

    def weave(src, tmp):
        r = lax.broadcasted_iota(jnp.int32, (R, R), 0)
        q = lax.broadcasted_iota(jnp.int32, (R, R), 1)
        put = jnp.where(q == lax.rem(r, 2) * LP + r // 2, 1.0, 0.0).astype(BF)

        @pl.loop(0, 4)
        def _(n):
            cols = lanes(n * 2, 256)
            tmp[:, cols] = dot(put, src[:, cols], 1, 0).astype(BF)

        @pl.loop(0, LP // 16)
        def _(i):
            woven[pl.ds(i * 16, 16)] = tmp[pl.ds(pl.multiple_of(i * 32, 32), 32), 0:1024].reshape(16, 2, 1024)

    def alive_of(b):
        return jnp.where(live_ref[c] > b, 1.0, 0.0)

    def project(s, b):
        for t in range(3):
            @pl.loop(0, 2)
            def _(n):
                cols = lanes(n * 2, 256)
                a = dot(low[rows_of(b), :], wqkv[t][s, :, cols], 1, 0)
                if t != 1:
                    base = 0 if t == 0 else 512
                    a = a + vec[s, 6:7, pl.ds(pl.multiple_of(base + n * 256, 256), 256)]
                qkvs[s, t, rows_of(b), cols] = a.astype(BF)

    def pick(h, v):
        return jnp.where(left if h == 0 else jnp.logical_not(left), v, jnp.zeros_like(v))

    def scores(q, k):
        return jnp.where(live_col, dot(q, k, 1, 1), -1e30)

    def attention(s, b):
        rows = rows_of(b)

        @pl.loop(0, 4)
        def _(i):
            cols = lanes(i)
            q, k, v = (qkvs[s, t, rows, cols] for t in range(3))
            q = q * jnp.asarray(0.125, BF)
            ones = jnp.ones_like(v)
            tops, parts = [], []
            for h in range(2):
                sc = scores(pick(h, q), k)
                tops.append(jnp.max(sc, axis=-1, keepdims=True))
                e = jnp.exp(sc - tops[h]).astype(BF)
                parts.append(dot(e, jnp.where(left, v, ones) if h == 0 else jnp.where(left, ones, v), 1, 0))
            den = pltpu.roll(jnp.where(left, parts[1], parts[0]), 64, 1)
            mixs[s, rows, cols] = (jnp.where(left, parts[0], parts[1]) / den).astype(BF)
            lse = jnp.where(left, tops[0], tops[1]) + jnp.log(den)
            stats[rows, :] = jnp.where(lax.rem(lane, 64) == 8 * s + i, lse, stats[rows, :])

    def out_project(s, b, k):
        @pl.loop(0, 4)
        def _(n):
            cols = lanes(n * 2, 256)
            ys[rows_of(b), cols] = dot(mixs[s, rows_of(b), :], wout[s, :, cols], 1, 0).astype(BF)
            y_start(k, b, n)

    def middle(s, b, k):
        shift, gain2, shift2 = row(s, 2), row(s, 3), row(s, 4)

        @chunks(b, 2)
        def _(rows):
            v = xs[s, rows, :].astype(F32) + y_sum(k, rows) + shift
            if s == 0:
                mid[rows, :] = v
            else:
                gb[0, rows, :] = v.astype(BF)
            nrm, _, inv = norm_chunk(v)
            nrm2s[s, rows, :] = nrm.astype(BF)
            put_stats(rows, (stat_at(s, INV2), inv))
            low[rows, :] = (nrm * gain2 + shift2).astype(BF)

    def up_project(s, b):
        @pl.loop(0, 8)
        def _(n):
            cols = lanes(n * 2, 256)
            acc[...] = dot(low[rows_of(b), :], wup[s, :, cols], 1, 0)
            at = pl.ds(pl.multiple_of(lax.rem(n, 4) * 256, 256), 256)
            bias = jnp.where(n < 4, vec[s, 7:8, at], vec[s, 8:9, at])

            @pl.loop(0, LP // 16)
            def _(i):
                rows = pl.ds(pl.multiple_of(b * LP + i * 16, 16), 16)
                a = acc[pl.ds(pl.multiple_of(i * 16, 16), 16), :] + bias
                phi = 0.5 * (1.0 + lax.erf(a * (2.0 ** -0.5)))
                dens = jnp.exp(-0.5 * a * a) * ((2.0 * math.pi) ** -0.5)
                gels[s, rows, cols] = (a * phi).astype(BF)
                slps[s, rows, cols] = (phi + a * dens).astype(BF)

    def down_project(s, b, k, send):
        @pl.loop(0, 4)
        def _(n):
            cols = lanes(n * 2, 256)
            y_src(k)[rows_of(b), cols] = dot(gels[s, rows_of(b), :], wdown[s, :, cols], 1, 0).astype(BF)
            if send:
                y_start(k, b, n)

    def finish(s, b, k, dst):
        shift, alive = row(s, 5), alive_of(b)

        @chunks(b)
        def _(rows):
            base = mid[rows, :] if s == 0 else slps[1, rows, 1024:2048].astype(F32)
            dst[rows, :] = ((base + y_sum(k, rows) + shift) * alive).astype(BF)

    def keep_middle(b):
        @chunks(b)
        def _(rows):
            slps[1, rows, 1024:2048] = gb[0, rows, :]

    def emit_copies(which, s):
        target = (act_out, gin_out)[which].at[c]
        src, q = woven.at[pl.ds(0, L)], which * 2 + s
        return pltpu.make_async_copy(src, target, osem.at[q]), remote(src, target, osem_s.at[q], osem_r.at[q], to_c)

    def emit(which, s):
        here, there = emit_copies(which, s)

        @pl.when(c == s)
        def _():
            here.start()

        @pl.when(c != s)
        def _():
            there.start()

    def emit_sent(which, s):
        here, there = emit_copies(which, s)

        @pl.when(c == s)
        def _():
            here.wait()

        @pl.when(c != s)
        def _():
            there.wait_send()

    def emit_got(which, s):
        @pl.when(c == s)
        def _():
            remote(
                woven.at[pl.ds(0, L)], (act_out, gin_out)[which].at[1 - c], osem_s.at[which * 2 + s], osem_r.at[which * 2 + s], to_c
            ).wait_recv()

    def relower(s, b, dst):
        gain2, shift2 = row(s, 3), row(s, 4)

        @chunks(b)
        def _(rows):
            dst[rows, :] = (nrm2s[s, rows, :].astype(F32) * gain2 + shift2).astype(BF)

    def fold8(v):
        return jnp.sum(v.reshape(v.shape[0] // 8, 8, v.shape[1]), axis=0)

    def colsum(v):
        return jnp.sum(v, axis=0, keepdims=True)

    def sum_rows(ref_slice, width):
        def step(i, tot):
            rows = pl.ds(pl.multiple_of(i * 32, 32), 32)
            return tot + fold8(ref_slice(rows).astype(F32))

        return colsum(lax.fori_loop(0, R // 32, step, jnp.zeros((8, width), F32)))

    def total(s, r, b, v):
        sv[s, r : r + 1, :] = v if b == 0 else sv[s, r : r + 1, :] + v

    def grad_gelu(s, b):
        @pl.loop(0, 8)
        def _(n):
            cols = lanes(n * 2, 256)
            rows_w = pl.ds(pl.multiple_of(n * 256, 256), 256)
            a = dot(gb[s, rows_of(b), :], wdown[s, rows_w, :], 1, 1)
            gpre[rows_of(b), cols] = (a * slps[s, rows_of(b), cols].astype(F32)).astype(BF)

    def grad_mlp_biases(s):
        sv[s, 5:6, :] = sum_rows(lambda r: gb[s, r, :], 1024)
        sv[s, 7:8, :] = sum_rows(lambda r: gpre[r, 0:1024], 1024)
        sv[s, 8:9, :] = sum_rows(lambda r: gpre[r, 1024:2048], 1024)

    def grad_down(s, h, dst):
        @pl.loop(0, 4)
        def _(i):
            first = h * 1024 + i * 256
            cols = pl.ds(pl.multiple_of(first, 256), 256)
            rows_w = pl.ds(pl.multiple_of(i * 256 if s == 1 else first, 256), 256)
            dst[rows_w, :] = dot(gels[s, :, cols], gb[s], 0, 0).astype(BF)

    def grad_low_two(s, b, k):
        @pl.loop(0, 4)
        def _(n):
            cols = lanes(n * 2, 256)
            rows_w = pl.ds(pl.multiple_of(n * 256, 256), 256)
            ys[rows_of(b), cols] = dot(gpre[rows_of(b), :], wup[s, rows_w, :], 1, 1).astype(BF)
            y_start(k, b, n)

    def grad_up(s, low2):
        @pl.loop(0, 4)
        def _(i):
            cols = lanes(i * 2, 256)
            rows_w = pl.ds(pl.multiple_of(i * 256, 256), 256)
            for q in range(2):
                wup[s, rows_w, q * 1024 : q * 1024 + 1024] = dot(
                    low2[:, cols], gpre[:, q * 1024 : q * 1024 + 1024], 0, 0
                ).astype(BF)

    def loop_sums(b, count, step):
        zero = jnp.zeros((8, 1024), F32)

        def body(i, tots):
            new = step(pl.ds(pl.multiple_of(b * LP + i * CH, CH), CH))
            return tuple(t + fold8(v) for t, v in zip(tots, new))

        return [colsum(t) for t in lax.fori_loop(0, LP // CH, body, (zero,) * count)]

    def grad_middle(s, b, k):
        gain = row(s, 3)

        def step(rows):
            g2 = y_sum(k, rows)
            nrm = nrm2s[s, rows, :].astype(F32)
            t = g2 * gain
            m1 = jnp.mean(t, axis=-1, keepdims=True)
            m2 = jnp.mean(t * nrm, axis=-1, keepdims=True)
            gm = gb[s, rows, :].astype(F32) + stat(s, INV2, rows) * (t - m1 - nrm * m2)
            mid[rows, :] = gm
            ga = gm.astype(BF)
            low[rows, :] = ga
            return g2 * nrm, g2, ga.astype(F32)

        for r, v in zip((3, 4, 2), loop_sums(b, 3, step)):
            total(s, r, b, v)

    def grad_mixed(s, b):
        @pl.loop(0, 2)
        def _(n):
            cols = lanes(n * 2, 256)
            rows_w = pl.ds(pl.multiple_of(n * 256, 256), 256)
            gpre[rows_of(b), cols] = dot(low[rows_of(b), :], wout[s, rows_w, :], 1, 1).astype(BF)

    def grad_out(s):
        @pl.loop(0, 2)
        def _(i):
            cols = lanes(i * 2, 256)
            rows_w = pl.ds(pl.multiple_of(i * 256, 256), 256)
            wout[s, rows_w, :] = dot(mixs[s, :, cols], low[...], 0, 0).astype(BF)

    def grad_attention(s, b):
        rows = rows_of(b)

        @pl.loop(0, 4)
        def _(i):
            cols = lanes(i)
            q, k, v = (qkvs[s, t, rows, cols] for t in range(3))
            q, k_low = q * jnp.asarray(0.125, BF), k * jnp.asarray(0.125, BF)
            gm = gpre[rows, cols]
            kept = stats[rows, :]
            res = []
            for h in range(2):
                lse = jnp.sum(jnp.where(lane == 64 * h + 8 * s + i, kept, 0.0), axis=-1, keepdims=True)
                probs = jnp.exp(scores(pick(h, q), k) - lse)
                gp = dot(pick(h, gm), v, 1, 1)
                gv = dot(probs.astype(BF), gm, 0, 0)
                gs = (probs * (gp - jnp.sum(probs * gp, axis=-1, keepdims=True))).astype(BF)
                res.append((dot(gs, k_low, 1, 0), dot(gs, q, 0, 0), gv))
            for t in range(3):
                gqkv[t, rows, cols] = jnp.where(left, res[0][t], res[1][t]).astype(BF)

    def grad_qv_bias(s):
        sv[s, 6:7, 0:512] = sum_rows(lambda r: gqkv[0, r, :], 512)
        sv[s, 6:7, 512:1024] = sum_rows(lambda r: gqkv[2, r, :], 512)

    def grad_lowered(s, b, k):
        rows = rows_of(b)

        @pl.loop(0, 4)
        def _(n):
            cols = lanes(n * 2, 256)
            rows_w = pl.ds(pl.multiple_of(n * 256, 256), 256)
            a = dot(gqkv[0, rows, :], wqkv[0][s, rows_w, :], 1, 1)
            a = a + dot(gqkv[1, rows, :], wqkv[1][s, rows_w, :], 1, 1)
            a = a + dot(gqkv[2, rows, :], wqkv[2][s, rows_w, :], 1, 1)
            ys[rows, cols] = a.astype(BF)
            y_start(k, b, n)

    def grad_qkv(s, t, low1):
        @pl.loop(0, 4)
        def _(i):
            cols = lanes(i * 2, 256)
            rows_w = pl.ds(pl.multiple_of(i * 256, 256), 256)
            wqkv[t][s, rows_w, :] = dot(low1[:, cols], gqkv[t], 0, 0).astype(BF)

    def grad_stream(s, b, k, dst):
        gain = row(s, 0)

        def step(rows):
            g1 = y_sum(k, rows)
            nrm = norm1(s, rows)
            t = g1 * gain
            m1 = jnp.mean(t, axis=-1, keepdims=True)
            m2 = jnp.mean(t * nrm, axis=-1, keepdims=True)
            dst[rows, :] = (mid[rows, :] + stat(s, INV1, rows) * (t - m1 - nrm * m2)).astype(BF)
            if s == 1:
                low[rows, :] = (nrm * gain + row(s, 1)).astype(BF)
            return g1 * nrm, g1

        for r, v in zip((0, 1), loop_sums(b, 2, step)):
            total(s, r, b, v)

    def add_rows(dst, src, count, chunk):
        @pl.loop(0, count // chunk)
        def _(i):
            rows = pl.ds(pl.multiple_of(i * chunk, chunk), chunk)
            dst[rows, :] = dst[rows, :] + src[rows, :]

    def shape_of(m):
        if m in BY_ROWS:
            return 128, (16 if m == UP else 64)
        return WIDTH[m] // 2, 128

    def add_block(m, dst, src):
        add_rows(dst, src, *shape_of(m))

    def g_half(s, m):
        return stage if (s, m) == (1, DOWN) else half(m, w[m], s, c)

    def g_block(s, m, d):
        if (s, m) == (1, DOWN):
            return stage.at[:, pl.ds(pl.multiple_of(d * 128, 128), 128)]
        return block(m, w[m], s, d, c)

    def r_view(s, m, h):
        return rbuf[m] if s == 1 else half(m, w[m], 1, h)

    def x_view(s, m, k, col):
        if (s, m) in Z_FIRST:
            return xbuf[m].at[s]
        if s == 0 and m in (Q, K, V):
            return gels.at[1, pl.ds((m - Q) * 128, 128), pl.ds(k * 256, 256)]
        if s == 0:
            return block(m, w[m], 1, at_dp(k, col), c)
        at = pl.ds(k * 128, 128)
        return xbuf[m].at[at, :] if m in BY_ROWS else xbuf[m].at[:, at]

    def z_view(s, m, slot, col, place):
        if s == 0 and m in (Q, K, V):
            i = col * 4 + slot if (s, m) in Z_FIRST else 4 + slot
            return gels.at[1, pl.ds((m - Q) * 128, 128), pl.ds(i * 256, 256)]
        if s == 0:
            return block(m, w[m], 1, place * 2 + (x if col == 0 else 1 - x), c)
        if m in (UP, DOWN):
            at = pl.ds(slot * 128, 128)
            return rbuf[m].at[at, :] if m == UP else rbuf[m].at[:, at]
        return zbuf[m].at[col * 4 + slot]

    def rs_c(s, m):
        q = s * 6 + m - 1
        if s == 0:
            pl.semaphore_wait(free_c.at[m - 1], 1)
        if (s, m) == (1, UP):
            pl.semaphore_wait(free_up, 1)
        src = rup if (s, m) == (1, DOWN) else half(m, w[m], s, 1 - c)
        remote(src, r_view(s, m, c), rsem_cs.at[q], rsem_c.at[q], to_c).start()

    def rs_sum(s, m):
        q = s * 6 + m - 1
        mine, got = g_half(s, m), r_view(s, m, 1 - c)
        cp = remote(mine, got, rsem_cs.at[q], rsem_c.at[q], to_c)
        cp.wait_recv()
        cp.wait_send()
        if (s, m) == (1, DOWN):
            pl.semaphore_signal(free_up, inc=1, device_id=to_c, device_id_type=MESH)
        elif s == 1:
            pl.semaphore_signal(free_c.at[m - 1], inc=1, device_id=to_c, device_id_type=MESH)
        rows = 1024 if m in BY_ROWS else WIDTH[m] // 2
        add_rows(mine, got, rows, 16 if m not in (Q, K, V) else 64)
        if s == 1 and m in (UP, DOWN):
            z_credit(free_r.at[m - UP])

    def rs_to_x(s, m):
        if s == 0:
            pl.semaphore_wait(free_x.at[m - 1], 1)
        for k in (INNER, FAR, NEAR, SELF):
            q = s * 6 + m - 1
            b = g_block(s, m, at_dp(k, 1))
            remote(b, x_view(s, m, k, 0), rsem_xs.at[q], rsem_x.at[rx[(s, m), k]], to_x).start()

    def rs_from_x(s, m, k):
        q = s * 6 + m - 1
        b = g_block(s, m, at_dp(k, 0))
        got = x_view(s, m, k, 1)
        remote(b, got, rsem_xs.at[q], rsem_x.at[rx[(s, m), k]], to_x).wait_recv()
        if k == SELF:
            wait_bytes(m, 4, rsem_xs.at[q])
        add_block(m, b, got)

    def down_freed():
        pl.semaphore_signal(free_c.at[DOWN - 1], inc=1, device_id=to_c, device_id_type=MESH)
        x_freed(DOWN)
        z_freed(DOWN)

    def gelu_freed():
        for m in (Q, K, V):
            if (0, m) not in Z_FIRST:
                x_freed(m)
        for m in (Q, K, V):
            z_freed(m)

    def x_freed(m):
        pl.semaphore_signal(free_x.at[m - 1], inc=1, device_id=to_x, device_id_type=MESH)

    def z_wait_credits(sem):
        @pl.when(inner)
        def _():
            pl.semaphore_wait(sem, 3)

        @pl.when(jnp.logical_not(inner))
        def _():
            pl.semaphore_wait(sem, 1)

    def z_credit(sem):
        for k in (NEAR, INNER):
            pl.semaphore_signal(sem, inc=1, device_id=to_z(places[k]), device_id_type=MESH)

    def z_ready(s, m):
        if s == 0:
            z_wait_credits(free_z.at[m - 1])
        elif m in (UP, DOWN):
            z_wait_credits(free_r.at[m - UP])

    def rs_to_z(s, m, k, col):
        q = s * 6 + m - 1
        b = g_block(s, m, at_dp(k, col))
        if k == NEAR:
            remote(b, z_view(s, m, 0, col, z), rsem_zs.at[q, col], rsem_z.at[rz[(s, m), col * 4]], to_z(near)).start()
        else:

            @pl.when(jnp.logical_not(inner))
            def _():
                remote(b, z_view(s, m, k, col, places[k]), rsem_zs.at[q, col], rsem_z.at[rz[(s, m), col * 4 + k]], to_z(near)).start()

    def rs_pass(s, m, k, col):
        q = s * 6 + m - 1

        @pl.when(inner)
        def _():
            b = g_block(s, m, at_dp(k, col))
            got = z_view(s, m, k, col, places[k])
            remote(b, got, rsem_zs.at[q, col], rsem_z.at[rz[(s, m), col * 4 + k]], to_z(near)).wait_recv()
            add_block(m, b, got)
            remote(b, z_view(s, m, 1, col, places[k]), rsem_zs.at[q, col], rsem_z.at[rz[(s, m), col * 4 + 1]], to_z(places[k])).start()

    def z_arrived(s, m, col):
        q = s * 6 + m - 1
        got = [z_view(s, m, 0, col, near), z_view(s, m, 1, col, z)]
        for slot in range(2):
            remote(got[slot], got[slot], rsem_zs.at[q, col], rsem_z.at[rz[(s, m), col * 4 + slot]], to_z(near)).wait_recv()
        return got

    def z_sent(s, m, col):
        wait_bytes(m, 3, rsem_zs.at[s * 6 + m - 1, col])

    def z_freed(m):
        z_credit(free_z.at[m - 1])

    def rs_fold(s, m):
        q = s * 6 + m - 1
        b = g_block(s, m, at_dp(SELF, 1))
        for got in z_arrived(s, m, 1):
            add_block(m, b, got)
        remote(b, xbuf[m].at[s], rsem_xs.at[q], rsem_x.at[rx[(s, m), 0]], to_x).start()

    def f_target(m):
        n = WIDTH[m] // 2
        at = pl.ds(pl.multiple_of(c * n, n), n)
        if m in (Q, K, V):
            return gqkv_out.at[m - 1, :, at]
        if m == UP:
            return gup_out.at[:, at]
        return (gout_out if m == OUT else gdown_out).at[at, :]

    def rs_f(s, m):
        q = s * 6 + m - 1
        mine = g_block(s, m, me)
        parts = [mine] + z_arrived(s, m, 0)
        if (s, m) in Z_FIRST:
            cp = remote(mine, xbuf[m].at[s], rsem_xs.at[q], rsem_x.at[rx[(s, m), 0]], to_x)
            cp.wait_recv()
            cp.wait_send()
            parts.append(xbuf[m].at[s])
        count, chunk = shape_of(m)
        chunk = min(chunk, 64)

        @pl.loop(0, count // chunk)
        def _(i):
            rows = pl.ds(pl.multiple_of(i * chunk, chunk), chunk)
            a = parts[0][rows, :].astype(F32)
            for part in parts[1:]:
                a = a + part[rows, :].astype(F32)
            fbuf[m][rows, :] = a

        for col in range(2) if (s, m) in Z_FIRST else (0,):
            z_sent(s, m, col)
        if s == 1 and m in (UP, OUT):
            z_freed(m)

        @pl.when(c == s)
        def _():
            pltpu.make_async_copy(fbuf[m], f_target(m), rsem_fs.at[q]).start()

        @pl.when(c != s)
        def _():
            remote(fbuf[m], f_target(m), rsem_fs.at[q], rsem_f.at[q], to_c).start()

    def rs_f_sent(s, m):
        q = s * 6 + m - 1

        @pl.when(c == s)
        def _():
            pltpu.make_async_copy(fbuf[m], f_target(m), rsem_fs.at[q]).wait()

        @pl.when(c != s)
        def _():
            remote(fbuf[m], f_target(m), rsem_fs.at[q], rsem_f.at[q], to_c).wait_send()

    def rs_end(s, m):
        q = s * 6 + m - 1

        @pl.when(c == s)
        def _():
            remote(fbuf[m], fbuf[m], rsem_fs.at[q], rsem_f.at[q], to_c).wait_recv()

    def vec_copies(i):
        if i == 0:
            return [remote(sv.at[1 - c], svc, vsem_s.at[0], vsem.at[0], to_c)]
        if i == 1:
            return [remote(sv.at[c], svx, vsem_s.at[1], vsem.at[1], to_x)]
        if i == 2:
            return [
                remote(svc, svz.at[j - 1], vsem_s.at[1 + j], vsem.at[1 + j], to_z(lax.rem(z + j, Z)))
                for j in range(1, Z)
            ]
        return [
            pltpu.make_async_copy(sv.at[c, pl.ds(0, 8)], gvec_out, isem.at[0]),
            pltpu.make_async_copy(vq, gqv_out, isem.at[1]),
            pltpu.make_async_copy(vu, gupb_out, isem.at[2]),
        ]

    def vec_step(i):
        if i:
            for cp in vec_copies(i - 1):
                cp.wait_recv()
                cp.wait_send()
        if i == 1:
            sv[c] = sv[c] + svc[...]
        if i == 2:
            svc[...] = sv[c] + svx[...]
        if i == 3:
            sv[c] = svc[...] + svz[0] + svz[1] + svz[2]
            for t in range(2):
                for h in range(8):
                    at = (t * 8 + h) * 64
                    vq[t, h : h + 1, :] = sv[c, 6:7, at : at + 64]
            for g in range(8):
                vu[g : g + 1, :] = sv[c, 7 + g // 4 : 8 + g // 4, g % 4 * 256 : g % 4 * 256 + 256]
        for cp in vec_copies(i):
            cp.start()

    clock = Clock()
    size = {SMALL: 8e3, Q: 131e3, K: 131e3, V: 131e3, OUT: 131e3, UP: 524e3, DOWN: 524e3}
    RATE = 82e3
    HOP = 1.8
    free = {"x": 0.0, "z": 0.0, "y": 0.0}
    got = {}

    def link(name, nbytes):
        free[name] = max(free[name], clock.now) + nbytes / RATE
        return free[name] + HOP

    order = (SMALL, Q, K, V, OUT, UP, DOWN)
    for cp in small_in:
        cp.start()
    for s in range(2):
        for m in order[1:]:
            ag_share(s, m)
    pack_small()
    for s in range(2):
        ag_share(s, SMALL)
    clock.now = 6.5

    def plan_gather(s, m):
        x_first = m in X_FIRST

        def at_x(k):
            ag_x(s, m, k)
            got[s, m] = got.get((s, m), 0) + 1
            if x_first:
                along_z(1)

        def at_z(k, col):
            ag_z(s, m, k, col)
            if x_first:
                got[s, m] = got.get((s, m), 0) + 1
            else:
                clock.add(link("x", size[m]), functools.partial(at_x, k))

        def along_z(col):
            begin = max(free["z"], clock.now)
            t = size[m] / RATE
            free["z"] = begin + 3 * t
            for k in (NEAR, INNER, FAR):
                late = HOP if k == NEAR else 2 * HOP
                clock.add(begin + k * t + late, functools.partial(at_z, k, col))

        def own():
            if not x_first:
                ag_shared(s, m)
            ag_own_z(s, m, 0)
            along_z(0)
            if not x_first:
                ag_to_x(s, m, SELF)
                clock.add(link("x", size[m]), functools.partial(at_x, SELF))

        def early():
            ag_shared(s, m)
            ag_to_x(s, m, SELF)
            clock.add(max(link("x", size[m]), z_begin[s, m] - LEAD + 0.1), functools.partial(at_x, SELF))

        if x_first:
            clock.add(x_begin[s, m], early)
        clock.add(max(z_begin[s, m] - LEAD, clock.now), own)

    LEAD, AHEAD = 23.0, 2.0
    z_begin, x_begin, at = {}, {}, 7.0
    for s in range(2):
        for m in order:
            z_begin[s, m] = at
            at += size[m] / RATE * (6 if m in X_FIRST else 3)
            x_begin[s, m] = max(clock.now, z_begin[s, m] - LEAD - AHEAD)
    for s in range(2):
        for m in order:
            plan_gather(s, m)

    def need(s, m):
        clock.drain(lambda: got.get((s, m), 0) == (7 if m in X_FIRST else 4))
        clock.now += 1.5
        ag_need(s, m)

    def y_sent():
        return link("y", 426e3 * 2) + 1.0

    passed = set()

    def reduce(s, m):
        x_first = (s, m) in Z_FIRST
        t = size[m] / RATE
        order = (INNER, FAR, NEAR)

        def z_start(k, col):
            rs_to_z(s, m, k, col)
            ready = link("z", size[m])
            if k != NEAR:
                clock.add(ready, functools.partial(z_pass, k, col), 0.4)

        def z_pass(k, col):
            rs_pass(s, m, k, col)
            done.append((k, col))
            if len([d for d in done if d[1] == col]) == 2:
                ready = clock.now + t + 2 * HOP + 8.0
                if x_first and col == 1:
                    clock.add(ready, fold, 0.4)
                elif not x_first:
                    clock.add(ready, finish_sum, 0.6)

        done = []

        def fold():
            rs_fold(s, m)
            clock.add(max(link("x", size[m]), clock.now + 2.0), finish_sum, 0.6)

        def sum_step():
            rs_sum(s, m)
            passed.add(("c", s, m))
            if x_first:
                if s == 0:
                    clock.drain(lambda: ("z", m) in passed)
                z_ready(s, m)
                for col in (1, 0):
                    for k in order:
                        z_start(k, col)
            else:
                if s == 0:
                    clock.drain(lambda: ("x", m) in passed)
                rs_to_x(s, m)
                for k in order + (SELF,):
                    clock.add(link("x", size[m]) + 1.5, functools.partial(from_x, k), 0.3)

        def from_x(k):
            rs_from_x(s, m, k)
            if k == SELF:
                done.append((SELF, -1))
                if s == 1:
                    if m == UP:
                        x_freed(m)
                        passed.add(("x", m))
                return
            if k == INNER:
                if s == 0:
                    clock.drain(lambda: ("z", m) in passed)
                z_ready(s, m)
            z_start(k, 0)

        def finish_sum():
            clock.drain(lambda: ready_to_finish())
            if s == 0:
                clock.drain(lambda: ("f", m) in passed)
                rs_f_sent(1, m)
            rs_f(s, m)
            if s == 1:
                passed.add(("f", m))
                if m in (UP, OUT):
                    passed.add(("z", m))

        def ready_to_finish():
            return x_first or (SELF, -1) in done

        if s == 0:
            clock.drain(lambda: ("c", 1, m) in passed)
        elif m == UP:
            clock.drain(lambda: ("c", 1, DOWN) in passed)
        rs_c(s, m)
        clock.add(clock.now + 4 * size[m] / 500e3 + 2.0, sum_step, 0.8)

    clock.run(2.0, load_woven, x_ref, isem.at[0], gpre)
    for b in range(2):
        clock.run(0.6, unweave, gpre, xs.at[0], b, None)
    y_at = {}
    for s in range(2):
        last = s == 1
        need(s, SMALL)
        unpack_small(s)
        for b in range(2):
            if last:
                clock.wait(y_at[1, b], y_wait, 1, b)
                clock.run(1.0, finish, 0, b, 1, xs.at[1])
            clock.run(1.7, ln1, s, b)
            if b == 0:
                for m in (Q, K, V):
                    need(s, m)
            clock.run(1.7, project, s, b)
            clock.run(3.0, attention, s, b)
            if b == 0:
                need(s, OUT)
            clock.run(0.9, out_project, s, b, s * 2)
            y_at[s * 2, b] = y_sent()
        if last:
            clock.run(1.5, weave, xs.at[1], gpre)
            emit(0, 0)
        for b in range(2):
            clock.wait(y_at[s * 2, b], y_wait, s * 2, b)
            clock.run(1.5, middle, s, b, s * 2)
            if b == 0:
                need(s, UP)
            clock.run(4.0, up_project, s, b)
        if not last:
            need(0, DOWN)
            for b in range(2):
                clock.run(1.5, down_project, 0, b, 1, True)
                y_at[1, b] = y_sent()
            clock.run(2.0, load_woven, cot_ref, isem.at[1], gpre)
            for b in range(2):
                clock.run(0.6, unweave, gpre, gb.at[1], b, alive_of(b))

    clock.run(1.9, grad_down, 1, 1 - c, rup)
    reduce(1, DOWN)
    clock.run(1.9, grad_down, 1, c, stage)
    need(1, DOWN)
    for b in range(2):
        clock.run(2.7, grad_gelu, 1, b)
        clock.run(2.0, grad_low_two, 1, b, 3)
        y_at[3, b] = y_sent()
    for q in range(2):
        for m in order:
            ag_sent(q, m)
    for s in (1, 0):
        k = 3 if s == 1 else 5
        clock.run(3.0, grad_up, s, low if s == 1 else gb.at[1])
        reduce(s, UP)
        if s == 0:
            for b in range(2):
                clock.run(1.7, down_project, 1, b, 7, False)
            down_freed()
            gelu_freed()
            passed.update({("c", 1, DOWN), ("x", DOWN), ("z", DOWN), ("x", Q), ("x", K), ("x", V), ("z", Q), ("z", K), ("z", V)})
            clock.run(1.9, grad_down, 0, 1 - c, wdown.at[0])
            reduce(0, DOWN)
            clock.run(1.9, grad_down, 0, c, wdown.at[0])
            for t in range(3):
                clock.run(1.4, grad_qkv, 1, t, low)
                reduce(1, Q + t)
            clock.run(0.5, grad_qv_bias, 1)
        clock.run(0.6, grad_mlp_biases, s)
        if s == 1:
            for b in range(2):
                clock.run(0.3, keep_middle, b)
        if s == 0:
            emit_sent(0, 0)
            clock.run(1.5, weave, gb.at[0], gpre)
            emit(1, 1)
        if s == 0:
            for b in range(2):
                clock.run(0.8, relow1, 0, b, gb.at[1])
        for b in range(2):
            clock.wait(y_at[k, b], y_wait, k, b)
            clock.run(1.9, grad_middle, s, b, k)
            clock.run(0.5, grad_mixed, s, b)
            if b == 1:
                clock.run(0.9, grad_out, s)
                reduce(s, OUT)
            clock.run(3.8, grad_attention, s, b)
            clock.run(1.6, grad_lowered, s, b, k + 1)
            y_at[k + 1, b] = y_sent()
        if s == 1:
            for b in range(2):
                clock.wait(y_at[4, b], y_wait, 4, b)
                clock.run(2.2, grad_stream, 1, b, 4, gb.at[0])
                clock.run(2.7, grad_gelu, 0, b)
                clock.run(2.0, grad_low_two, 0, b, 5)
                y_at[5, b] = y_sent()
                if b == 0:
                    for q in range(2):
                        clock.run(0.5, relower, 0, q, gb.at[1])
        else:
            pl.semaphore_signal(free_y, inc=1, device_id=to_y, device_id_type=MESH)
            pl.semaphore_wait(free_y, 1)
            for b in range(2):
                for n in range(4):
                    y_start(7, b, n)
                y_at[7, b] = y_sent()
            for t in range(3):
                clock.run(1.4, grad_qkv, 0, t, gb.at[1])
                reduce(0, Q + t)
            clock.run(0.5, grad_qv_bias, 0)
    for b in range(2):
        clock.wait(y_at[6, b], y_wait, 6, b)
        clock.run(2.2, grad_stream, 0, b, 6, low)
    def vec_chain(i):
        vec_step(i)
        if i < 3:
            ready = (clock.now + 3.0, link("x", 131e3) + 1.0, link("z", 262e3) + 4.0)[i]
            clock.add(ready, functools.partial(vec_chain, i + 1), 0.5)

    vec_chain(0)
    emit_sent(1, 1)
    clock.run(2.0, weave, low, gpre)
    emit(1, 0)
    for b in range(2):
        clock.wait(y_at[7, b], y_wait, 7, b)
        clock.run(1.0, finish, 1, b, 7, gb.at[1])
    emit_sent(1, 0)
    clock.run(2.0, weave, gb.at[1], gpre)
    emit(0, 1)
    clock.drain(lambda: not clock.queue)
    for cp in vec_copies(3):
        cp.wait()
    for m in MATS:
        rs_f_sent(0, m)
    for s in range(2):
        for m in MATS:
            rs_end(s, m)
    emit_sent(0, 1)
    for which in range(2):
        for s in range(2):
            emit_got(which, s)


def run_kernel(*args):
    any_spec = pl.BlockSpec(memory_space=pl.ANY)
    V = pltpu.VMEM
    D_ = pltpu.SemaphoreType.DMA
    REG = pltpu.SemaphoreType.REGULAR
    S = jax.ShapeDtypeStruct
    mats = ((1024, 512), (1024, 512), (1024, 512), (512, 1024), (1024, 2048), (2048, 1024))
    by_rows = (True, True, True, False, True, False)
    first = (False, True, False, True, False, False)

    def halved(shape, rows, cut):
        return (shape[0] // cut, shape[1] // 2) if rows else (shape[0] // 2, shape[1] // cut)

    scratch = [V((2, 8, 32, 128), BF)]
    scratch += [V((2,) + shape, BF) for shape in mats]
    scratch += [V(halved(shape, rows, 1), BF) for shape, rows in zip(mats, by_rows)]
    scratch += [
        V((2,) + halved(shape, rows, 8) if f else halved(shape, rows, 2), BF)
        for shape, rows, f in zip(mats, by_rows, first)
    ]
    scratch += [V((8 if f else 4,) + halved(shape, rows, 8), BF) for shape, rows, f in zip(mats[:4], by_rows, first)]
    scratch += [V(halved(shape, rows, 8), F32) for shape, rows in zip(mats, by_rows)]
    scratch += [
        V((2, R, 1024), BF), V((2, 3, R, 512), BF), V((2, R, 512), BF), V((2, R, 1024), BF),
        V((2, R, 2048), BF), V((2, R, 2048), BF), V((R, 128), F32),
        V((R, 1024), BF), V((R, 1024), F32), V((2, R, 1024), BF), V((R, 2048), BF), V((3, R, 512), BF),
        V((R, 1024), BF), V((2, R, 1024), BF), V((LP, 256), F32),
        V((2, 16, 1024), F32), V((2, 16, 1024), F32), V((16, 1024), F32), V((16, 1024), F32), V((3, 16, 1024), F32),
        V((LP, 2, 1024), BF), V((1024, 1024), BF), V((32, 128), BF), V((6, 1, 128), BF), V((2, 8, 8), BF), V((8, 32), BF), V((2, 8, 64), F32), V((8, 256), F32),
        D_((14,)), D_((14, 2)), D_((54,)), D_((44,)),
        D_((12,)), D_((12,)), D_((12,)), D_((48,)), D_((12, 2)), D_((64,)), D_((12,)), D_((12,)),
        D_((16,)), D_((16,)), D_((4,)), D_((4,)), D_((4,)), D_((10,)), D_((5,)), D_((5,)),
        REG((6,)), REG((6,)), REG((6,)), REG, REG((2,)), REG,
    ]
    return pl.pallas_call(
        kernel,
        out_shape=[
            S((2, L, 2, 1024), BF), S((2, L, 2, 1024), BF), S((3, 128, 512), F32), S((512, 128), F32),
            S((128, 2048), F32), S((2048, 128), F32), S((8, 1024), F32), S((2, 8, 64), F32), S((8, 256), F32),
        ],
        in_specs=[any_spec] * 14 + [pl.BlockSpec(memory_space=pltpu.SMEM)],
        out_specs=[any_spec] * 9,
        scratch_shapes=scratch,
        compiler_params=pltpu.CompilerParams(
            collective_id=1, has_side_effects=True, vmem_limit_bytes=67043328
        ),
        name="sections",
    )(*args)


def local_fast(images, cotangent, live_count, ln1_gain, ln1_bias, qkv_weight, qv_bias, out_weight, out_bias,
               ln2_gain, ln2_bias, up_weight, up_bias, down_weight, down_bias):
    d = lax.axis_index("dp")

    def woven(a):
        return jnp.transpose(a, (0, 2, 1, 3))

    act, gin, gqkv, gout, gup, gdown, gvec, gqv, gupb = run_kernel(
        ln1_gain, ln1_bias, out_bias, ln2_gain, ln2_bias, down_bias, qv_bias[0], up_bias[0],
        qkv_weight[0], out_weight[0], up_weight[0], down_weight[0], woven(images), woven(cotangent), live_count.reshape(2),
    )

    def cut(v, axis, n):
        return lax.dynamic_slice_in_dim(v, d * n, n, axis=axis)

    act, gin = woven(act)[None], woven(gin)[None]
    vecs = cut(gvec, 1, 128)
    qv = cut(gqv, 2, 8)
    upb = cut(gupb, 1, 32)
    return (
        act, gin, vecs[0:1], vecs[1:2], gqkv[None], qv[None], gout[None], vecs[2:3], vecs[3:4], vecs[4:5],
        gup[None], upb[None], gdown[None], vecs[5:6],
    )


def solution(mesh):
    fast = dict(mesh.shape) == {"section": 2, "dp": 8, "mp": 2}
    return jax.shard_map(
        local_fast if fast else local,
        mesh=mesh,
        in_specs=(
            P(None, "dp", None, None),
            P(None, "dp", None, None),
            P(None, "dp"),
            P("section", "dp"),
            P("section", "dp"),
            P("section", None, "dp", "mp"),
            P("section", None, "mp", "dp"),
            P("section", "mp", "dp"),
            P("section", "dp"),
            P("section", "dp"),
            P("section", "dp"),
            P("section", "dp", "mp"),
            P("section", "mp", "dp"),
            P("section", "mp", "dp"),
            P("section", "dp"),
        ),
        out_specs=(
            P("section", None, "dp", None, None),
            P("section", None, "dp", None, None),
            P("section", "dp"),
            P("section", "dp"),
            P("section", None, "dp", "mp"),
            P("section", None, "mp", "dp"),
            P("section", "mp", "dp"),
            P("section", "dp"),
            P("section", "dp"),
            P("section", "dp"),
            P("section", "dp", "mp"),
            P("section", "mp", "dp"),
            P("section", "mp", "dp"),
            P("section", "dp"),
        ),
        check_vma=False,
    )
```

```python
import functools
import heapq
import math

import jax
import jax.numpy as jnp
from jax import lax
from jax.experimental import pallas as pl
from jax.experimental.pallas import tpu as pltpu
from jax.sharding import PartitionSpec as P

HD = 64


epsilon = 1e-06


def gather_all(small, big):
    flat = jnp.concatenate([piece.reshape(-1) for piece in small])
    packed = lax.all_gather(flat, "dp", axis=0, tiled=False)
    count = packed.shape[0]
    whole, offset = [], 0
    for piece, axis in zip(small, (1, 1, 3, 1, 1, 1, 2, 1)):
        part = packed[:, offset : offset + piece.size].reshape((count,) + piece.shape)
        offset += piece.size
        part = jnp.moveaxis(part, 0, axis)
        shape = list(piece.shape)
        shape[axis] *= count
        whole.append(part.reshape(shape))
    qkv, out, up, down = (
        lax.all_gather(piece, "dp", axis=axis, tiled=True) for piece, axis in zip(big, (2, 2, 1, 2))
    )
    return (
        whole[0],
        whole[1],
        qkv,
        whole[2],
        out,
        whole[3],
        whole[4],
        whole[5],
        up,
        whole[6],
        down,
        whole[7],
    )


def scatter_all(totals, shards):
    small_at = (0, 1, 3, 5, 6, 7, 9, 11)
    count = lax.axis_size("dp")
    rows = []
    for index, axis in zip(small_at, (1, 1, 3, 1, 1, 1, 2, 1)):
        piece = totals[index]
        shape = list(piece.shape)
        shape[axis : axis + 1] = [count, shape[axis] // count]
        rows.append(jnp.moveaxis(piece.reshape(shape), axis, 0).reshape(count, -1))
    packed = lax.psum_scatter(jnp.concatenate(rows, axis=1), "dp", scatter_dimension=0, tiled=False)
    owned, offset = [None] * 12, 0
    for index in small_at:
        size = shards[index].size
        owned[index] = packed[offset : offset + size].reshape(shards[index].shape)
        offset += size
    for index, axis in zip((2, 4, 8, 10), (2, 2, 1, 2)):
        owned[index] = lax.psum_scatter(
            totals[index].astype(jnp.bfloat16), "dp", scatter_dimension=axis, tiled=True
        ).astype(jnp.float32)
    return owned


def both_halves(partial):
    return lax.psum(partial.astype(jnp.bfloat16), "mp").astype(jnp.float32)


def from_behind(x, axis, by):
    length = lax.axis_size(axis)
    pairs = [(i, i + by) for i in range(length) if 0 <= i + by < length]
    return lax.ppermute(x, axis, pairs)


def norm_parts(stream):
    centered = stream - jnp.mean(stream, axis=-1, keepdims=True)
    inverse = lax.rsqrt(jnp.mean(centered * centered, axis=-1, keepdims=True) + epsilon)
    return (centered * inverse, inverse)


def norm_back(grad_normed, normed, inverse):
    first_mean = jnp.mean(grad_normed, axis=-1, keepdims=True)
    second_mean = jnp.mean(grad_normed * normed, axis=-1, keepdims=True)
    return inverse * (grad_normed - first_mean - normed * second_mean)


def gelu_slope(preact):
    cumul = 0.5 * (1.0 + lax.erf(preact * 2.0 ** (-0.5)))
    density = jnp.exp(-0.5 * preact * preact) * (2.0 * math.pi) ** (-0.5)
    return cumul + preact * density


def unpack_weights(whole):
    return (
        whole[0][0].astype(jnp.float32),
        whole[1][0].astype(jnp.float32),
        whole[2][0],
        whole[3][0].reshape(2, -1).astype(jnp.float32),
        whole[4][0],
        whole[5][0].astype(jnp.float32),
        whole[6][0].astype(jnp.float32),
        whole[7][0].astype(jnp.float32),
        whole[8][0],
        whole[9][0].reshape(-1).astype(jnp.float32),
        whole[10][0],
        whole[11][0].astype(jnp.float32),
    )


def forward(stream, params, rows):
    (
        gain_one,
        shift_one,
        qkv_mat,
        qv_shift,
        out_mat,
        out_shift,
        gain_two,
        shift_two,
        up_mat,
        up_shift,
        down_mat,
        down_shift,
    ) = params
    batch_size, seq_len, model_width = stream.shape
    head_count = qkv_mat.shape[2] // HD
    scale = HD ** (-0.5)
    normed, inverse = norm_parts(stream)
    lowered = (normed * gain_one + shift_one).astype(jnp.bfloat16)
    projected = jnp.einsum("bld,cde->cble", lowered, qkv_mat, preferred_element_type=jnp.float32)
    split_shape = (batch_size, seq_len, head_count, HD)
    queries = (projected[0] + qv_shift[0]).astype(jnp.bfloat16).reshape(split_shape)
    keys_low = projected[1].astype(jnp.bfloat16).reshape(split_shape)
    values_low = (projected[2] + qv_shift[1]).astype(jnp.bfloat16).reshape(split_shape)
    scores = (
        jnp.einsum("blhe,bmhe->bhlm", queries, keys_low, preferred_element_type=jnp.float32) * scale
    )
    row_max = jnp.max(scores, axis=-1, keepdims=True)
    log_total = row_max + jnp.log(jnp.sum(jnp.exp(scores - row_max), axis=-1, keepdims=True))
    attn_probs = jnp.exp(scores - log_total)
    mixed = jnp.einsum(
        "bhlm,bmhe->blhe",
        attn_probs.astype(jnp.bfloat16),
        values_low,
        preferred_element_type=jnp.float32,
    )
    mixed = mixed.astype(jnp.bfloat16).reshape(batch_size, seq_len, -1)
    partial_attn = jnp.einsum("bld,de->ble", mixed, out_mat, preferred_element_type=jnp.float32)
    middle = stream + both_halves(partial_attn) + out_shift
    normed_two, inverse_two = norm_parts(middle)
    lowered_two = (normed_two * gain_two + shift_two).astype(jnp.bfloat16)
    preact = (
        jnp.einsum("bld,df->blf", lowered_two, up_mat, preferred_element_type=jnp.float32)
        + up_shift
    )
    gelu_out = jax.nn.gelu(preact, approximate=False).astype(jnp.bfloat16)
    partial_mlp = jnp.einsum("blf,fd->bld", gelu_out, down_mat, preferred_element_type=jnp.float32)
    result = (middle + both_halves(partial_mlp) + down_shift) * rows
    return (result, (stream, middle, queries, keys_low, values_low, log_total, mixed, preact))


def backward(seed, saved, params, shapes):
    (
        gain_one,
        shift_one,
        qkv_mat,
        qv_shift,
        out_mat,
        out_shift,
        gain_two,
        shift_two,
        up_mat,
        up_shift,
        down_mat,
        down_shift,
    ) = params
    stream, middle, queries, keys_low, values_low, log_total, mixed, preact = saved
    batch_size, seq_len, head_count, head_dim = queries.shape
    scale = HD ** (-0.5)
    normed, inverse = norm_parts(stream)
    lowered = (normed * gain_one + shift_one).astype(jnp.bfloat16)
    normed_two, inverse_two = norm_parts(middle)
    lowered_two = (normed_two * gain_two + shift_two).astype(jnp.bfloat16)
    gelu_out = jax.nn.gelu(preact, approximate=False).astype(jnp.bfloat16)
    grad_mlp = seed.astype(jnp.bfloat16)
    grad_down_shift = jnp.sum(grad_mlp.astype(jnp.float32), axis=(0, 1))
    grad_down_mat = jnp.einsum(
        "blf,bld->fd", gelu_out, grad_mlp, preferred_element_type=jnp.float32
    )
    grad_gelu = jnp.einsum("bld,fd->blf", grad_mlp, down_mat, preferred_element_type=jnp.float32)
    grad_pre = (grad_gelu * gelu_slope(preact)).astype(jnp.bfloat16)
    grad_up_shift = jnp.sum(grad_pre.astype(jnp.float32), axis=(0, 1))
    grad_up_mat = jnp.einsum(
        "bld,blf->df", lowered_two, grad_pre, preferred_element_type=jnp.float32
    )
    grad_low_two = both_halves(
        jnp.einsum("blf,df->bld", grad_pre, up_mat, preferred_element_type=jnp.float32)
    )
    grad_gain_two = jnp.sum(grad_low_two * normed_two, axis=(0, 1))
    grad_shift_two = jnp.sum(grad_low_two, axis=(0, 1))
    grad_middle = seed + norm_back(grad_low_two * gain_two, normed_two, inverse_two)
    grad_attn = grad_middle.astype(jnp.bfloat16)
    grad_out_shift = jnp.sum(grad_attn.astype(jnp.float32), axis=(0, 1))
    grad_out_mat = jnp.einsum("bld,ble->de", mixed, grad_attn, preferred_element_type=jnp.float32)
    grad_mixed = jnp.einsum("ble,de->bld", grad_attn, out_mat, preferred_element_type=jnp.float32)
    grad_mixed = grad_mixed.astype(jnp.bfloat16).reshape(batch_size, seq_len, head_count, head_dim)
    scores = (
        jnp.einsum("blhe,bmhe->bhlm", queries, keys_low, preferred_element_type=jnp.float32) * scale
    )
    attn_probs = jnp.exp(scores - log_total)
    grad_probs = jnp.einsum(
        "blhe,bmhe->bhlm", grad_mixed, values_low, preferred_element_type=jnp.float32
    )
    grad_values = jnp.einsum(
        "bhlm,blhe->bmhe",
        attn_probs.astype(jnp.bfloat16),
        grad_mixed,
        preferred_element_type=jnp.float32,
    ).astype(jnp.bfloat16)
    grad_scores = (
        attn_probs * (grad_probs - jnp.sum(attn_probs * grad_probs, axis=-1, keepdims=True))
    ).astype(jnp.bfloat16)
    grad_queries = (
        jnp.einsum("bhlm,bmhe->blhe", grad_scores, keys_low, preferred_element_type=jnp.float32)
        * scale
    ).astype(jnp.bfloat16)
    grad_keys = (
        jnp.einsum("bhlm,blhe->bmhe", grad_scores, queries, preferred_element_type=jnp.float32)
        * scale
    ).astype(jnp.bfloat16)
    grad_proj = jnp.stack([grad_queries, grad_keys, grad_values]).reshape(
        3, batch_size, seq_len, -1
    )
    grad_qv_shift = jnp.stack(
        [
            jnp.sum(grad_queries.astype(jnp.float32), axis=(0, 1)),
            jnp.sum(grad_values.astype(jnp.float32), axis=(0, 1)),
        ]
    )
    grad_qkv_mat = jnp.einsum(
        "bld,cble->cde", lowered, grad_proj, preferred_element_type=jnp.float32
    )
    grad_lowered = both_halves(
        jnp.einsum("cble,cde->bld", grad_proj, qkv_mat, preferred_element_type=jnp.float32)
    )
    grad_gain_one = jnp.sum(grad_lowered * normed, axis=(0, 1))
    grad_shift_one = jnp.sum(grad_lowered, axis=(0, 1))
    grad_stream = grad_middle + norm_back(grad_lowered * gain_one, normed, inverse)
    terms = [
        grad_gain_one,
        grad_shift_one,
        grad_qkv_mat,
        grad_qv_shift,
        grad_out_mat,
        grad_out_shift,
        grad_gain_two,
        grad_shift_two,
        grad_up_mat,
        grad_up_shift,
        grad_down_mat,
        grad_down_shift,
    ]
    return (grad_stream, [term.reshape(shape) for term, shape in zip(terms, shapes)])


def local(
    images,
    cotangent,
    live_count,
    ln1_gain,
    ln1_bias,
    qkv_weight,
    qv_bias,
    out_weight,
    out_bias,
    ln2_gain,
    ln2_bias,
    up_weight,
    up_bias,
    down_weight,
    down_bias,
):
    first_section = lax.axis_index("section") == 0
    micro_count = images.shape[0]
    slot_count = images.shape[1]
    slot_ids = jnp.arange(slot_count)
    small = (ln1_gain, ln1_bias, qv_bias, out_bias, ln2_gain, ln2_bias, up_bias, down_bias)
    gathered = gather_all(small, (qkv_weight, out_weight, up_weight, down_weight))
    params = unpack_weights(gathered)
    shapes = [piece.shape for piece in gathered]

    def row_mask(batch_index, valid):
        alive = jnp.logical_and(slot_ids < live_count[batch_index, 0], valid)
        return alive.astype(jnp.float32).reshape(slot_count, 1, 1)

    def choose(for_first, for_second):
        return jnp.where(first_section, for_first, for_second)

    incoming = jnp.zeros(images.shape[1:], jnp.bfloat16)
    outputs = []
    kept = []
    for moment in range(micro_count + 1):
        own = images[min(moment, micro_count - 1)]
        source = choose(own, incoming).astype(jnp.float32)
        rows = choose(
            row_mask(min(moment, micro_count - 1), moment < micro_count),
            row_mask(max(moment - 1, 0), moment >= 1),
        )
        result, saved = forward(source, params, rows)
        result = result.astype(jnp.bfloat16)
        outputs.append(result)
        kept.append(saved)
        if moment < micro_count:
            incoming = from_behind(result, "section", 1)
    activations = jnp.stack(
        [choose(outputs[index], outputs[index + 1]) for index in range(micro_count)]
    )
    totals = [jnp.zeros(shape, jnp.float32) for shape in shapes]
    incoming = jnp.zeros(images.shape[1:], jnp.bfloat16)
    returned = []
    for moment in range(micro_count + 1):
        later_index = min(moment, micro_count - 1)
        rows = choose(
            row_mask(max(moment - 1, 0), moment >= 1), row_mask(later_index, moment < micro_count)
        )
        seed = choose(incoming, cotangent[later_index]).astype(jnp.float32) * rows
        saved = jax.tree.map(choose, kept[max(moment - 1, 0)], kept[min(moment + 1, micro_count)])
        grad_stream, terms = backward(seed, saved, params, shapes)
        grad_low = grad_stream.astype(jnp.bfloat16)
        returned.append(grad_low)
        if moment < micro_count:
            incoming = from_behind(grad_low, "section", -1)
        totals = [first_part + second_part for first_part, second_part in zip(totals, terms)]
    shards = (
        ln1_gain,
        ln1_bias,
        qkv_weight,
        qv_bias,
        out_weight,
        out_bias,
        ln2_gain,
        ln2_bias,
        up_weight,
        up_bias,
        down_weight,
        down_bias,
    )
    owned = scatter_all(totals, shards)
    input_grads = jnp.stack(
        [choose(returned[index + 1], returned[index]) for index in range(micro_count)]
    )
    return (
        activations[None],
        input_grads[None],
        owned[0],
        owned[1],
        owned[2],
        owned[3],
        owned[4],
        owned[5],
        owned[6],
        owned[7],
        owned[8],
        owned[9],
        owned[10],
        owned[11],
    )


MESH = pl.DeviceIdType.MESH
BF = jnp.bfloat16
F32 = jnp.float32
Z = 4
EPS = 1e-06
L = 197
LP = 208
R = 2 * LP
SMALL, Q, K, V, OUT, UP, DOWN = range(7)
MATS = (Q, K, V, OUT, UP, DOWN)
BY_ROWS = (Q, K, V, UP)
X_FIRST = (K, OUT)
Z_FIRST = ((1, K), (1, OUT), (0, OUT))
WIDTH = {Q: 512, K: 512, V: 512, OUT: 512, UP: 2048, DOWN: 2048}
SELF, NEAR, INNER, FAR = range(4)


class Clock:
    def __init__(self):
        self.now, self.queue, self.count = 0.0, [], 0

    def add(self, ready, step, cost=0.2):
        heapq.heappush(self.queue, (ready, self.count, cost, step))
        self.count += 1

    def pop(self):
        ready, _, cost, step = heapq.heappop(self.queue)
        self.now = max(self.now, ready)
        step()
        self.now += cost

    def flush(self, until):
        while self.queue and self.queue[0][0] <= until:
            self.pop()

    def run(self, cost, step, *args):
        self.flush(self.now)
        step(*args)
        self.now += cost

    def wait(self, until, step, *args):
        self.flush(until)
        self.now = max(self.now, until)
        step(*args)

    def drain(self, done):
        while not done():
            self.pop()


def lanes(d, n=128):
    return pl.ds(pl.multiple_of(d * 128, 128), n)


def dot(a, b, ca, cb):
    return lax.dot_general(a, b, (((ca,), (cb,)), ((), ())), preferred_element_type=F32)


def half(m, ref, s, h):
    n = WIDTH[m] // 2
    at = pl.ds(pl.multiple_of(h * n, n), n)
    return ref.at[s, :, at] if m in BY_ROWS else ref.at[s, at, :]


def block(m, ref, s, d, h=None):
    if m == SMALL:
        return ref.at[s, d] if h is None else ref.at[s, d, pl.ds(h * 16, 16), :]
    own = pl.ds(pl.multiple_of(d * 128, 128), 128)
    n = WIDTH[m] // 2
    other = pl.ds(0, 2 * n) if h is None else pl.ds(pl.multiple_of(h * n, n), n)
    return ref.at[s, own, other] if m in BY_ROWS else ref.at[s, other, own]


def kernel(
    gain1_ref, shift1_ref, bias_o_ref, gain2_ref, shift2_ref, bias_d_ref, qv_ref, upb_ref,
    qkv_ref, out_ref, up_ref, down_ref, x_ref, cot_ref, live_ref,
    act_out, gin_out, gqkv_out, gout_out, gup_out, gdown_out, gvec_out, gqv_out, gupb_out,
    wsmall, wq, wk, wv, wout, wup, wdown,
    rq, rk, rv, rout, rup, rdown, xq, xk, xv, xout, xup, xdown,
    zq, zk, zv, zout, fq, fk, fv, fout, fup, fdown,
    xs, qkvs, mixs, nrm2s, gels, slps, stats,
    low, mid, gb, gpre, gqkv, ys, yr, acc, vec, sv, svc, svx, svz, woven, stage, pack, raw, rawq, rawu, vq, vu,
    asem_s, asem_c, asem_z, asem_x, rsem_cs, rsem_c, rsem_xs, rsem_x, rsem_zs, rsem_z, rsem_fs, rsem_f,
    ysem, ysem_s, osem, osem_r, osem_s, isem, vsem, vsem_s, free_c, free_x, free_z, free_up, free_r, free_y,
):
    shards = (pack, qkv_ref.at[0], qkv_ref.at[1], qkv_ref.at[2], out_ref, up_ref, down_ref)
    wqkv = (wq, wk, wv)
    w = (wsmall, wq, wk, wv, wout, wup, wdown)
    rbuf = (None, rq, rk, rv, rout, rup, rdown)
    xbuf = (None, xq, xk, xv, xout, xup, xdown)
    zbuf = (None, zq, zk, zv, zout)
    fbuf = (None, fq, fk, fv, fout, fup, fdown)

    c = lax.axis_index("section")
    me = lax.axis_index("dp")
    y = lax.axis_index("mp")
    z, x = me // 2, lax.rem(me, 2)
    to_x = {"dp": z * 2 + 1 - x}
    to_c = {"section": 1 - c}
    to_y = {"mp": 1 - y}

    inner = jnp.logical_or(z == 1, z == 2)
    near = z + 1 - 2 * lax.rem(z, 2)
    lower = (z < 2).astype(jnp.int32)
    places = (z, near, 1 + lower, 3 * lower)
    inner_i = jnp.where(inner, 1, 0)

    def at_dp(k, col):
        return places[k] * 2 + (x if col == 0 else 1 - x)

    def to_z(zi):
        return {"dp": zi * 2 + x}

    def remote(a, b, ss, rs, dev):
        return pltpu.make_async_remote_copy(
            src_ref=a, dst_ref=b, send_sem=ss, recv_sem=rs, device_id=dev, device_id_type=MESH
        )

    barrier = pltpu.get_barrier_semaphore()
    for dev in [to_z(places[k]) for k in (NEAR, INNER, FAR)] + [to_x, to_c, to_y]:
        pl.semaphore_signal(barrier, inc=1, device_id=dev, device_id_type=MESH)
    pl.semaphore_wait(barrier, Z + 2)

    def number(per):
        table = {}
        for key, count in per:
            for i in range(count):
                table[key, i] = len(table)
        return table

    pieces = [(s, m) for s in range(2) for m in range(7)]
    az = number((p, 6 if p[1] in X_FIRST else 3) for p in pieces)
    ax = number((p, 1 if p[1] in X_FIRST else 4) for p in pieces)
    rz = number((p, 8 if p in Z_FIRST else 4) for p in pieces if p[1])
    rx = number((p, 1 if p in Z_FIRST else 4) for p in pieces if p[1])

    def wait_bytes(m, count, sem):
        if m == SMALL:
            v = stats.at[pl.ds(0, 8 * count), :]
        else:
            v = wdown.at[:, pl.ds(0, count * WIDTH[m] // 32), :]
        pltpu.make_async_copy(v, v, sem).wait()

    def ag_share(s, m):
        p = s * 7 + m

        @pl.when(c == s)
        def _():
            dst = block(m, w[m], s, me)
            remote(shards[m], dst, asem_s.at[p], asem_c.at[p, 0], to_c).start()
            pltpu.make_async_copy(shards[m], dst, asem_c.at[p, 0]).start()

    def ag_shared(s, m):
        whole = block(m, w[m], s, me)
        pltpu.make_async_copy(whole, whole, asem_c.at[s * 7 + m, 0]).wait()

    def ag_own_z(s, m, col):
        p, first = s * 7 + m, az[(s, m), col * 3]
        b = block(m, w[m], s, at_dp(SELF, col), c)
        slot = jnp.where(inner, INNER, FAR) - 1
        remote(b, b, asem_s.at[p], asem_z.at[first], to_z(near)).start()
        remote(b, b, asem_s.at[p], asem_z.at[first + slot], to_z(places[INNER])).start()

    def ag_to_x(s, m, k):
        b = block(m, w[m], s, at_dp(k, 0), c)
        remote(b, b, asem_s.at[s * 7 + m], asem_x.at[ax[(s, m), k]], to_x).start()

    def ag_to_c(s, m, k, col):
        p = s * 7 + m
        b = block(m, w[m], s, at_dp(k, col), c)
        remote(b, b, asem_s.at[p], asem_c.at[p, 1], to_c).start()

    def ag_z(s, m, k, col):
        b = block(m, w[m], s, at_dp(k, col), c)
        cp = remote(b, b, asem_s.at[s * 7 + m], asem_z.at[az[(s, m), col * 3 + k - 1]], to_z(near))
        cp.wait_recv()
        if k != NEAR:

            @pl.when(inner)
            def _():
                cp.start()

        if m not in X_FIRST:
            ag_to_x(s, m, k)
        ag_to_c(s, m, k, col)

    def ag_x(s, m, k):
        b = block(m, w[m], s, at_dp(k, 1), c)
        remote(b, b, asem_s.at[s * 7 + m], asem_x.at[ax[(s, m), k]], to_x).wait_recv()
        if m in X_FIRST:
            ag_own_z(s, m, 1)
        ag_to_c(s, m, k, 1)

    def ag_need(s, m):
        wait_bytes(m, 7, asem_c.at[s * 7 + m, 1])

    def ag_sent(s, m):
        count = 7 + (1 + 4 if m in X_FIRST else 4 + 2)
        extra = 4 if m in X_FIRST else 2
        for ins in range(2):
            for own in range(2):

                @pl.when(jnp.logical_and(inner_i == ins, jnp.where(c == s, 1, 0) == own))
                def _():
                    wait_bytes(m, count + extra * ins + 2 * own, asem_s.at[s * 7 + m])

    def rows_of(b):
        return pl.ds(b * LP, LP)

    def y_src(k):
        return slps.at[1, :, pl.ds(0, 1024)] if k == 7 else ys

    def y_start(k, b, n):
        cols = lanes(n * 2, 256)
        src = y_src(k).at[rows_of(b), cols]
        remote(src, yr.at[k % 2, rows_of(b), cols], ysem_s.at[k * 2 + b], ysem.at[k * 2 + b], to_y).start()

    def y_wait(k, b):
        src = y_src(k).at[rows_of(b), pl.ds(0, 1024)]
        cp = remote(src, yr.at[k % 2, rows_of(b), :], ysem_s.at[k * 2 + b], ysem.at[k * 2 + b], to_y)
        cp.wait_recv()
        cp.wait_send()

    def y_sum(k, rows):
        return y_src(k)[rows, :].astype(F32) + yr[k % 2, rows, :].astype(F32)

    small_in = [
        pltpu.make_async_copy(ref, raw.at[i], isem.at[2 + i])
        for i, ref in enumerate((gain1_ref, shift1_ref, bias_o_ref, gain2_ref, shift2_ref, bias_d_ref))
    ] + [pltpu.make_async_copy(qv_ref, rawq, isem.at[8]), pltpu.make_async_copy(upb_ref, rawu, isem.at[9])]

    def pack_small():
        for cp in small_in:
            cp.wait()

        def iota(shape, axis):
            return lax.broadcasted_iota(jnp.int32, shape, axis)

        def hot(test):
            return jnp.where(test, 1.0, 0.0).astype(BF)

        r = iota((32, 128), 0)
        v = jnp.zeros((32, 128), F32)
        for i in range(6):
            v = jnp.where(r == i, raw[i].astype(F32), v)
        for t in range(2):
            for e in range(2):
                pick_rows = hot(iota((32, 8), 1) == 2 * (iota((32, 8), 0) - 6 - 4 * t) + e)
                spread = hot(iota((8, 128), 1) == e * 64 + me * 8 + iota((8, 128), 0))
                rows = dot(pick_rows, rawq[t], 1, 0).astype(BF)
                v = v + dot(rows, spread, 1, 0)
        odd = me // 4
        pick_rows = hot(2 * iota((32, 8), 1) + odd == iota((32, 8), 0) - 14)
        spread = hot(iota((32, 128), 1) == lax.rem(me, 4) * 32 + iota((32, 128), 0))
        v = v + dot(dot(pick_rows, rawu[...], 1, 0).astype(BF), spread, 1, 0)
        pack[...] = v.astype(BF)

    def unpack_small(s):
        total = jnp.zeros((32, 128), F32)
        for d in range(2 * Z):
            piece = wsmall[s, d].astype(F32)
            total = total + piece
            for r in range(6):
                vec[s, r : r + 1, d * 128 : d * 128 + 128] = piece[r : r + 1, :]
        for k in range(8):
            vec[s, 6:7, k * 128 : k * 128 + 128] = total[6 + k : 7 + k, :]
            vec[s, 7:8, k * 128 : k * 128 + 128] = total[14 + k : 15 + k, :]
            vec[s, 8:9, k * 128 : k * 128 + 128] = total[22 + k : 23 + k, :]

    def row(s, r):
        return vec[s, r : r + 1, :]

    CH = 16

    lane = lax.broadcasted_iota(jnp.int32, (1, 128), 1)
    left = lane < 64
    live_col = lax.broadcasted_iota(jnp.int32, (1, LP), 1) < L
    INV2, MEAN1, INV1 = range(3)

    def stat_at(s, which):
        return 16 + 4 * s + which

    def put_stats(rows, *pairs):
        v = stats[rows, :]
        for at, value in pairs:
            v = jnp.where(lane == at, value, v)
        stats[rows, :] = v

    def stat(s, which, rows):
        at = stat_at(s, which)
        return stats[rows, :][:, at : at + 1]

    def norm_chunk(v):
        mean = jnp.mean(v, axis=-1, keepdims=True)
        cen = v - mean
        inv = lax.rsqrt(jnp.mean(cen * cen, axis=-1, keepdims=True) + EPS)
        return cen * inv, mean, inv

    def chunks(b, pair=1):
        def at(i):
            return pl.ds(pl.multiple_of(b * LP + i * CH, CH), CH)

        def wrap(body):
            count = LP // CH

            @pl.loop(0, count // pair)
            def _(i):
                for j in range(pair):
                    body(at(i * pair + j))

            for j in range(count % pair):
                body(at(count - 1 - j))

        return wrap

    def ln1(s, b):
        gain, shift = row(s, 0), row(s, 1)

        @chunks(b, 2)
        def _(rows):
            nrm, mean, inv = norm_chunk(xs[s, rows, :].astype(F32))
            put_stats(rows, (stat_at(s, MEAN1), mean), (stat_at(s, INV1), inv))
            low[rows, :] = (nrm * gain + shift).astype(BF)

    def norm1(s, rows):
        return (xs[s, rows, :].astype(F32) - stat(s, MEAN1, rows)) * stat(s, INV1, rows)

    def relow1(s, b, dst):
        gain, shift = row(s, 0), row(s, 1)

        @chunks(b)
        def _(rows):
            dst[rows, :] = (norm1(s, rows) * gain + shift).astype(BF)

    def load_woven(ref, sem, dst):
        cp = pltpu.make_async_copy(ref.at[c], woven.at[pl.ds(0, L)], sem)
        cp.start()
        cp.wait()
        woven[L:LP] = jnp.zeros((LP - L, 2, 1024), BF)

        @pl.loop(0, LP // 16)
        def _(i):
            dst[pl.ds(pl.multiple_of(i * 32, 32), 32), 0:1024] = woven[pl.ds(i * 16, 16)].reshape(32, 1024)

    def unweave(src, dst, b, alive):
        r = lax.broadcasted_iota(jnp.int32, (LP, R), 0)
        q = lax.broadcasted_iota(jnp.int32, (LP, R), 1)
        take = jnp.where(q == 2 * r + b, 1.0, 0.0)
        if alive is not None:
            take = take * alive
        take = take.astype(BF)

        @pl.loop(0, 4)
        def _(n):
            cols = lanes(n * 2, 256)
            dst[rows_of(b), cols] = dot(take, src[:, cols], 1, 0).astype(BF)

    def weave(src, tmp):
        r = lax.broadcasted_iota(jnp.int32, (R, R), 0)
        q = lax.broadcasted_iota(jnp.int32, (R, R), 1)
        put = jnp.where(q == lax.rem(r, 2) * LP + r // 2, 1.0, 0.0).astype(BF)

        @pl.loop(0, 4)
        def _(n):
            cols = lanes(n * 2, 256)
            tmp[:, cols] = dot(put, src[:, cols], 1, 0).astype(BF)

        @pl.loop(0, LP // 16)
        def _(i):
            woven[pl.ds(i * 16, 16)] = tmp[pl.ds(pl.multiple_of(i * 32, 32), 32), 0:1024].reshape(16, 2, 1024)

    def alive_of(b):
        return jnp.where(live_ref[c] > b, 1.0, 0.0)

    def project(s, b):
        for t in range(3):
            @pl.loop(0, 2)
            def _(n):
                cols = lanes(n * 2, 256)
                a = dot(low[rows_of(b), :], wqkv[t][s, :, cols], 1, 0)
                if t != 1:
                    base = 0 if t == 0 else 512
                    a = a + vec[s, 6:7, pl.ds(pl.multiple_of(base + n * 256, 256), 256)]
                qkvs[s, t, rows_of(b), cols] = a.astype(BF)

    def pick(h, v):
        return jnp.where(left if h == 0 else jnp.logical_not(left), v, jnp.zeros_like(v))

    def scores(q, k):
        return jnp.where(live_col, dot(q, k, 1, 1), -1e30)

    def attention(s, b):
        rows = rows_of(b)

        @pl.loop(0, 4)
        def _(i):
            cols = lanes(i)
            q, k, v = (qkvs[s, t, rows, cols] for t in range(3))
            q = q * jnp.asarray(0.125, BF)
            ones = jnp.ones_like(v)
            tops, parts = [], []
            for h in range(2):
                sc = scores(pick(h, q), k)
                tops.append(jnp.max(sc, axis=-1, keepdims=True))
                e = jnp.exp(sc - tops[h]).astype(BF)
                parts.append(dot(e, jnp.where(left, v, ones) if h == 0 else jnp.where(left, ones, v), 1, 0))
            den = pltpu.roll(jnp.where(left, parts[1], parts[0]), 64, 1)
            mixs[s, rows, cols] = (jnp.where(left, parts[0], parts[1]) / den).astype(BF)
            lse = jnp.where(left, tops[0], tops[1]) + jnp.log(den)
            stats[rows, :] = jnp.where(lax.rem(lane, 64) == 8 * s + i, lse, stats[rows, :])

    def out_project(s, b, k):
        @pl.loop(0, 4)
        def _(n):
            cols = lanes(n * 2, 256)
            ys[rows_of(b), cols] = dot(mixs[s, rows_of(b), :], wout[s, :, cols], 1, 0).astype(BF)
            y_start(k, b, n)

    def middle(s, b, k):
        shift, gain2, shift2 = row(s, 2), row(s, 3), row(s, 4)

        @chunks(b, 2)
        def _(rows):
            v = xs[s, rows, :].astype(F32) + y_sum(k, rows) + shift
            if s == 0:
                mid[rows, :] = v
            else:
                gb[0, rows, :] = v.astype(BF)
            nrm, _, inv = norm_chunk(v)
            nrm2s[s, rows, :] = nrm.astype(BF)
            put_stats(rows, (stat_at(s, INV2), inv))
            low[rows, :] = (nrm * gain2 + shift2).astype(BF)

    def up_project(s, b):
        @pl.loop(0, 8)
        def _(n):
            cols = lanes(n * 2, 256)
            acc[...] = dot(low[rows_of(b), :], wup[s, :, cols], 1, 0)
            at = pl.ds(pl.multiple_of(lax.rem(n, 4) * 256, 256), 256)
            bias = jnp.where(n < 4, vec[s, 7:8, at], vec[s, 8:9, at])

            @pl.loop(0, LP // 16)
            def _(i):
                rows = pl.ds(pl.multiple_of(b * LP + i * 16, 16), 16)
                a = acc[pl.ds(pl.multiple_of(i * 16, 16), 16), :] + bias
                phi = 0.5 * (1.0 + lax.erf(a * (2.0 ** -0.5)))
                dens = jnp.exp(-0.5 * a * a) * ((2.0 * math.pi) ** -0.5)
                gels[s, rows, cols] = (a * phi).astype(BF)
                slps[s, rows, cols] = (phi + a * dens).astype(BF)

    def down_project(s, b, k, send):
        @pl.loop(0, 4)
        def _(n):
            cols = lanes(n * 2, 256)
            y_src(k)[rows_of(b), cols] = dot(gels[s, rows_of(b), :], wdown[s, :, cols], 1, 0).astype(BF)
            if send:
                y_start(k, b, n)

    def finish(s, b, k, dst):
        shift, alive = row(s, 5), alive_of(b)

        @chunks(b)
        def _(rows):
            base = mid[rows, :] if s == 0 else slps[1, rows, 1024:2048].astype(F32)
            dst[rows, :] = ((base + y_sum(k, rows) + shift) * alive).astype(BF)

    def keep_middle(b):
        @chunks(b)
        def _(rows):
            slps[1, rows, 1024:2048] = gb[0, rows, :]

    def emit_copies(which, s):
        target = (act_out, gin_out)[which].at[c]
        src, q = woven.at[pl.ds(0, L)], which * 2 + s
        return pltpu.make_async_copy(src, target, osem.at[q]), remote(src, target, osem_s.at[q], osem_r.at[q], to_c)

    def emit(which, s):
        here, there = emit_copies(which, s)

        @pl.when(c == s)
        def _():
            here.start()

        @pl.when(c != s)
        def _():
            there.start()

    def emit_sent(which, s):
        here, there = emit_copies(which, s)

        @pl.when(c == s)
        def _():
            here.wait()

        @pl.when(c != s)
        def _():
            there.wait_send()

    def emit_got(which, s):
        @pl.when(c == s)
        def _():
            remote(
                woven.at[pl.ds(0, L)], (act_out, gin_out)[which].at[1 - c], osem_s.at[which * 2 + s], osem_r.at[which * 2 + s], to_c
            ).wait_recv()

    def relower(s, b, dst):
        gain2, shift2 = row(s, 3), row(s, 4)

        @chunks(b)
        def _(rows):
            dst[rows, :] = (nrm2s[s, rows, :].astype(F32) * gain2 + shift2).astype(BF)

    def fold8(v):
        return jnp.sum(v.reshape(v.shape[0] // 8, 8, v.shape[1]), axis=0)

    def colsum(v):
        return jnp.sum(v, axis=0, keepdims=True)

    def sum_rows(ref_slice, width):
        def step(i, tot):
            rows = pl.ds(pl.multiple_of(i * 32, 32), 32)
            return tot + fold8(ref_slice(rows).astype(F32))

        return colsum(lax.fori_loop(0, R // 32, step, jnp.zeros((8, width), F32)))

    def total(s, r, b, v):
        sv[s, r : r + 1, :] = v if b == 0 else sv[s, r : r + 1, :] + v

    def grad_gelu(s, b):
        @pl.loop(0, 8)
        def _(n):
            cols = lanes(n * 2, 256)
            rows_w = pl.ds(pl.multiple_of(n * 256, 256), 256)
            a = dot(gb[s, rows_of(b), :], wdown[s, rows_w, :], 1, 1)
            gpre[rows_of(b), cols] = (a * slps[s, rows_of(b), cols].astype(F32)).astype(BF)

    def grad_mlp_biases(s):
        sv[s, 5:6, :] = sum_rows(lambda r: gb[s, r, :], 1024)
        sv[s, 7:8, :] = sum_rows(lambda r: gpre[r, 0:1024], 1024)
        sv[s, 8:9, :] = sum_rows(lambda r: gpre[r, 1024:2048], 1024)

    def grad_down(s, h, dst):
        @pl.loop(0, 4)
        def _(i):
            first = h * 1024 + i * 256
            cols = pl.ds(pl.multiple_of(first, 256), 256)
            rows_w = pl.ds(pl.multiple_of(i * 256 if s == 1 else first, 256), 256)
            dst[rows_w, :] = dot(gels[s, :, cols], gb[s], 0, 0).astype(BF)

    def grad_low_two(s, b, k):
        @pl.loop(0, 4)
        def _(n):
            cols = lanes(n * 2, 256)
            rows_w = pl.ds(pl.multiple_of(n * 256, 256), 256)
            ys[rows_of(b), cols] = dot(gpre[rows_of(b), :], wup[s, rows_w, :], 1, 1).astype(BF)
            y_start(k, b, n)

    def grad_up(s, low2):
        @pl.loop(0, 4)
        def _(i):
            cols = lanes(i * 2, 256)
            rows_w = pl.ds(pl.multiple_of(i * 256, 256), 256)
            for q in range(2):
                wup[s, rows_w, q * 1024 : q * 1024 + 1024] = dot(
                    low2[:, cols], gpre[:, q * 1024 : q * 1024 + 1024], 0, 0
                ).astype(BF)

    def loop_sums(b, count, step):
        zero = jnp.zeros((8, 1024), F32)

        def body(i, tots):
            new = step(pl.ds(pl.multiple_of(b * LP + i * CH, CH), CH))
            return tuple(t + fold8(v) for t, v in zip(tots, new))

        return [colsum(t) for t in lax.fori_loop(0, LP // CH, body, (zero,) * count)]

    def grad_middle(s, b, k):
        gain = row(s, 3)

        def step(rows):
            g2 = y_sum(k, rows)
            nrm = nrm2s[s, rows, :].astype(F32)
            t = g2 * gain
            m1 = jnp.mean(t, axis=-1, keepdims=True)
            m2 = jnp.mean(t * nrm, axis=-1, keepdims=True)
            gm = gb[s, rows, :].astype(F32) + stat(s, INV2, rows) * (t - m1 - nrm * m2)
            mid[rows, :] = gm
            ga = gm.astype(BF)
            low[rows, :] = ga
            return g2 * nrm, g2, ga.astype(F32)

        for r, v in zip((3, 4, 2), loop_sums(b, 3, step)):
            total(s, r, b, v)

    def grad_mixed(s, b):
        @pl.loop(0, 2)
        def _(n):
            cols = lanes(n * 2, 256)
            rows_w = pl.ds(pl.multiple_of(n * 256, 256), 256)
            gpre[rows_of(b), cols] = dot(low[rows_of(b), :], wout[s, rows_w, :], 1, 1).astype(BF)

    def grad_out(s):
        @pl.loop(0, 2)
        def _(i):
            cols = lanes(i * 2, 256)
            rows_w = pl.ds(pl.multiple_of(i * 256, 256), 256)
            wout[s, rows_w, :] = dot(mixs[s, :, cols], low[...], 0, 0).astype(BF)

    def grad_attention(s, b):
        rows = rows_of(b)

        @pl.loop(0, 4)
        def _(i):
            cols = lanes(i)
            q, k, v = (qkvs[s, t, rows, cols] for t in range(3))
            q, k_low = q * jnp.asarray(0.125, BF), k * jnp.asarray(0.125, BF)
            gm = gpre[rows, cols]
            kept = stats[rows, :]
            res = []
            for h in range(2):
                lse = jnp.sum(jnp.where(lane == 64 * h + 8 * s + i, kept, 0.0), axis=-1, keepdims=True)
                probs = jnp.exp(scores(pick(h, q), k) - lse)
                gp = dot(pick(h, gm), v, 1, 1)
                gv = dot(probs.astype(BF), gm, 0, 0)
                gs = (probs * (gp - jnp.sum(probs * gp, axis=-1, keepdims=True))).astype(BF)
                res.append((dot(gs, k_low, 1, 0), dot(gs, q, 0, 0), gv))
            for t in range(3):
                gqkv[t, rows, cols] = jnp.where(left, res[0][t], res[1][t]).astype(BF)

    def grad_qv_bias(s):
        sv[s, 6:7, 0:512] = sum_rows(lambda r: gqkv[0, r, :], 512)
        sv[s, 6:7, 512:1024] = sum_rows(lambda r: gqkv[2, r, :], 512)

    def grad_lowered(s, b, k):
        rows = rows_of(b)

        @pl.loop(0, 4)
        def _(n):
            cols = lanes(n * 2, 256)
            rows_w = pl.ds(pl.multiple_of(n * 256, 256), 256)
            a = dot(gqkv[0, rows, :], wqkv[0][s, rows_w, :], 1, 1)
            a = a + dot(gqkv[1, rows, :], wqkv[1][s, rows_w, :], 1, 1)
            a = a + dot(gqkv[2, rows, :], wqkv[2][s, rows_w, :], 1, 1)
            ys[rows, cols] = a.astype(BF)
            y_start(k, b, n)

    def grad_qkv(s, t, low1):
        @pl.loop(0, 4)
        def _(i):
            cols = lanes(i * 2, 256)
            rows_w = pl.ds(pl.multiple_of(i * 256, 256), 256)
            wqkv[t][s, rows_w, :] = dot(low1[:, cols], gqkv[t], 0, 0).astype(BF)

    def grad_stream(s, b, k, dst):
        gain = row(s, 0)

        def step(rows):
            g1 = y_sum(k, rows)
            nrm = norm1(s, rows)
            t = g1 * gain
            m1 = jnp.mean(t, axis=-1, keepdims=True)
            m2 = jnp.mean(t * nrm, axis=-1, keepdims=True)
            dst[rows, :] = (mid[rows, :] + stat(s, INV1, rows) * (t - m1 - nrm * m2)).astype(BF)
            if s == 1:
                low[rows, :] = (nrm * gain + row(s, 1)).astype(BF)
            return g1 * nrm, g1

        for r, v in zip((0, 1), loop_sums(b, 2, step)):
            total(s, r, b, v)

    def add_rows(dst, src, count, chunk):
        @pl.loop(0, count // chunk)
        def _(i):
            rows = pl.ds(pl.multiple_of(i * chunk, chunk), chunk)
            dst[rows, :] = dst[rows, :] + src[rows, :]

    def shape_of(m):
        if m in BY_ROWS:
            return 128, (16 if m == UP else 64)
        return WIDTH[m] // 2, 128

    def add_block(m, dst, src):
        add_rows(dst, src, *shape_of(m))

    def g_half(s, m):
        return stage if (s, m) == (1, DOWN) else half(m, w[m], s, c)

    def g_block(s, m, d):
        if (s, m) == (1, DOWN):
            return stage.at[:, pl.ds(pl.multiple_of(d * 128, 128), 128)]
        return block(m, w[m], s, d, c)

    def r_view(s, m, h):
        return rbuf[m] if s == 1 else half(m, w[m], 1, h)

    def x_view(s, m, k, col):
        if (s, m) in Z_FIRST:
            return xbuf[m].at[s]
        if s == 0 and m in (Q, K, V):
            return gels.at[1, pl.ds((m - Q) * 128, 128), pl.ds(k * 256, 256)]
        if s == 0:
            return block(m, w[m], 1, at_dp(k, col), c)
        at = pl.ds(k * 128, 128)
        return xbuf[m].at[at, :] if m in BY_ROWS else xbuf[m].at[:, at]

    def z_view(s, m, slot, col, place):
        if s == 0 and m in (Q, K, V):
            i = col * 4 + slot if (s, m) in Z_FIRST else 4 + slot
            return gels.at[1, pl.ds((m - Q) * 128, 128), pl.ds(i * 256, 256)]
        if s == 0:
            return block(m, w[m], 1, place * 2 + (x if col == 0 else 1 - x), c)
        if m in (UP, DOWN):
            at = pl.ds(slot * 128, 128)
            return rbuf[m].at[at, :] if m == UP else rbuf[m].at[:, at]
        return zbuf[m].at[col * 4 + slot]

    def rs_c(s, m):
        q = s * 6 + m - 1
        if s == 0:
            pl.semaphore_wait(free_c.at[m - 1], 1)
        if (s, m) == (1, UP):
            pl.semaphore_wait(free_up, 1)
        src = rup if (s, m) == (1, DOWN) else half(m, w[m], s, 1 - c)
        remote(src, r_view(s, m, c), rsem_cs.at[q], rsem_c.at[q], to_c).start()

    def rs_sum(s, m):
        q = s * 6 + m - 1
        mine, got = g_half(s, m), r_view(s, m, 1 - c)
        cp = remote(mine, got, rsem_cs.at[q], rsem_c.at[q], to_c)
        cp.wait_recv()
        cp.wait_send()
        if (s, m) == (1, DOWN):
            pl.semaphore_signal(free_up, inc=1, device_id=to_c, device_id_type=MESH)
        elif s == 1:
            pl.semaphore_signal(free_c.at[m - 1], inc=1, device_id=to_c, device_id_type=MESH)
        rows = 1024 if m in BY_ROWS else WIDTH[m] // 2
        add_rows(mine, got, rows, 16 if m not in (Q, K, V) else 64)
        if s == 1 and m in (UP, DOWN):
            z_credit(free_r.at[m - UP])

    def rs_to_x(s, m):
        if s == 0:
            pl.semaphore_wait(free_x.at[m - 1], 1)
        for k in (INNER, FAR, NEAR, SELF):
            q = s * 6 + m - 1
            b = g_block(s, m, at_dp(k, 1))
            remote(b, x_view(s, m, k, 0), rsem_xs.at[q], rsem_x.at[rx[(s, m), k]], to_x).start()

    def rs_from_x(s, m, k):
        q = s * 6 + m - 1
        b = g_block(s, m, at_dp(k, 0))
        got = x_view(s, m, k, 1)
        remote(b, got, rsem_xs.at[q], rsem_x.at[rx[(s, m), k]], to_x).wait_recv()
        if k == SELF:
            wait_bytes(m, 4, rsem_xs.at[q])
        add_block(m, b, got)

    def down_freed():
        pl.semaphore_signal(free_c.at[DOWN - 1], inc=1, device_id=to_c, device_id_type=MESH)
        x_freed(DOWN)
        z_freed(DOWN)

    def gelu_freed():
        for m in (Q, K, V):
            if (0, m) not in Z_FIRST:
                x_freed(m)
        for m in (Q, K, V):
            z_freed(m)

    def x_freed(m):
        pl.semaphore_signal(free_x.at[m - 1], inc=1, device_id=to_x, device_id_type=MESH)

    def z_wait_credits(sem):
        @pl.when(inner)
        def _():
            pl.semaphore_wait(sem, 3)

        @pl.when(jnp.logical_not(inner))
        def _():
            pl.semaphore_wait(sem, 1)

    def z_credit(sem):
        for k in (NEAR, INNER):
            pl.semaphore_signal(sem, inc=1, device_id=to_z(places[k]), device_id_type=MESH)

    def z_ready(s, m):
        if s == 0:
            z_wait_credits(free_z.at[m - 1])
        elif m in (UP, DOWN):
            z_wait_credits(free_r.at[m - UP])

    def rs_to_z(s, m, k, col):
        q = s * 6 + m - 1
        b = g_block(s, m, at_dp(k, col))
        if k == NEAR:
            remote(b, z_view(s, m, 0, col, z), rsem_zs.at[q, col], rsem_z.at[rz[(s, m), col * 4]], to_z(near)).start()
        else:

            @pl.when(jnp.logical_not(inner))
            def _():
                remote(b, z_view(s, m, k, col, places[k]), rsem_zs.at[q, col], rsem_z.at[rz[(s, m), col * 4 + k]], to_z(near)).start()

    def rs_pass(s, m, k, col):
        q = s * 6 + m - 1

        @pl.when(inner)
        def _():
            b = g_block(s, m, at_dp(k, col))
            got = z_view(s, m, k, col, places[k])
            remote(b, got, rsem_zs.at[q, col], rsem_z.at[rz[(s, m), col * 4 + k]], to_z(near)).wait_recv()
            add_block(m, b, got)
            remote(b, z_view(s, m, 1, col, places[k]), rsem_zs.at[q, col], rsem_z.at[rz[(s, m), col * 4 + 1]], to_z(places[k])).start()

    def z_arrived(s, m, col):
        q = s * 6 + m - 1
        got = [z_view(s, m, 0, col, near), z_view(s, m, 1, col, z)]
        for slot in range(2):
            remote(got[slot], got[slot], rsem_zs.at[q, col], rsem_z.at[rz[(s, m), col * 4 + slot]], to_z(near)).wait_recv()
        return got

    def z_sent(s, m, col):
        wait_bytes(m, 3, rsem_zs.at[s * 6 + m - 1, col])

    def z_freed(m):
        z_credit(free_z.at[m - 1])

    def rs_fold(s, m):
        q = s * 6 + m - 1
        b = g_block(s, m, at_dp(SELF, 1))
        for got in z_arrived(s, m, 1):
            add_block(m, b, got)
        remote(b, xbuf[m].at[s], rsem_xs.at[q], rsem_x.at[rx[(s, m), 0]], to_x).start()

    def f_target(m):
        n = WIDTH[m] // 2
        at = pl.ds(pl.multiple_of(c * n, n), n)
        if m in (Q, K, V):
            return gqkv_out.at[m - 1, :, at]
        if m == UP:
            return gup_out.at[:, at]
        return (gout_out if m == OUT else gdown_out).at[at, :]

    def rs_f(s, m):
        q = s * 6 + m - 1
        mine = g_block(s, m, me)
        parts = [mine] + z_arrived(s, m, 0)
        if (s, m) in Z_FIRST:
            cp = remote(mine, xbuf[m].at[s], rsem_xs.at[q], rsem_x.at[rx[(s, m), 0]], to_x)
            cp.wait_recv()
            cp.wait_send()
            parts.append(xbuf[m].at[s])
        count, chunk = shape_of(m)
        chunk = min(chunk, 64)

        @pl.loop(0, count // chunk)
        def _(i):
            rows = pl.ds(pl.multiple_of(i * chunk, chunk), chunk)
            a = parts[0][rows, :].astype(F32)
            for part in parts[1:]:
                a = a + part[rows, :].astype(F32)
            fbuf[m][rows, :] = a

        for col in range(2) if (s, m) in Z_FIRST else (0,):
            z_sent(s, m, col)
        if s == 1 and m in (UP, OUT):
            z_freed(m)

        @pl.when(c == s)
        def _():
            pltpu.make_async_copy(fbuf[m], f_target(m), rsem_fs.at[q]).start()

        @pl.when(c != s)
        def _():
            remote(fbuf[m], f_target(m), rsem_fs.at[q], rsem_f.at[q], to_c).start()

    def rs_f_sent(s, m):
        q = s * 6 + m - 1

        @pl.when(c == s)
        def _():
            pltpu.make_async_copy(fbuf[m], f_target(m), rsem_fs.at[q]).wait()

        @pl.when(c != s)
        def _():
            remote(fbuf[m], f_target(m), rsem_fs.at[q], rsem_f.at[q], to_c).wait_send()

    def rs_end(s, m):
        q = s * 6 + m - 1

        @pl.when(c == s)
        def _():
            remote(fbuf[m], fbuf[m], rsem_fs.at[q], rsem_f.at[q], to_c).wait_recv()

    def vec_copies(i):
        if i == 0:
            return [remote(sv.at[1 - c], svc, vsem_s.at[0], vsem.at[0], to_c)]
        if i == 1:
            return [remote(sv.at[c], svx, vsem_s.at[1], vsem.at[1], to_x)]
        if i == 2:
            return [
                remote(svc, svz.at[j - 1], vsem_s.at[1 + j], vsem.at[1 + j], to_z(lax.rem(z + j, Z)))
                for j in range(1, Z)
            ]
        return [
            pltpu.make_async_copy(sv.at[c, pl.ds(0, 8)], gvec_out, isem.at[0]),
            pltpu.make_async_copy(vq, gqv_out, isem.at[1]),
            pltpu.make_async_copy(vu, gupb_out, isem.at[2]),
        ]

    def vec_step(i):
        if i:
            for cp in vec_copies(i - 1):
                cp.wait_recv()
                cp.wait_send()
        if i == 1:
            sv[c] = sv[c] + svc[...]
        if i == 2:
            svc[...] = sv[c] + svx[...]
        if i == 3:
            sv[c] = svc[...] + svz[0] + svz[1] + svz[2]
            for t in range(2):
                for h in range(8):
                    at = (t * 8 + h) * 64
                    vq[t, h : h + 1, :] = sv[c, 6:7, at : at + 64]
            for g in range(8):
                vu[g : g + 1, :] = sv[c, 7 + g // 4 : 8 + g // 4, g % 4 * 256 : g % 4 * 256 + 256]
        for cp in vec_copies(i):
            cp.start()

    clock = Clock()
    size = {SMALL: 8e3, Q: 131e3, K: 131e3, V: 131e3, OUT: 131e3, UP: 524e3, DOWN: 524e3}
    RATE = 82e3
    HOP = 1.8
    free = {"x": 0.0, "z": 0.0, "y": 0.0}
    got = {}

    def link(name, nbytes):
        free[name] = max(free[name], clock.now) + nbytes / RATE
        return free[name] + HOP

    order = (SMALL, Q, K, V, OUT, UP, DOWN)
    for cp in small_in:
        cp.start()
    for s in range(2):
        for m in order[1:]:
            ag_share(s, m)
    pack_small()
    for s in range(2):
        ag_share(s, SMALL)
    clock.now = 6.5

    def plan_gather(s, m):
        x_first = m in X_FIRST

        def at_x(k):
            ag_x(s, m, k)
            got[s, m] = got.get((s, m), 0) + 1
            if x_first:
                along_z(1)

        def at_z(k, col):
            ag_z(s, m, k, col)
            if x_first:
                got[s, m] = got.get((s, m), 0) + 1
            else:
                clock.add(link("x", size[m]), functools.partial(at_x, k))

        def along_z(col):
            begin = max(free["z"], clock.now)
            t = size[m] / RATE
            free["z"] = begin + 3 * t
            for k in (NEAR, INNER, FAR):
                late = HOP if k == NEAR else 2 * HOP
                clock.add(begin + k * t + late, functools.partial(at_z, k, col))

        def own():
            if not x_first:
                ag_shared(s, m)
            ag_own_z(s, m, 0)
            along_z(0)
            if not x_first:
                ag_to_x(s, m, SELF)
                clock.add(link("x", size[m]), functools.partial(at_x, SELF))

        def early():
            ag_shared(s, m)
            ag_to_x(s, m, SELF)
            clock.add(max(link("x", size[m]), z_begin[s, m] - LEAD + 0.1), functools.partial(at_x, SELF))

        if x_first:
            clock.add(x_begin[s, m], early)
        clock.add(max(z_begin[s, m] - LEAD, clock.now), own)

    LEAD, AHEAD = 23.0, 8.0
    z_begin, x_begin, at = {}, {}, 7.0
    for s in range(2):
        for m in order:
            z_begin[s, m] = at
            at += size[m] / RATE * (6 if m in X_FIRST else 3)
            x_begin[s, m] = max(clock.now, z_begin[s, m] - LEAD - AHEAD)
    for s in range(2):
        for m in order:
            plan_gather(s, m)

    def need(s, m):
        clock.drain(lambda: got.get((s, m), 0) == (7 if m in X_FIRST else 4))
        clock.now += 1.5
        ag_need(s, m)

    def y_sent():
        return link("y", 426e3 * 2) + 1.0

    passed = set()

    def reduce(s, m):
        x_first = (s, m) in Z_FIRST
        t = size[m] / RATE
        order = (INNER, FAR, NEAR)

        def z_start(k, col):
            rs_to_z(s, m, k, col)
            ready = link("z", size[m])
            if k != NEAR:
                clock.add(ready, functools.partial(z_pass, k, col), 0.4)

        def z_pass(k, col):
            rs_pass(s, m, k, col)
            done.append((k, col))
            if len([d for d in done if d[1] == col]) == 2:
                ready = clock.now + t + 2 * HOP + 8.0
                if x_first and col == 1:
                    clock.add(ready, fold, 0.4)
                elif not x_first:
                    clock.add(ready, finish_sum, 0.6)

        done = []

        def fold():
            rs_fold(s, m)
            clock.add(max(link("x", size[m]), clock.now + 2.0), finish_sum, 0.6)

        def sum_step():
            rs_sum(s, m)
            passed.add(("c", s, m))
            if x_first:
                if s == 0:
                    clock.drain(lambda: ("z", m) in passed)
                z_ready(s, m)
                for col in (1, 0):
                    for k in order:
                        z_start(k, col)
            else:
                if s == 0:
                    clock.drain(lambda: ("x", m) in passed)
                rs_to_x(s, m)
                for k in order + (SELF,):
                    clock.add(link("x", size[m]) + 1.5, functools.partial(from_x, k), 0.3)

        def from_x(k):
            rs_from_x(s, m, k)
            if k == SELF:
                done.append((SELF, -1))
                if s == 1:
                    if m == UP:
                        x_freed(m)
                        passed.add(("x", m))
                return
            if k == INNER:
                if s == 0:
                    clock.drain(lambda: ("z", m) in passed)
                z_ready(s, m)
            z_start(k, 0)

        def finish_sum():
            clock.drain(lambda: ready_to_finish())
            if s == 0:
                clock.drain(lambda: ("f", m) in passed)
                rs_f_sent(1, m)
            rs_f(s, m)
            if s == 1:
                passed.add(("f", m))
                if m in (UP, OUT):
                    passed.add(("z", m))

        def ready_to_finish():
            return x_first or (SELF, -1) in done

        if s == 0:
            clock.drain(lambda: ("c", 1, m) in passed)
        elif m == UP:
            clock.drain(lambda: ("c", 1, DOWN) in passed)
        rs_c(s, m)
        clock.add(clock.now + 4 * size[m] / 500e3 + 2.0, sum_step, 0.8)

    clock.run(2.0, load_woven, x_ref, isem.at[0], gpre)
    for b in range(2):
        clock.run(0.6, unweave, gpre, xs.at[0], b, None)
    y_at = {}
    for s in range(2):
        last = s == 1
        need(s, SMALL)
        unpack_small(s)
        for b in range(2):
            if last:
                clock.wait(y_at[1, b], y_wait, 1, b)
                clock.run(1.0, finish, 0, b, 1, xs.at[1])
            clock.run(1.7, ln1, s, b)
            if b == 0:
                for m in (Q, K, V):
                    need(s, m)
            clock.run(1.7, project, s, b)
            clock.run(3.0, attention, s, b)
            if b == 0:
                need(s, OUT)
            clock.run(0.9, out_project, s, b, s * 2)
            y_at[s * 2, b] = y_sent()
        if last:
            clock.run(1.5, weave, xs.at[1], gpre)
            emit(0, 0)
        for b in range(2):
            clock.wait(y_at[s * 2, b], y_wait, s * 2, b)
            clock.run(1.5, middle, s, b, s * 2)
            if b == 0:
                need(s, UP)
            clock.run(4.0, up_project, s, b)
        if not last:
            need(0, DOWN)
            for b in range(2):
                clock.run(1.5, down_project, 0, b, 1, True)
                y_at[1, b] = y_sent()
            clock.run(2.0, load_woven, cot_ref, isem.at[1], gpre)
            for b in range(2):
                clock.run(0.6, unweave, gpre, gb.at[1], b, alive_of(b))

    clock.run(1.9, grad_down, 1, 1 - c, rup)
    reduce(1, DOWN)
    clock.run(1.9, grad_down, 1, c, stage)
    need(1, DOWN)
    for b in range(2):
        clock.run(2.7, grad_gelu, 1, b)
        clock.run(2.0, grad_low_two, 1, b, 3)
        y_at[3, b] = y_sent()
    for q in range(2):
        for m in order:
            ag_sent(q, m)
    for s in (1, 0):
        k = 3 if s == 1 else 5
        clock.run(3.0, grad_up, s, low if s == 1 else gb.at[1])
        reduce(s, UP)
        if s == 0:
            for b in range(2):
                clock.run(1.7, down_project, 1, b, 7, False)
            down_freed()
            gelu_freed()
            passed.update({("c", 1, DOWN), ("x", DOWN), ("z", DOWN), ("x", Q), ("x", K), ("x", V), ("z", Q), ("z", K), ("z", V)})
            clock.run(1.9, grad_down, 0, 1 - c, wdown.at[0])
            reduce(0, DOWN)
            clock.run(1.9, grad_down, 0, c, wdown.at[0])
            for t in range(3):
                clock.run(1.4, grad_qkv, 1, t, low)
                reduce(1, Q + t)
            clock.run(0.5, grad_qv_bias, 1)
        clock.run(0.6, grad_mlp_biases, s)
        if s == 1:
            for b in range(2):
                clock.run(0.3, keep_middle, b)
        if s == 0:
            emit_sent(0, 0)
            clock.run(1.5, weave, gb.at[0], gpre)
            emit(1, 1)
        if s == 0:
            for b in range(2):
                clock.run(0.8, relow1, 0, b, gb.at[1])
        for b in range(2):
            clock.wait(y_at[k, b], y_wait, k, b)
            clock.run(1.9, grad_middle, s, b, k)
            clock.run(0.5, grad_mixed, s, b)
            if b == 1:
                clock.run(0.9, grad_out, s)
                reduce(s, OUT)
            clock.run(3.8, grad_attention, s, b)
            clock.run(1.6, grad_lowered, s, b, k + 1)
            y_at[k + 1, b] = y_sent()
        if s == 1:
            for b in range(2):
                clock.wait(y_at[4, b], y_wait, 4, b)
                clock.run(2.2, grad_stream, 1, b, 4, gb.at[0])
                clock.run(2.7, grad_gelu, 0, b)
                clock.run(2.0, grad_low_two, 0, b, 5)
                y_at[5, b] = y_sent()
                if b == 0:
                    for q in range(2):
                        clock.run(0.5, relower, 0, q, gb.at[1])
        else:
            pl.semaphore_signal(free_y, inc=1, device_id=to_y, device_id_type=MESH)
            pl.semaphore_wait(free_y, 1)
            for b in range(2):
                for n in range(4):
                    y_start(7, b, n)
                y_at[7, b] = y_sent()
            for t in range(3):
                clock.run(1.4, grad_qkv, 0, t, gb.at[1])
                reduce(0, Q + t)
            clock.run(0.5, grad_qv_bias, 0)
    for b in range(2):
        clock.wait(y_at[6, b], y_wait, 6, b)
        clock.run(2.2, grad_stream, 0, b, 6, low)
    def vec_chain(i):
        vec_step(i)
        if i < 3:
            ready = (clock.now + 3.0, link("x", 131e3) + 1.0, link("z", 262e3) + 4.0)[i]
            clock.add(ready, functools.partial(vec_chain, i + 1), 0.5)

    vec_chain(0)
    emit_sent(1, 1)
    clock.run(2.0, weave, low, gpre)
    emit(1, 0)
    for b in range(2):
        clock.wait(y_at[7, b], y_wait, 7, b)
        clock.run(1.0, finish, 1, b, 7, gb.at[1])
    emit_sent(1, 0)
    clock.run(2.0, weave, gb.at[1], gpre)
    emit(0, 1)
    clock.drain(lambda: not clock.queue)
    for cp in vec_copies(3):
        cp.wait()
    for m in MATS:
        rs_f_sent(0, m)
    for s in range(2):
        for m in MATS:
            rs_end(s, m)
    emit_sent(0, 1)
    for which in range(2):
        for s in range(2):
            emit_got(which, s)


def run_kernel(*args):
    any_spec = pl.BlockSpec(memory_space=pl.ANY)
    V = pltpu.VMEM
    D_ = pltpu.SemaphoreType.DMA
    REG = pltpu.SemaphoreType.REGULAR
    S = jax.ShapeDtypeStruct
    mats = ((1024, 512), (1024, 512), (1024, 512), (512, 1024), (1024, 2048), (2048, 1024))
    by_rows = (True, True, True, False, True, False)
    first = (False, True, False, True, False, False)

    def halved(shape, rows, cut):
        return (shape[0] // cut, shape[1] // 2) if rows else (shape[0] // 2, shape[1] // cut)

    scratch = [V((2, 8, 32, 128), BF)]
    scratch += [V((2,) + shape, BF) for shape in mats]
    scratch += [V(halved(shape, rows, 1), BF) for shape, rows in zip(mats, by_rows)]
    scratch += [
        V((2,) + halved(shape, rows, 8) if f else halved(shape, rows, 2), BF)
        for shape, rows, f in zip(mats, by_rows, first)
    ]
    scratch += [V((8 if f else 4,) + halved(shape, rows, 8), BF) for shape, rows, f in zip(mats[:4], by_rows, first)]
    scratch += [V(halved(shape, rows, 8), F32) for shape, rows in zip(mats, by_rows)]
    scratch += [
        V((2, R, 1024), BF), V((2, 3, R, 512), BF), V((2, R, 512), BF), V((2, R, 1024), BF),
        V((2, R, 2048), BF), V((2, R, 2048), BF), V((R, 128), F32),
        V((R, 1024), BF), V((R, 1024), F32), V((2, R, 1024), BF), V((R, 2048), BF), V((3, R, 512), BF),
        V((R, 1024), BF), V((2, R, 1024), BF), V((LP, 256), F32),
        V((2, 16, 1024), F32), V((2, 16, 1024), F32), V((16, 1024), F32), V((16, 1024), F32), V((3, 16, 1024), F32),
        V((LP, 2, 1024), BF), V((1024, 1024), BF), V((32, 128), BF), V((6, 1, 128), BF), V((2, 8, 8), BF), V((8, 32), BF), V((2, 8, 64), F32), V((8, 256), F32),
        D_((14,)), D_((14, 2)), D_((54,)), D_((44,)),
        D_((12,)), D_((12,)), D_((12,)), D_((48,)), D_((12, 2)), D_((64,)), D_((12,)), D_((12,)),
        D_((16,)), D_((16,)), D_((4,)), D_((4,)), D_((4,)), D_((10,)), D_((5,)), D_((5,)),
        REG((6,)), REG((6,)), REG((6,)), REG, REG((2,)), REG,
    ]
    return pl.pallas_call(
        kernel,
        out_shape=[
            S((2, L, 2, 1024), BF), S((2, L, 2, 1024), BF), S((3, 128, 512), F32), S((512, 128), F32),
            S((128, 2048), F32), S((2048, 128), F32), S((8, 1024), F32), S((2, 8, 64), F32), S((8, 256), F32),
        ],
        in_specs=[any_spec] * 14 + [pl.BlockSpec(memory_space=pltpu.SMEM)],
        out_specs=[any_spec] * 9,
        scratch_shapes=scratch,
        compiler_params=pltpu.CompilerParams(
            collective_id=1, has_side_effects=True, vmem_limit_bytes=67043328
        ),
        name="sections",
    )(*args)


def local_fast(images, cotangent, live_count, ln1_gain, ln1_bias, qkv_weight, qv_bias, out_weight, out_bias,
               ln2_gain, ln2_bias, up_weight, up_bias, down_weight, down_bias):
    d = lax.axis_index("dp")

    def woven(a):
        return jnp.transpose(a, (0, 2, 1, 3))

    act, gin, gqkv, gout, gup, gdown, gvec, gqv, gupb = run_kernel(
        ln1_gain, ln1_bias, out_bias, ln2_gain, ln2_bias, down_bias, qv_bias[0], up_bias[0],
        qkv_weight[0], out_weight[0], up_weight[0], down_weight[0], woven(images), woven(cotangent), live_count.reshape(2),
    )

    def cut(v, axis, n):
        return lax.dynamic_slice_in_dim(v, d * n, n, axis=axis)

    act, gin = woven(act)[None], woven(gin)[None]
    vecs = cut(gvec, 1, 128)
    qv = cut(gqv, 2, 8)
    upb = cut(gupb, 1, 32)
    return (
        act, gin, vecs[0:1], vecs[1:2], gqkv[None], qv[None], gout[None], vecs[2:3], vecs[3:4], vecs[4:5],
        gup[None], upb[None], gdown[None], vecs[5:6],
    )


def solution(mesh):
    fast = dict(mesh.shape) == {"section": 2, "dp": 8, "mp": 2}
    return jax.shard_map(
        local_fast if fast else local,
        mesh=mesh,
        in_specs=(
            P(None, "dp", None, None),
            P(None, "dp", None, None),
            P(None, "dp"),
            P("section", "dp"),
            P("section", "dp"),
            P("section", None, "dp", "mp"),
            P("section", None, "mp", "dp"),
            P("section", "mp", "dp"),
            P("section", "dp"),
            P("section", "dp"),
            P("section", "dp"),
            P("section", "dp", "mp"),
            P("section", "mp", "dp"),
            P("section", "mp", "dp"),
            P("section", "dp"),
        ),
        out_specs=(
            P("section", None, "dp", None, None),
            P("section", None, "dp", None, None),
            P("section", "dp"),
            P("section", "dp"),
            P("section", None, "dp", "mp"),
            P("section", None, "mp", "dp"),
            P("section", "mp", "dp"),
            P("section", "dp"),
            P("section", "dp"),
            P("section", "dp"),
            P("section", "dp", "mp"),
            P("section", "mp", "dp"),
            P("section", "mp", "dp"),
            P("section", "dp"),
        ),
        check_vma=False,
    )
```
